128 devices in a mesh: frame: 8 (over y_lo, z), space: 16 (over x, y_hi, core).
Axes of the slice: x: 4, y: 4 (y_hi: 2, y_lo: 2; y = y_hi * 2 + y_lo), z: 4, core: 2. Of those that a mesh axis runs over, the one named last changes fastest.
Arguments:
- tokens: bfloat16 [64, 304, 1024], P('space', 'frame'), may hold values from -16 to 16
- tube_count: int32 [16], P('space'), may hold values from 1 to 4, as said below
- ln_gain: float32 [1024], replicated, may hold values from 0.25 to 1.75
- ln_bias: float32 [1024], replicated, may hold values from -3 to 3
- w_qkv: bfloat16 [1024, 1536], replicated, may hold values from -1.5 to 1.5
- w_out: bfloat16 [512, 1024], replicated, may hold values from -0.25 to 0.25
Outputs:
- mixed: bfloat16 [64, 304, 1024], P('space', 'frame')
The draws below stay inside these ranges and needn't reach their ends.
Inputs may be any that keep to these rules, and one draw needn't show every extreme that they name: tube_count[s] is how many of the 4 slots of space index s hold visible tubes; they are the first ones. Some index has all 4, some only 1.
All inputs are finite; a program needn't handle non-finite values.
Results may differ from the reference program's by a relative error of at most 0.005.
Values may be sent and summed in bfloat16 or wider, within the bound.
A program may use at most 128 MiB of HBM per device.

```python
import math
import jax
import jax.numpy as jnp
from jax import lax

D = 1024
HEADS = 8
HD = 64
VIS = 4
TIME = 304
SLOTS = 64
N_SPACE = 16


def draw_tokens(key, part):
    noise_key = jax.random.fold_in(jax.random.fold_in(key, 11), 0)
    drawn = jax.random.normal(noise_key, (SLOTS, TIME, D), jnp.float32)
    return jnp.clip(drawn, -16.0, 16.0).astype(jnp.bfloat16)


def draw_w_qkv(key, part):
    first_key = jax.random.fold_in(jax.random.fold_in(key, 23), 0)
    drawn = jax.random.normal(first_key, (D, 3 * HEADS * HD), jnp.float32) / math.sqrt(D)
    return jnp.clip(drawn, -1.5, 1.5).astype(jnp.bfloat16)


def draw_tube_count(key, part):
    first_key, second_key, third_key, fourth_key = jax.random.split(jax.random.fold_in(key, 37), 4)
    many = jax.random.randint(first_key, (N_SPACE,), 2, VIS + 1)
    chosen = jax.random.randint(second_key, (N_SPACE,), 0, 3) == 0
    counts = jnp.where(chosen, many, 1)
    full_at = jax.random.randint(third_key, (), 0, N_SPACE)
    step_by = jax.random.randint(fourth_key, (), 1, N_SPACE)
    sparse_at = (full_at + step_by) % N_SPACE
    index = jnp.arange(N_SPACE)
    counts = jnp.where(index == full_at, VIS, counts)
    counts = jnp.where(index == sparse_at, 1, counts)
    return counts.astype(jnp.int32)


def bell_draw(stream_key, dims, deviation, bound, held_as=jnp.bfloat16):
    values = deviation * jax.random.normal(stream_key, dims, jnp.float32)
    return jnp.clip(values, min=-bound, max=bound).astype(held_as)


def setup_inputs(seed: int = 0) -> dict:
    splits = jax.random.split(jax.random.key(seed), 7)
    return {
        "tokens": draw_tokens(jax.random.fold_in(splits[6], 71), 0),
        "tube_count": draw_tube_count(jax.random.fold_in(splits[6], 71), 0),
        "ln_gain": jnp.clip(1.0 + 0.15 * jax.random.normal(splits[2], (D,), jnp.float32), 0.25, 1.75),
        "ln_bias": bell_draw(splits[3], (D,), 0.5, 3.0, jnp.float32),
        "w_qkv": draw_w_qkv(jax.random.fold_in(splits[6], 71), 0),
        "w_out": bell_draw(splits[5], (HEADS * HD, D), (HEADS * HD) ** -0.5, 0.25),
    }


EPSILON = 1e-06

def layer_norm(flat, ln_gain, ln_bias):
    values32 = flat.astype(jnp.float32)
    center = values32 - lax.optimization_barrier(jnp.mean(values32, axis=-1, keepdims=True))
    spread = lax.optimization_barrier(jnp.mean(center * center, axis=-1, keepdims=True))
    return (center * lax.rsqrt(spread + EPSILON) * ln_gain + ln_bias).astype(jnp.bfloat16)

def reference(tokens, tube_count, ln_gain, ln_bias, w_qkv, w_out):
    slot_total, time_total, width = tokens.shape
    inner = HEADS * HD
    flat = tokens.reshape(slot_total * time_total, width)
    normed = layer_norm(flat, ln_gain, ln_bias)
    projected = jnp.dot(normed, w_qkv, preferred_element_type=jnp.float32).astype(jnp.bfloat16)
    query_all = projected[:, :inner].astype(jnp.float32).reshape(slot_total, time_total, HEADS, HD)
    key_heads = projected[:, inner:2 * inner].astype(jnp.float32).reshape(-1, HEADS, HD)
    value_heads = projected[:, 2 * inner:].astype(jnp.float32).reshape(-1, HEADS, HD)
    slot_index = jnp.arange(slot_total)
    owner = jnp.arange(N_SPACE)
    slot_count = lax.optimization_barrier(jnp.sum(jnp.where(owner[None, :] == (slot_index // VIS)[:, None], tube_count[None, :], 0), axis=1))
    live_slot = (slot_index % VIS < slot_count).astype(jnp.int32)
    live_int = jnp.broadcast_to(live_slot[:, None], (slot_total, time_total)).reshape(-1)
    live_flat = live_int == 1
    scaling = HD ** (-0.5)

    def one_block(query_block):
        scores = jnp.einsum('qhd,khd->hqk', query_block, key_heads) * scaling
        scores = jnp.where(live_flat[None, None, :], scores, -1e+30)
        highest = lax.optimization_barrier(jnp.max(scores, axis=-1, keepdims=True))
        expw = jnp.exp(scores - highest)
        rounded = lax.optimization_barrier(expw.astype(jnp.bfloat16)).astype(jnp.float32)
        summed = jnp.einsum('hqk,khd->hqd', rounded, value_heads)
        result = summed / lax.optimization_barrier(jnp.sum(expw, axis=-1))[..., None]
        return jnp.transpose(result, (1, 0, 2)).reshape(time_total, inner).astype(jnp.bfloat16)
    attended = lax.map(one_block, query_all).reshape(-1, inner)
    mixed = flat.astype(jnp.float32) + jnp.dot(attended, w_out, preferred_element_type=jnp.float32)
    mixed = jnp.where(live_flat[:, None], mixed, 0.0)
    return mixed.astype(jnp.bfloat16).reshape(slot_total, time_total, width)
```

```python
import functools

import jax
import jax.numpy as jnp
from jax import lax
from jax.experimental import pallas as pl
from jax.experimental.pallas import tpu as pltpu
from jax.sharding import PartitionSpec as P

HEADS = 8
HD = 64
SLOT = 40
KB = 256
QB = 512
DEAD = -1e30
EPSILON = 1e-06
SCALE = 1.4426950408889634 / 8.0
ANY = pl.ANY
VMEM = pltpu.VMEM
SMEM = pltpu.SMEM


def spec(space):
    return pl.BlockSpec(memory_space=space)


def place():
    f, s = lax.axis_index("frame"), lax.axis_index("space")
    return f, s, s // 4, s % 4


def remote(src, dst, send, recv, frame, space):
    return pltpu.make_async_remote_copy(
        src_ref=src, dst_ref=dst, send_sem=send, recv_sem=recv,
        device_id={"frame": frame, "space": space}, device_id_type=pl.DeviceIdType.MESH)


def each(lo, hi, body):
    def step(i, c):
        body(i)
        return c
    lax.fori_loop(lo, hi, step, 0)


def project_kernel(tok_ref, cnt_ref, gain_ref, bias_ref, w_ref, q_out, kv_out, cnt_out,
                   w_v, xf, nb, kvs, qs, cnts, kv_in,
                   w_sem, kv_send, kv_recv, q_send, q_recv, c_send, c_recv, x_send, x_recv):
    f, s, x, loc = place()
    slots, times, width = tok_ref.shape
    inner = HEADS * HD

    copies = []
    for n, at in enumerate((inner, 2 * inner, 0)):
        cols = pl.ds(at, inner)
        copy = pltpu.make_async_copy(w_ref.at[:, cols], w_v.at[:, cols], w_sem.at[n])
        copy.start()
        copies.append(copy)

    barrier = pltpu.get_barrier_semaphore()

    def greet(frame, space):
        pl.semaphore_signal(barrier, inc=1, device_id={"frame": frame, "space": space},
                            device_id_type=pl.DeviceIdType.MESH)

    each(1, 32, lambda n: greet((f + n // 4) % 8, x * 4 + (loc + n % 4) % 4))
    each(0, 12, lambda n: greet(f, ((x + 1 + n // 4) % 4) * 4 + n % 4))

    cnts[...] = jnp.full(cnts.shape, cnt_ref[0], jnp.int32)

    for i in range(slots):
        xf[i * SLOT + SLOT - 8:i * SLOT + SLOT, :] = jnp.zeros((8, width), jnp.float32)
        xf[i * SLOT:i * SLOT + times, :] = tok_ref[i].astype(jnp.float32)
    for i in range(slots):
        rows = slice(i * SLOT, i * SLOT + SLOT)
        values = xf[rows, :]
        center = values - jnp.mean(values, axis=-1, keepdims=True)
        spread = jnp.mean(center * center, axis=-1, keepdims=True)
        xf[rows, :] = center * lax.rsqrt(spread + EPSILON) * gain_ref[...] + bias_ref[...]
    nb[...] = xf[...].astype(jnp.bfloat16)

    rows_all = slots * SLOT
    half = rows_all // 2
    low = lax.broadcasted_iota(jnp.int32, (rows_all, 128), 1) < HD
    low_half = lax.broadcasted_iota(jnp.int32, (half, 128), 1) < HD

    copies[0].wait()
    copies[1].wait()
    for g in range(2):
        k4 = jnp.dot(nb[...], w_v[:, inner + 256 * g:inner + 256 * g + 256], preferred_element_type=jnp.float32)
        v4 = jnp.dot(nb[...], w_v[:, 2 * inner + 256 * g:2 * inner + 256 * g + 256],
                     preferred_element_type=jnp.float32)
        for j in range(2):
            k2, v2 = k4[:, 128 * j:128 * j + 128], v4[:, 128 * j:128 * j + 128]
            h = 4 * g + 2 * j
            kvs[h] = jnp.where(low, k2, pltpu.roll(v2, HD, 1)).astype(jnp.bfloat16)
            kvs[h + 1] = jnp.where(low, pltpu.roll(k2, HD, 1), v2).astype(jnp.bfloat16)

    part = f // 2
    source = (f % 2) * 4 + loc
    pl.semaphore_wait(barrier, 43)

    @pl.when(part == loc)
    def _():
        pltpu.make_async_copy(kvs.at[f], kv_in.at[source], kv_recv.at[source]).start()

    @pl.when(part != loc)
    def _():
        remote(kvs.at[f], kv_in.at[source], kv_send.at[0], kv_recv.at[source], f, x * 4 + part).start()

    def kv_copy(d):
        h = (f + d) % 8
        return remote(kvs.at[h], kv_in.at[source], kv_send.at[d], kv_recv.at[source], h, x * 4 + part)

    each(1, 8, lambda d: kv_copy(d).start())

    def count_copy(e):
        return remote(cnts, cnt_out.at[s], c_send.at[e], c_recv.at[s], f, (s + e) % 16)

    each(1, 16, lambda e: count_copy(e).start())
    pltpu.make_async_copy(cnts, cnt_out.at[s], c_recv.at[s]).start()

    copies[2].wait()
    for g in range(2):
        q4 = jnp.dot(nb[...], w_v[:, 256 * g:256 * g + 256], preferred_element_type=jnp.float32) * SCALE
        for j in range(2):
            q2 = q4[:, 128 * j:128 * j + 128]
            h = 4 * g + 2 * j
            qs[h] = jnp.where(low_half, q2[:half], pltpu.roll(q2[half:], HD, 1)).astype(jnp.bfloat16)
            qs[h + 1] = jnp.where(low_half, pltpu.roll(q2[:half], HD, 1), q2[half:]).astype(jnp.bfloat16)

    me = f * 4 + loc

    def q_copy(n):
        h = (f + n // 4) % 8
        return remote(qs.at[h], q_out.at[me], q_send.at[n], q_recv.at[me], h, x * 4 + (loc + n % 4) % 4)

    each(1, 32, lambda n: q_copy(n).start())
    pltpu.make_async_copy(qs.at[f], q_out.at[me], q_recv.at[me]).start()

    def forward(n):
        i, e = n % 8, n // 8 + 1
        return remote(kv_in.at[i], kv_out.at[x * 8 + i], x_send.at[n], x_recv.at[x * 8 + i],
                      f, ((x + e) % 4) * 4 + loc)

    def arrived(i):
        pltpu.make_async_copy(kv_in.at[i], kv_in.at[i], kv_recv.at[i]).wait()
        each(0, 3, lambda e: forward(e * 8 + i).start())
        pltpu.make_async_copy(kv_in.at[i], kv_out.at[x * 8 + i], x_recv.at[x * 8 + i]).start()

    each(0, 8, arrived)

    @pl.when(part != loc)
    def _():
        remote(kvs.at[f], kv_in.at[source], kv_send.at[0], kv_recv.at[source], f, x * 4 + part).wait_send()

    each(1, 8, lambda d: kv_copy(d).wait_send())
    each(1, 16, lambda e: count_copy(e).wait_send())
    each(1, 32, lambda n: q_copy(n).wait_send())
    each(0, 24, lambda n: forward(n).wait_send())
    each(0, 16, lambda n: pltpu.make_async_copy(cnts, cnt_out.at[n], c_recv.at[n]).wait())
    each(0, 32, lambda n: pltpu.make_async_copy(qs.at[0], q_out.at[n], q_recv.at[n]).wait())
    each(0, 32, lambda n: pltpu.make_async_copy(kv_in.at[0], kv_out.at[n], x_recv.at[n]).wait())


def project(tokens, count, gain, bias, w_qkv):
    slots, times, width = tokens.shape
    rows = slots * SLOT
    bf16, i32 = jnp.bfloat16, jnp.int32
    dma = pltpu.SemaphoreType.DMA
    return pl.pallas_call(
        project_kernel,
        out_shape=(jax.ShapeDtypeStruct((32, rows // 2, 128), bf16),
                   jax.ShapeDtypeStruct((32, rows, 128), bf16),
                   jax.ShapeDtypeStruct((16, 1, 128), i32)),
        in_specs=[spec(VMEM), spec(SMEM), spec(VMEM), spec(VMEM), spec(ANY)],
        out_specs=(spec(ANY), spec(ANY), spec(ANY)),
        scratch_shapes=[
            VMEM(w_qkv.shape, bf16), VMEM((rows, width), jnp.float32), VMEM((rows, width), bf16),
            VMEM((HEADS, rows, 128), bf16), VMEM((HEADS, rows // 2, 128), bf16), VMEM((1, 128), i32),
            VMEM((8, rows, 128), bf16),
            dma((3,)), dma((8,)), dma((8,)), dma((32,)), dma((32,)), dma((16,)), dma((16,)),
            dma((24,)), dma((32,)),
        ],
        compiler_params=pltpu.CompilerParams(collective_id=0, has_side_effects=True),
        name="project",
    )(tokens, count, gain, bias, w_qkv)


def attention_kernel(cnt_ref, q_ref, kv_ref, o_ref, kf, vf, kb, vt, qf, qt, of, sa, sb, *, times):
    base = (lax.axis_index("space") // 4) * 4
    sources_q, half_rows = q_ref.shape[0], q_ref.shape[1]
    sources_k, piece = kv_ref.shape[0], kv_ref.shape[1]
    row = lax.broadcasted_iota(jnp.int32, (piece, 128), 0)
    lane = lax.broadcasted_iota(jnp.int32, (piece, 128), 1)
    slot_of = row // SLOT
    empty = row - slot_of * SLOT >= times
    lane_half = lax.broadcasted_iota(jnp.int32, (half_rows, 128), 1)

    def take_keys(i, at):
        count = cnt_ref[(i // 8) * 4 + i % 4, 0, 0]
        values = kv_ref[i].astype(jnp.float32)
        dead = empty | (slot_of >= count)
        keys = jnp.where(lane < HD, values, jnp.where((lane == HD) & dead, DEAD, 0.0))
        here = pl.multiple_of(at, 8)
        kf[pl.ds(here, piece), :] = keys
        vf[pl.ds(here, piece), :] = values
        return at + count * SLOT

    key_rows = lax.fori_loop(0, sources_k, take_keys, jnp.int32(0))
    lane_pad = lax.broadcasted_iota(jnp.int32, (KB, 128), 1)
    here = pl.multiple_of(key_rows, 8)
    kf[pl.ds(here, KB), :] = jnp.where(lane_pad == HD, DEAD, 0.0)
    vf[pl.ds(here, KB), :] = jnp.zeros((KB, 128), jnp.float32)
    key_blocks = (key_rows + KB - 1) // KB

    def take_queries(i, at):
        values = q_ref[i].astype(jnp.float32)
        here = pl.multiple_of(at, 8)
        qf[pl.ds(here, half_rows), :] = values
        there = pl.multiple_of(at + half_rows, 8)
        qf[pl.ds(there, half_rows), :] = pltpu.roll(values, HD, 1)
        return at + cnt_ref[base + i % 4, 0, 0] * SLOT

    query_rows = lax.fori_loop(0, sources_q, take_queries, jnp.int32(0))
    query_tiles = (query_rows + QB - 1) // QB

    ones_row = jnp.where(lax.broadcasted_iota(jnp.int32, (16, KB), 0) == 0, 1.0, 0.0).astype(jnp.bfloat16)

    def shape_keys(b, _):
        rows = pl.ds(pl.multiple_of(b * KB, KB), KB)
        kb[rows, :] = kf[rows, :].astype(jnp.bfloat16)
        turned = jnp.transpose(vf[rows, :])
        vt[b, 0:HD, :] = turned[HD:, :].astype(jnp.bfloat16)
        vt[b, HD:HD + 16, :] = ones_row
        return 0

    lax.fori_loop(0, key_blocks, shape_keys, 0)

    ones_q = jnp.where(lax.broadcasted_iota(jnp.int32, (64, QB), 0) == 0, 1.0, 0.0).astype(jnp.bfloat16)

    def tile(j, _):
        rows = pl.ds(pl.multiple_of(j * QB, QB), QB)
        for part in range(QB // 128):
            turned = jnp.transpose(qf[pl.ds(pl.multiple_of(j * QB + part * 128, 128), 128), :])
            qt[0:HD, part * 128:part * 128 + 128] = turned[0:HD, :].astype(jnp.bfloat16)
        qt[HD:, :] = ones_q

        def product(b, buf):
            keys = kb[pl.ds(pl.multiple_of(b * KB, KB), KB), :]
            scores = jnp.dot(keys, qt[...], preferred_element_type=jnp.float32)
            buf[...] = scores
            return jnp.max(scores, axis=0, keepdims=True)

        def weigh(b, buf, block_best, best, total):
            best_next = jnp.maximum(best, block_best)
            fading = jnp.exp2(best - best_next)
            weights = jnp.exp2(buf[...] - best_next).astype(jnp.bfloat16)
            total = total * fading + jnp.dot(vt[b], weights, preferred_element_type=jnp.float32)
            return best_next, total

        def pair(i, carry):
            best, total, block_best = carry
            other_best = product(2 * i + 1, sb)
            best, total = weigh(2 * i, sa, block_best, best, total)
            block_best = product(2 * i + 2, sa)
            best, total = weigh(2 * i + 1, sb, other_best, best, total)
            return best, total, block_best

        first = product(0, sa)
        best, total, block_best = lax.fori_loop(
            0, key_blocks // 2, pair,
            (jnp.full((1, QB), DEAD, jnp.float32), jnp.zeros((HD + 16, QB), jnp.float32), first),
        )
        best, total = lax.cond(
            key_blocks % 2 == 1,
            lambda: weigh(key_blocks - 1, sa, block_best, best, total),
            lambda: (best, total))
        weight_sum = total[HD:HD + 1, :]
        out = total[0:HD, :] / weight_sum
        lse = best + jnp.log2(weight_sum)
        out = jnp.concatenate([out, jnp.broadcast_to(lse, (64, QB))], axis=0)
        of[rows, :] = jnp.transpose(out)
        return 0

    lax.fori_loop(0, query_tiles, tile, 0)

    row_m = lax.broadcasted_iota(jnp.int32, (128, 128), 0)
    lane_m = lax.broadcasted_iota(jnp.int32, (128, 128), 1)
    eye = row_m == lane_m
    eye_tail = (lax.broadcasted_iota(jnp.int32, (piece - 128, 128), 0)
                == lax.broadcasted_iota(jnp.int32, (piece - 128, 128), 1))
    row16 = lax.broadcasted_iota(jnp.int32, (16, 128), 0)

    def give_back(i, at):
        here = pl.multiple_of(at, 8)
        low = of[pl.ds(here, half_rows), :]
        there = pl.multiple_of(at + half_rows, 8)
        high = of[pl.ds(there, half_rows), :]
        o_ref[i, 0:half_rows, :] = jnp.where(
            lane_half < HD, low, pltpu.roll(high, HD, 1)).astype(jnp.bfloat16)
        wide = jnp.concatenate([low, high], axis=0)
        wide = jnp.where(lane < HD, pltpu.roll(wide, HD, 1), wide)
        head = jnp.sum(jnp.where(eye, wide[0:128], 0.0), axis=0, keepdims=True)
        tail = jnp.sum(jnp.where(eye_tail, wide[128:], 0.0), axis=0, keepdims=True)
        head1 = head.astype(jnp.bfloat16).astype(jnp.float32)
        tail1 = tail.astype(jnp.bfloat16).astype(jnp.float32)
        head2 = (head - head1).astype(jnp.bfloat16).astype(jnp.float32)
        tail2 = (tail - tail1).astype(jnp.bfloat16).astype(jnp.float32)
        parts = (head1, tail1, head2, tail2, head - head1 - head2, tail - tail1 - tail2)
        block = jnp.zeros((16, 128), jnp.float32)
        for n, part in enumerate(parts):
            block = jnp.where(row16 == n, part, block)
        o_ref[i, half_rows:half_rows + 16, :] = block.astype(jnp.bfloat16)
        return at + cnt_ref[base + i % 4, 0, 0] * SLOT

    lax.fori_loop(0, sources_q, give_back, jnp.int32(0))


def attention(counts, q_all, kv_all, times):
    sources_q, half_rows, _ = q_all.shape
    sources_k, piece, _ = kv_all.shape
    q_rows = (sources_q * piece + QB - 1) // QB * QB
    k_rows = (sources_k * piece + KB - 1) // KB * KB
    return pl.pallas_call(
        functools.partial(attention_kernel, times=times),
        out_shape=jax.ShapeDtypeStruct((sources_q, half_rows + 16, 128), jnp.bfloat16),
        in_specs=[spec(SMEM), spec(VMEM), spec(VMEM)],
        out_specs=spec(VMEM),
        scratch_shapes=[
            VMEM((k_rows + KB, 128), jnp.float32),
            VMEM((k_rows + KB, 128), jnp.float32),
            VMEM((k_rows + KB, 128), jnp.bfloat16),
            VMEM((k_rows // KB, HD + 16, KB), jnp.bfloat16),
            VMEM((q_rows + QB, 128), jnp.float32),
            VMEM((128, QB), jnp.bfloat16),
            VMEM((q_rows + QB, 128), jnp.float32),
            VMEM((KB, QB), jnp.float32),
            VMEM((KB, QB), jnp.float32),
        ],
        name="attention",
    )(counts, q_all, kv_all)


def return_kernel(o_ref, back_ref, send, recv):
    f, _, x, loc = place()
    barrier = pltpu.get_barrier_semaphore()

    def greet(n):
        pl.semaphore_signal(
            barrier, inc=1, device_id={"frame": (f + n // 4) % 8, "space": x * 4 + (loc + n % 4) % 4},
            device_id_type=pl.DeviceIdType.MESH)

    each(1, 32, greet)
    me = f * 4 + loc

    def copy(n):
        frame, there = (f + n // 4) % 8, (loc + n % 4) % 4
        return remote(o_ref.at[frame * 4 + there], back_ref.at[me], send.at[n], recv.at[me], frame, x * 4 + there)

    pl.semaphore_wait(barrier, 31)
    each(1, 32, lambda n: copy(n).start())
    pltpu.make_async_copy(o_ref.at[me], back_ref.at[me], recv.at[me]).start()
    each(1, 32, lambda n: copy(n).wait_send())
    each(0, 32, lambda n: pltpu.make_async_copy(o_ref.at[0], back_ref.at[n], recv.at[n]).wait())


def give_results(partial):
    return pl.pallas_call(
        return_kernel,
        out_shape=jax.ShapeDtypeStruct(partial.shape, partial.dtype),
        in_specs=[spec(ANY)],
        out_specs=spec(ANY),
        scratch_shapes=[pltpu.SemaphoreType.DMA((32,)), pltpu.SemaphoreType.DMA((32,))],
        compiler_params=pltpu.CompilerParams(collective_id=1, has_side_effects=True),
        name="give_results",
    )(partial)


def finish_kernel(tok_ref, cnt_ref, back_ref, w_ref, o_ref, lse, att):
    slots, times, width = tok_ref.shape
    half = slots * SLOT // 2
    rows = slots * SLOT
    for h in range(HEADS):
        for p in range(4):
            packed = back_ref[h * 4 + p, half:half + 16, :].astype(jnp.float32)
            whole = packed[0:2] + packed[2:4] + packed[4:6]
            lse[p * 8 + h:p * 8 + h + 1, 0:128] = whole[0:1]
            lse[p * 8 + h:p * 8 + h + 1, 128:256] = whole[1:2]
    sizes = [lse[p * 8:p * 8 + 8, :] for p in range(4)]
    top = jnp.maximum(jnp.maximum(sizes[0], sizes[1]), jnp.maximum(sizes[2], sizes[3]))
    shares = [jnp.exp2(v - top) for v in sizes]
    total = shares[0] + shares[1] + shares[2] + shares[3]
    spread = jnp.concatenate([v / total for v in shares] + [jnp.zeros((96, 256), jnp.float32)], axis=0)
    turned = jnp.transpose(spread)
    low = lax.broadcasted_iota(jnp.int32, (half, 128), 1) < HD

    def merged(h):
        out = jnp.zeros((half, 128), jnp.float32)
        for p in range(4):
            n = p * 8 + h
            share = jnp.where(low, turned[0:half, n:n + 1], turned[half:rows, n:n + 1])
            out = out + back_ref[h * 4 + p, 0:half, :].astype(jnp.float32) * share
        return out

    for j in range(HEADS // 2):
        a, b = merged(2 * j), merged(2 * j + 1)
        cols = slice(128 * j, 128 * j + 128)
        att[0:half, cols] = jnp.where(low, a, pltpu.roll(b, HD, 1)).astype(jnp.bfloat16)
        att[half:rows, cols] = jnp.where(low, pltpu.roll(a, HD, 1), b).astype(jnp.bfloat16)
    mixed = jnp.dot(att[...], w_ref[...], preferred_element_type=jnp.float32)
    for i in range(slots):
        value = tok_ref[i].astype(jnp.float32) + mixed[i * SLOT:i * SLOT + times]
        o_ref[i] = jnp.where(i < cnt_ref[0], value, 0.0).astype(jnp.bfloat16)


def finish(tokens, count, back, w_out):
    rows = tokens.shape[0] * SLOT
    return pl.pallas_call(
        finish_kernel,
        out_shape=jax.ShapeDtypeStruct(tokens.shape, tokens.dtype),
        in_specs=[spec(VMEM), spec(SMEM), spec(VMEM), spec(VMEM)],
        out_specs=spec(VMEM),
        scratch_shapes=[VMEM((32, 256), jnp.float32), VMEM((rows, w_out.shape[0]), jnp.bfloat16)],
        name="finish",
    )(tokens, count, back, w_out)


def on_device(tokens, tube_count, ln_gain, ln_bias, w_qkv, w_out):
    q_all, kv_all, counts = project(
        tokens, tube_count, ln_gain.reshape(1, -1), ln_bias.reshape(1, -1), w_qkv)
    partial = attention(counts, q_all, kv_all, tokens.shape[1])
    return finish(tokens, tube_count, give_results(partial), w_out)


def solution(mesh):
    in_specs = (P("space", "frame", None), P("space"), P(), P(), P(), P())
    return jax.shard_map(
        on_device, mesh=mesh, in_specs=in_specs, out_specs=P("space", "frame", None), check_vma=False)
```

```python
import functools

import jax
import jax.numpy as jnp
from jax import lax
from jax.experimental import pallas as pl
from jax.experimental.pallas import tpu as pltpu
from jax.sharding import PartitionSpec as P

HEADS = 8
HD = 64
SLOT = 40
KB = 256
UN = 8
QB = 512
DEAD = -1e30
Q_AFTER = 2
SAFE = 100.0
EPSILON = 1e-06
SCALE = 1.4426950408889634 / 8.0
ANY = pl.ANY
VMEM = pltpu.VMEM
SMEM = pltpu.SMEM


def spec(space):
    return pl.BlockSpec(memory_space=space)


def place():
    f, s = lax.axis_index("frame"), lax.axis_index("space")
    return f, s, s // 4, s % 4


def remote(src, dst, send, recv, frame, space):
    return pltpu.make_async_remote_copy(
        src_ref=src, dst_ref=dst, send_sem=send, recv_sem=recv,
        device_id={"frame": frame, "space": space}, device_id_type=pl.DeviceIdType.MESH)


def each(lo, hi, body):
    def step(i, c):
        body(i)
        return c
    lax.fori_loop(lo, hi, step, 0)


def project_kernel(tok_ref, cnt_ref, gain_ref, bias_ref, w_ref, q_out, kv_out, cnt_out,
                   w_v, xs, nb, kvs, qs, cnts, kv_all,
                   w_sem, kv_send, kv_recv, q_send, q_recv, c_send, c_recv, x_send, r_send, x_recv, out_sem):
    f, s, x, loc = place()
    times, slots, width = tok_ref.shape
    inner = HEADS * HD

    copies = []
    for n, at in enumerate((inner, 2 * inner, 0)):
        cols = pl.ds(at, inner)
        copy = pltpu.make_async_copy(w_ref.at[:, cols], w_v.at[:, cols], w_sem.at[n])
        copy.start()
        copies.append(copy)

    barrier = pltpu.get_barrier_semaphore()

    def greet(frame, space):
        pl.semaphore_signal(barrier, inc=1, device_id={"frame": frame, "space": space},
                            device_id_type=pl.DeviceIdType.MESH)

    each(1, 32, lambda n: greet((f + n // 4) % 8, x * 4 + (loc + n % 4) % 4))
    each(0, 12, lambda n: greet(f, ((x + 1 + n // 4) % 4) * 4 + n % 4))

    cnts[...] = jnp.full(cnts.shape, cnt_ref[0], jnp.int32)

    for t in range(SLOT):
        values = tok_ref[t % times].astype(jnp.float32)
        for c in range(width // 128):
            xs[c, t * slots:t * slots + slots, :] = values[:, 128 * c:128 * c + 128]
    for i in range(slots):
        values = jnp.concatenate(
            [xs[c, pl.ds(i, SLOT, stride=slots), :] for c in range(width // 128)], axis=1)
        center = values - jnp.mean(values, axis=-1, keepdims=True)
        spread = jnp.mean(center * center, axis=-1, keepdims=True)
        normed = center * lax.rsqrt(spread + EPSILON) * gain_ref[...] + bias_ref[...]
        nb[i * SLOT:i * SLOT + SLOT, :] = normed.astype(jnp.bfloat16)

    rows_all = slots * SLOT
    half = rows_all // 2
    low = lax.broadcasted_iota(jnp.int32, (rows_all, 128), 1) < HD
    low_half = lax.broadcasted_iota(jnp.int32, (half, 128), 1) < HD

    copies[0].wait()
    copies[1].wait()
    for g in range(2):
        k4 = jnp.dot(nb[...], w_v[:, inner + 256 * g:inner + 256 * g + 256], preferred_element_type=jnp.float32)
        v4 = jnp.dot(nb[...], w_v[:, 2 * inner + 256 * g:2 * inner + 256 * g + 256],
                     preferred_element_type=jnp.float32)
        for j in range(2):
            k2, v2 = k4[:, 128 * j:128 * j + 128], v4[:, 128 * j:128 * j + 128]
            h = 4 * g + 2 * j
            kvs[h] = jnp.where(low, k2, pltpu.roll(v2, HD, 1)).astype(jnp.bfloat16)
            kvs[h + 1] = jnp.where(low, pltpu.roll(k2, HD, 1), v2).astype(jnp.bfloat16)

    part = f // 2
    source = x * 8 + (f % 2) * 4 + loc
    mine = (f % 2) * 4 + loc
    pl.semaphore_wait(barrier, 43)

    def kv_copy(d):
        h = (f + d + 2 * loc) % 8
        stays = (h == f) & (part == loc)
        return stays, h, remote(
            kvs.at[h], kv_all.at[source], kv_send.at[d], kv_recv.at[mine], h, x * 4 + part)

    def kv_start(d):
        stays, h, copy = kv_copy(d)

        @pl.when(stays)
        def _():
            pltpu.make_async_copy(kvs.at[h], kv_all.at[source], kv_recv.at[mine]).start()

        @pl.when(jnp.logical_not(stays))
        def _():
            copy.start()

    each(0, 8, kv_start)

    def count_copy(e):
        return remote(cnts, cnt_out.at[s], c_send.at[e], c_recv.at[s], f, (s + e) % 16)

    each(1, 16, lambda e: count_copy(e).start())
    pltpu.make_async_copy(cnts, cnt_out.at[s], c_recv.at[s]).start()

    copies[2].wait()
    for g in range(2):
        q4 = jnp.dot(nb[...], w_v[:, 256 * g:256 * g + 256], preferred_element_type=jnp.float32) * SCALE
        for j in range(2):
            q2 = q4[:, 128 * j:128 * j + 128]
            h = 4 * g + 2 * j
            qs[h] = jnp.where(low_half, q2[:half], pltpu.roll(q2[half:], HD, 1)).astype(jnp.bfloat16)
            qs[h + 1] = jnp.where(low_half, pltpu.roll(q2[:half], HD, 1), q2[half:]).astype(jnp.bfloat16)

    me = f * 4 + loc

    def q_copy(n):
        h = (f + n // 4) % 8
        return remote(qs.at[h], q_out.at[me], q_send.at[n], q_recv.at[me], h, x * 4 + (loc + n % 4) % 4)

    def ring(n, piece, send, step):
        there = (x + step) % 4
        return remote(kv_all.at[piece], kv_all.at[piece], send.at[n], x_recv.at[piece], f, there * 4 + loc)

    def keep(piece):
        return pltpu.make_async_copy(kv_all.at[piece], kv_out.at[piece], out_sem.at[piece])

    def nth(t):
        u = (f - 2 * loc - t + 16) % 8
        return (u % 2) * 4 + u // 2

    right, left, over = ((x + 1) % 4) * 8, ((x + 3) % 4) * 8, ((x + 2) % 4) * 8

    def landed(sem, index, piece):
        pltpu.make_async_copy(kv_all.at[piece], kv_all.at[piece], sem.at[index]).wait()

    def arrived(t):
        i = nth(t)
        piece = x * 8 + i
        landed(kv_recv, i, piece)
        ring(2 * t, piece, x_send, 1).start()
        ring(2 * t + 1, piece, x_send, 3).start()
        keep(piece).start()

    each(0, Q_AFTER, arrived)
    each(1, 32, lambda n: q_copy(n).start())
    pltpu.make_async_copy(qs.at[f], q_out.at[me], q_recv.at[me]).start()
    each(Q_AFTER, 8, arrived)

    def relay(t):
        i = nth(2 * t)
        landed(x_recv, left + i, left + i)
        ring(2 * t, left + i, r_send, 1).start()
        keep(left + i).start()
        i = nth(2 * t + 1)
        landed(x_recv, right + i, right + i)
        ring(2 * t + 1, right + i, r_send, 3).start()
        keep(right + i).start()

    each(0, 4, relay)

    def rest(t):
        i = nth(2 * t + 1)
        landed(x_recv, left + i, left + i)
        keep(left + i).start()
        i = nth(2 * t)
        landed(x_recv, right + i, right + i)
        keep(right + i).start()

    each(0, 4, rest)

    def last(t):
        i = nth(t)
        landed(x_recv, over + i, over + i)
        keep(over + i).start()

    each(0, 8, last)

    def kv_sent(d):
        stays, _, copy = kv_copy(d)

        @pl.when(jnp.logical_not(stays))
        def _():
            copy.wait_send()

    def ring_sent(t):
        piece = x * 8 + nth(t)
        ring(2 * t, piece, x_send, 1).wait_send()
        ring(2 * t + 1, piece, x_send, 3).wait_send()

    def relay_sent(t):
        ring(2 * t, left + nth(2 * t), r_send, 1).wait_send()
        ring(2 * t + 1, right + nth(2 * t + 1), r_send, 3).wait_send()

    each(0, 8, kv_sent)
    each(1, 16, lambda e: count_copy(e).wait_send())
    each(1, 32, lambda n: q_copy(n).wait_send())
    each(0, 8, ring_sent)
    each(0, 4, relay_sent)
    each(0, 16, lambda n: pltpu.make_async_copy(cnts, cnt_out.at[n], c_recv.at[n]).wait())
    each(0, 32, lambda n: pltpu.make_async_copy(qs.at[0], q_out.at[n], q_recv.at[n]).wait())
    each(0, 32, lambda n: keep(n).wait())


def project(tokens, count, gain, bias, w_qkv):
    times, slots, width = tokens.shape
    rows = slots * SLOT
    bf16, i32 = jnp.bfloat16, jnp.int32
    dma = pltpu.SemaphoreType.DMA
    return pl.pallas_call(
        project_kernel,
        out_shape=(jax.ShapeDtypeStruct((32, rows // 2, 128), bf16),
                   jax.ShapeDtypeStruct((32, rows, 128), bf16),
                   jax.ShapeDtypeStruct((16, 1, 128), i32)),
        in_specs=[spec(VMEM), spec(SMEM), spec(VMEM), spec(VMEM), spec(ANY)],
        out_specs=(spec(ANY), spec(ANY), spec(ANY)),
        scratch_shapes=[
            VMEM(w_qkv.shape, bf16), VMEM((width // 128, rows, 128), jnp.float32), VMEM((rows, width), bf16),
            VMEM((HEADS, rows, 128), bf16), VMEM((HEADS, rows // 2, 128), bf16), VMEM((1, 128), i32),
            VMEM((32, rows, 128), bf16),
            dma((3,)), dma((8,)), dma((8,)), dma((32,)), dma((32,)), dma((16,)), dma((16,)),
            dma((16,)), dma((8,)), dma((32,)), dma((32,)),
        ],
        compiler_params=pltpu.CompilerParams(collective_id=0, has_side_effects=True),
        name="project",
    )(tokens, count, gain, bias, w_qkv)


def attention_kernel(cnt_ref, q_hbm, kv_hbm, o_ref, lse_ref, kvc, qc, vt, qt, acc, of, at_q, q_sem, k_sem, *held, times):
    base = (lax.axis_index("space") // 4) * 4
    kv_flat = kvc.reshape(kvc.shape[0] * SLOT, 128)
    q_flat = qc.reshape(qc.shape[0] * SLOT, 128)
    step_keys = KB

    def q_copy(j, l, unit):
        return pltpu.make_async_copy(
            q_hbm.at[:, l, pl.ds((j % 2) * SLOT, SLOT), :], qc.at[pl.ds(unit, 8)], q_sem.at[j * 4 + l])

    def k_copy(xs, l, j, unit):
        return pltpu.make_async_copy(
            kv_hbm.at[xs, :, l, pl.ds(j * SLOT, SLOT), :], kvc.at[pl.ds(unit, 2)], k_sem.at[(xs * 4 + l) * 4 + j])

    def start_keys(n, unit):
        count = cnt_ref[n, 0, 0]
        for j in range(4):
            @pl.when(j < count)
            def _(j=j):
                k_copy(n // 4, n % 4, j, unit + 2 * j).start()
        return unit + 2 * count

    key_units = lax.fori_loop(0, 16, start_keys, jnp.int32(0))
    fill = -(-step_keys // (2 * SLOT))

    def fill_copy(n):
        return pltpu.make_async_copy(
            kv_hbm.at[0, :, 0, pl.ds(0, SLOT), :], kvc.at[pl.ds(key_units + 2 * n, 2)], k_sem.at[64 + n])

    each(0, fill, lambda n: fill_copy(n).start())

    unit = jnp.int32(0)
    for j in range(4):
        if j == 2:
            low_units = unit
        for l in range(4):
            live = j < cnt_ref[base + l, 0, 0]
            at_q[j * 4 + l] = jnp.where(live, unit, 0)

            @pl.when(live)
            def _(j=j, l=l, unit=unit):
                q_copy(j, l, unit).start()
            unit = unit + jnp.where(live, 8, 0)
    query_rows = unit * SLOT
    query_tiles = (query_rows + QB - 1) // QB
    key_rows = key_units * SLOT
    key_steps = (key_rows + step_keys - 1) // step_keys

    def wait_keys(n, c):
        count = cnt_ref[n, 0, 0]
        for j in range(4):
            @pl.when(j < count)
            def _(j=j):
                k_copy(n // 4, n % 4, j, 0).wait()
        return c

    lax.fori_loop(0, 16, wait_keys, 0)
    each(0, fill, lambda n: fill_copy(n).wait())

    key_at = lax.broadcasted_iota(jnp.int32, (HD, KB), 1)
    row16 = lax.broadcasted_iota(jnp.int32, (16, KB), 0)

    def shape_keys(b, longest):
        turned = jnp.transpose(kv_flat[pl.ds(pl.multiple_of(b * KB, KB), KB), :].astype(jnp.float32))
        index = key_at + b * KB
        live = (index % SLOT < times) & (index < key_rows)
        vt[b, 0:HD, :] = jnp.where(live, turned[HD:], 0.0).astype(jnp.bfloat16)
        vt[b, HD:HD + 16, :] = jnp.where(live[:16] & (row16 == 0), 1.0, 0.0).astype(jnp.bfloat16)
        keys = turned[:HD]
        return jnp.maximum(longest, jnp.sum(keys * keys, axis=0, keepdims=True))

    longest_key = lax.fori_loop(0, key_steps, shape_keys, jnp.zeros((1, KB), jnp.float32))

    for j in range(4):
        for l in range(4):
            @pl.when(j < cnt_ref[base + l, 0, 0])
            def _(j=j, l=l):
                q_copy(j, l, 0).wait()

    col = lax.broadcasted_iota(jnp.int32, (HD, QB), 1)
    low_rows = low_units * SLOT

    def shape_queries(t, longest):
        turned = jnp.transpose(q_flat[pl.ds(pl.multiple_of(t * QB, QB), QB), :].astype(jnp.float32))
        index = col + t * QB
        query = jnp.where(index < low_rows, turned[:HD], turned[HD:])
        query = jnp.where(index < query_rows, query, 0.0)
        qt[t, 0:HD, :] = query.astype(jnp.bfloat16)
        qt[t, HD:, :] = jnp.zeros((HD, QB), jnp.bfloat16)
        return jnp.maximum(longest, jnp.sum(query * query, axis=0, keepdims=True))

    longest_query = lax.fori_loop(0, query_tiles, shape_queries, jnp.zeros((1, QB), jnp.float32))
    safe = jnp.max(longest_key) * jnp.max(longest_query) < SAFE * SAFE

    def put(t, total, best):
        weight_sum = total[HD:HD + 1, :]
        out = total[0:HD, :] / weight_sum
        lse = jnp.broadcast_to(best + jnp.log2(weight_sum), (HD, QB))
        low = col + t * QB < low_rows
        both = jnp.concatenate([jnp.where(low, out, lse), jnp.where(low, lse, out)], axis=0)
        of[pl.ds(pl.multiple_of(t * QB, QB), QB), :] = jnp.transpose(both)

    def block_scores(b, t):
        keys = kv_flat[pl.ds(pl.multiple_of(b * KB, KB), KB), :]
        return jnp.dot(keys, qt[t], preferred_element_type=jnp.float32)

    def clear(t):
        acc[t] = jnp.zeros((HD + 16, QB), jnp.float32)

    def after(item):
        t, b = item
        turn = b + 1 == key_steps
        return jnp.minimum(jnp.where(turn, t + 1, t), query_tiles), jnp.where(turn, 0, b + 1)

    def plain(i, carry):
        before, now = carry
        then = now[-1]
        later = []
        for u in range(UN):
            t, b = before[u]
            acc[t] += jnp.dot(vt[b], held[u][...], preferred_element_type=jnp.float32)
            t, b = now[u]
            held[u][...] = jnp.exp2(block_scores(b, t)).astype(jnp.bfloat16)
            then = after(then)
            later.append(then)
        return now, tuple(later)

    def plain_all():
        each(0, query_tiles, clear)
        first = [(jnp.int32(0), jnp.int32(0))]
        for _ in range(UN - 1):
            first.append(after(first[-1]))
        nowhere = ((query_tiles, jnp.int32(0)),) * UN
        steps = (query_tiles * key_steps + UN - 1) // UN + 1
        lax.fori_loop(0, steps, plain, (nowhere, tuple(first)))

        each(0, query_tiles, lambda t: put(t, acc[t], 0.0))

    def shifted_tile(t):
        def step(b, carry):
            best, total = carry
            scores = block_scores(b, t)
            best_next = jnp.maximum(best, jnp.max(scores, axis=0, keepdims=True))
            weights = jnp.exp2(scores - best_next).astype(jnp.bfloat16)
            total = total * jnp.exp2(best - best_next) + jnp.dot(
                vt[b], weights, preferred_element_type=jnp.float32)
            return best_next, total

        best, total = lax.fori_loop(
            0, key_steps, step,
            (jnp.full((1, QB), DEAD, jnp.float32), jnp.zeros((HD + 16, QB), jnp.float32)))
        put(t, total, best)

    @pl.when(safe)
    def _():
        plain_all()

    @pl.when(jnp.logical_not(safe))
    def _():
        each(0, query_tiles, shifted_tile)

    lane = lax.broadcasted_iota(jnp.int32, (SLOT, 128), 1)
    in_low = lane < HD

    def give_back(i, sizes):
        f, l = i // 4, i % 4
        sizes_next = []
        for j in range(2):
            first = of[pl.ds(pl.multiple_of((at_q[j * 4 + l] + f) * SLOT, 8), SLOT), :]
            second = of[pl.ds(pl.multiple_of((at_q[j * 4 + 8 + l] + f) * SLOT, 8), SLOT), :]
            o_ref[i, j * SLOT:j * SLOT + SLOT, :] = jnp.where(in_low, first, second).astype(jnp.bfloat16)
            sizes_next.append(jnp.where(lane % HD == i, jnp.where(in_low, second, first), sizes[j]))
        return tuple(sizes_next)

    sizes = lax.fori_loop(0, 32, give_back, (jnp.zeros((SLOT, 128), jnp.float32),) * 2)
    turned = jnp.transpose(jnp.concatenate([*sizes, jnp.zeros((128 - 2 * SLOT, 128), jnp.float32)], axis=0))
    for i in range(32):
        lse_ref[i, 0:1, :] = turned[HD + i:HD + i + 1]
        lse_ref[i, 1:2, :] = turned[i:i + 1]


def attention(counts, q_all, kv_all, times):
    sources, half_rows, _ = q_all.shape
    q_units, k_units = 4 * sources, 4 * sources
    q_rows = (q_units * SLOT + QB - 1) // QB * QB
    step = KB
    k_rows = (k_units * SLOT + step - 1) // step * step
    fill = -(-step // (2 * SLOT))
    dma = pltpu.SemaphoreType.DMA
    return pl.pallas_call(
        functools.partial(attention_kernel, times=times),
        out_shape=(jax.ShapeDtypeStruct((sources, half_rows, 128), jnp.bfloat16),
                   jax.ShapeDtypeStruct((sources, 2, 128), jnp.float32)),
        in_specs=[spec(SMEM), spec(ANY), spec(ANY)],
        out_specs=(spec(VMEM), spec(VMEM)),
        scratch_shapes=[
            VMEM((k_units + 2 * fill, SLOT, 128), jnp.bfloat16),
            VMEM((q_rows // SLOT + 1, SLOT, 128), jnp.bfloat16),
            VMEM((k_rows // KB, HD + 16, KB), jnp.bfloat16),
            VMEM((q_rows // QB + 1, 128, QB), jnp.bfloat16),
            VMEM((q_rows // QB + 1, HD + 16, QB), jnp.float32),
            VMEM((q_rows, 128), jnp.float32),
            SMEM((16,), jnp.int32),
            dma((16,)), dma((64 + fill,)),
            *[VMEM((KB, QB), jnp.bfloat16) for _ in range(UN)],
        ],
        name="attention",
    )(counts, q_all.reshape(8, 4, half_rows, 128), kv_all.reshape(4, 2, 4, 2 * half_rows, 128))


def return_kernel(o_ref, lse_ref, back_ref, back_lse, o_send, o_recv, l_send, l_recv):
    f, _, x, loc = place()
    barrier = pltpu.get_barrier_semaphore()

    def greet(n):
        pl.semaphore_signal(
            barrier, inc=1, device_id={"frame": (f + n // 4) % 8, "space": x * 4 + (loc + n % 4) % 4},
            device_id_type=pl.DeviceIdType.MESH)

    each(1, 32, greet)
    me = loc * 8 + f

    def copies(n):
        frame, there = (f + n // 4) % 8, (loc + n % 4) % 4
        source = frame * 4 + there
        return (remote(o_ref.at[source], back_ref.at[me], o_send.at[n], o_recv.at[me], frame, x * 4 + there),
                remote(lse_ref.at[source], back_lse.at[me], l_send.at[n], l_recv.at[me], frame, x * 4 + there))

    def start(n):
        for copy in copies(n):
            copy.start()

    def sent(n):
        for copy in copies(n):
            copy.wait_send()

    pl.semaphore_wait(barrier, 31)
    each(1, 32, start)
    own = f * 4 + loc
    pltpu.make_async_copy(o_ref.at[own], back_ref.at[me], o_recv.at[me]).start()
    pltpu.make_async_copy(lse_ref.at[own], back_lse.at[me], l_recv.at[me]).start()
    each(1, 32, sent)
    each(0, 32, lambda n: pltpu.make_async_copy(o_ref.at[0], back_ref.at[n], o_recv.at[n]).wait())
    each(0, 32, lambda n: pltpu.make_async_copy(lse_ref.at[0], back_lse.at[n], l_recv.at[n]).wait())


def give_results(partial, sizes):
    dma = pltpu.SemaphoreType.DMA
    return pl.pallas_call(
        return_kernel,
        out_shape=(jax.ShapeDtypeStruct(partial.shape, partial.dtype),
                   jax.ShapeDtypeStruct(sizes.shape, sizes.dtype)),
        in_specs=[spec(ANY), spec(ANY)],
        out_specs=(spec(ANY), spec(ANY)),
        scratch_shapes=[dma((32,)), dma((32,)), dma((32,)), dma((32,))],
        compiler_params=pltpu.CompilerParams(collective_id=1, has_side_effects=True),
        name="give_results",
    )(partial, sizes)


def finish_kernel(tok_ref, cnt_ref, back_ref, lse_ref, w_ref, o_ref, att, ys):
    times, slots, width = tok_ref.shape
    half = slots * SLOT // 2
    rows = slots * SLOT

    def shares(n):
        sizes = [lse_ref[p * 8:p * 8 + 8, n, :] for p in range(4)]
        top = jnp.maximum(jnp.maximum(sizes[0], sizes[1]), jnp.maximum(sizes[2], sizes[3]))
        powers = [jnp.exp2(v - top) for v in sizes]
        total = powers[0] + powers[1] + powers[2] + powers[3]
        return jnp.transpose(
            jnp.concatenate([v / total for v in powers] + [jnp.zeros((96, 128), jnp.float32)], axis=0))

    first, second = shares(0), shares(1)
    low = lax.broadcasted_iota(jnp.int32, (half, 128), 1) < HD

    def merged(h):
        out = jnp.zeros((half, 128), jnp.float32)
        for p in range(4):
            n = p * 8 + h
            share = jnp.where(low, first[0:half, n:n + 1], second[0:half, n:n + 1])
            out = out + back_ref[n].astype(jnp.float32) * share
        return out

    for j in range(HEADS // 2):
        a, b = merged(2 * j), merged(2 * j + 1)
        cols = slice(128 * j, 128 * j + 128)
        att[0:half, cols] = jnp.where(low, a, pltpu.roll(b, HD, 1)).astype(jnp.bfloat16)
        att[half:rows, cols] = jnp.where(low, pltpu.roll(a, HD, 1), b).astype(jnp.bfloat16)
    for c in range(width // 256):
        cols = slice(256 * c, 256 * c + 256)
        mixed = jnp.dot(att[...], w_ref[:, cols], preferred_element_type=jnp.float32)
        for i in range(slots):
            for e in range(2):
                ys[2 * c + e, pl.ds(i, SLOT, stride=slots), :] = (
                    mixed[i * SLOT:i * SLOT + SLOT, 128 * e:128 * e + 128])
    live = lax.broadcasted_iota(jnp.int32, (slots, width), 0) < cnt_ref[0]
    for t in range(times):
        mixed = jnp.concatenate([ys[c, t * slots:t * slots + slots, :] for c in range(width // 128)], axis=1)
        value = tok_ref[t].astype(jnp.float32) + mixed
        o_ref[t] = jnp.where(live, value, 0.0).astype(jnp.bfloat16)


def finish(tokens, count, back, sizes, w_out):
    times, slots, width = tokens.shape
    rows = slots * SLOT
    return pl.pallas_call(
        finish_kernel,
        out_shape=jax.ShapeDtypeStruct(tokens.shape, tokens.dtype),
        in_specs=[spec(VMEM), spec(SMEM), spec(VMEM), spec(VMEM), spec(VMEM)],
        out_specs=spec(VMEM),
        scratch_shapes=[VMEM((rows, w_out.shape[0]), jnp.bfloat16), VMEM((width // 128, rows, 128), jnp.float32)],
        name="finish",
    )(tokens, count, back, sizes, w_out)


def on_device(tokens, tube_count, ln_gain, ln_bias, w_qkv, w_out):
    tokens = jnp.transpose(tokens, (1, 0, 2))
    q_all, kv_all, counts = project(
        tokens, tube_count, ln_gain.reshape(1, -1), ln_bias.reshape(1, -1), w_qkv)
    partial, sizes = attention(counts, q_all, kv_all, tokens.shape[0])
    mixed = finish(tokens, tube_count, *give_results(partial, sizes), w_out)
    return jnp.transpose(mixed, (1, 0, 2))


def solution(mesh):
    in_specs = (P("space", "frame", None), P("space"), P(), P(), P(), P())
    return jax.shard_map(
        on_device, mesh=mesh, in_specs=in_specs, out_specs=P("space", "frame", None), check_vma=False)
```

```python
import functools

import jax
import jax.numpy as jnp
from jax import lax
from jax.experimental import pallas as pl
from jax.experimental.pallas import tpu as pltpu
from jax.sharding import PartitionSpec as P

HEADS = 8
HD = 64
SLOT = 40
KB = 256
UN = 8
QB = 512
DEAD = -1e30
Q_AFTER = 2
SAFE = 100.0
EPSILON = 1e-06
SCALE = 1.4426950408889634 / 8.0
ANY = pl.ANY
VMEM = pltpu.VMEM
SMEM = pltpu.SMEM


def spec(space):
    return pl.BlockSpec(memory_space=space)


def place():
    f, s = lax.axis_index("frame"), lax.axis_index("space")
    return f, s, s // 4, s % 4


def remote(src, dst, send, recv, frame, space):
    return pltpu.make_async_remote_copy(
        src_ref=src, dst_ref=dst, send_sem=send, recv_sem=recv,
        device_id={"frame": frame, "space": space}, device_id_type=pl.DeviceIdType.MESH)


def each(lo, hi, body):
    def step(i, c):
        body(i)
        return c
    lax.fori_loop(lo, hi, step, 0)


def project_kernel(tok_ref, cnt_ref, gain_ref, bias_ref, w_ref, q_out, kv_out, cnt_out,
                   w_v, xs, nb, kvs, qs, cnts, kv_all,
                   w_sem, kv_send, kv_recv, q_send, q_recv, c_send, c_recv, x_send, r_send, x_recv, out_sem):
    f, s, x, loc = place()
    times, slots, width = tok_ref.shape
    inner = HEADS * HD

    copies = []
    for n, at in enumerate((inner, 2 * inner, 0)):
        cols = pl.ds(at, inner)
        copy = pltpu.make_async_copy(w_ref.at[:, cols], w_v.at[:, cols], w_sem.at[n])
        copy.start()
        copies.append(copy)

    barrier = pltpu.get_barrier_semaphore()

    def greet(frame, space):
        pl.semaphore_signal(barrier, inc=1, device_id={"frame": frame, "space": space},
                            device_id_type=pl.DeviceIdType.MESH)

    each(1, 32, lambda n: greet((f + n // 4) % 8, x * 4 + (loc + n % 4) % 4))
    each(0, 12, lambda n: greet(f, ((x + 1 + n // 4) % 4) * 4 + n % 4))

    cnts[...] = jnp.full(cnts.shape, cnt_ref[0], jnp.int32)

    for t in range(SLOT):
        values = tok_ref[t % times].astype(jnp.float32)
        for c in range(width // 128):
            xs[c, t * slots:t * slots + slots, :] = values[:, 128 * c:128 * c + 128]
    for i in range(slots):
        values = jnp.concatenate(
            [xs[c, pl.ds(i, SLOT, stride=slots), :] for c in range(width // 128)], axis=1)
        center = values - jnp.mean(values, axis=-1, keepdims=True)
        spread = jnp.mean(center * center, axis=-1, keepdims=True)
        normed = center * lax.rsqrt(spread + EPSILON) * gain_ref[...] + bias_ref[...]
        nb[i * SLOT:i * SLOT + SLOT, :] = normed.astype(jnp.bfloat16)

    rows_all = slots * SLOT
    half = rows_all // 2
    low = lax.broadcasted_iota(jnp.int32, (rows_all, 128), 1) < HD
    low_half = lax.broadcasted_iota(jnp.int32, (half, 128), 1) < HD

    copies[0].wait()
    copies[1].wait()
    for g in range(2):
        k4 = jnp.dot(nb[...], w_v[:, inner + 256 * g:inner + 256 * g + 256], preferred_element_type=jnp.float32)
        v4 = jnp.dot(nb[...], w_v[:, 2 * inner + 256 * g:2 * inner + 256 * g + 256],
                     preferred_element_type=jnp.float32)
        for j in range(2):
            k2, v2 = k4[:, 128 * j:128 * j + 128], v4[:, 128 * j:128 * j + 128]
            h = 4 * g + 2 * j
            kvs[h] = jnp.where(low, k2, pltpu.roll(v2, HD, 1)).astype(jnp.bfloat16)
            kvs[h + 1] = jnp.where(low, pltpu.roll(k2, HD, 1), v2).astype(jnp.bfloat16)

    part = f // 2
    source = x * 8 + (f % 2) * 4 + loc
    mine = (f % 2) * 4 + loc
    pl.semaphore_wait(barrier, 43)

    def kv_copy(d):
        h = (f + d + 2 * loc) % 8
        stays = (h == f) & (part == loc)
        return stays, h, remote(
            kvs.at[h], kv_all.at[source], kv_send.at[d], kv_recv.at[mine], h, x * 4 + part)

    def kv_start(d):
        stays, h, copy = kv_copy(d)

        @pl.when(stays)
        def _():
            pltpu.make_async_copy(kvs.at[h], kv_all.at[source], kv_recv.at[mine]).start()

        @pl.when(jnp.logical_not(stays))
        def _():
            copy.start()

    each(0, 8, kv_start)

    def count_copy(e):
        return remote(cnts, cnt_out.at[s], c_send.at[e], c_recv.at[s], f, (s + e) % 16)

    each(1, 16, lambda e: count_copy(e).start())
    pltpu.make_async_copy(cnts, cnt_out.at[s], c_recv.at[s]).start()

    copies[2].wait()
    for g in range(2):
        q4 = jnp.dot(nb[...], w_v[:, 256 * g:256 * g + 256], preferred_element_type=jnp.float32) * SCALE
        for j in range(2):
            q2 = q4[:, 128 * j:128 * j + 128]
            h = 4 * g + 2 * j
            qs[h] = jnp.where(low_half, q2[:half], pltpu.roll(q2[half:], HD, 1)).astype(jnp.bfloat16)
            qs[h + 1] = jnp.where(low_half, pltpu.roll(q2[:half], HD, 1), q2[half:]).astype(jnp.bfloat16)

    me = f * 4 + loc

    def q_copy(n):
        h = (f + n // 4) % 8
        return remote(qs.at[h], q_out.at[me], q_send.at[n], q_recv.at[me], h, x * 4 + (loc + n % 4) % 4)

    def ring(n, piece, send, step):
        there = (x + step) % 4
        return remote(kv_all.at[piece], kv_all.at[piece], send.at[n], x_recv.at[piece], f, there * 4 + loc)

    def keep(piece):
        return pltpu.make_async_copy(kv_all.at[piece], kv_out.at[piece], out_sem.at[piece])

    def nth(t):
        u = (f - 2 * loc - t + 16) % 8
        return (u % 2) * 4 + u // 2

    right, left, over = ((x + 1) % 4) * 8, ((x + 3) % 4) * 8, ((x + 2) % 4) * 8

    def landed(sem, index, piece):
        pltpu.make_async_copy(kv_all.at[piece], kv_all.at[piece], sem.at[index]).wait()

    def arrived(t):
        i = nth(t)
        piece = x * 8 + i
        landed(kv_recv, i, piece)
        ring(2 * t, piece, x_send, 1).start()
        ring(2 * t + 1, piece, x_send, 3).start()
        keep(piece).start()

    each(0, Q_AFTER, arrived)
    each(1, 32, lambda n: q_copy(n).start())
    pltpu.make_async_copy(qs.at[f], q_out.at[me], q_recv.at[me]).start()
    each(Q_AFTER, 8, arrived)

    def relay(t):
        i = nth(2 * t)
        landed(x_recv, left + i, left + i)
        ring(2 * t, left + i, r_send, 1).start()
        keep(left + i).start()
        i = nth(2 * t + 1)
        landed(x_recv, right + i, right + i)
        ring(2 * t + 1, right + i, r_send, 3).start()
        keep(right + i).start()

    each(0, 4, relay)

    def rest(t):
        i = nth(2 * t + 1)
        landed(x_recv, left + i, left + i)
        keep(left + i).start()
        i = nth(2 * t)
        landed(x_recv, right + i, right + i)
        keep(right + i).start()

    each(0, 4, rest)

    def last(t):
        i = nth(t)
        landed(x_recv, over + i, over + i)
        keep(over + i).start()

    each(0, 8, last)

    def kv_sent(d):
        stays, _, copy = kv_copy(d)

        @pl.when(jnp.logical_not(stays))
        def _():
            copy.wait_send()

    def ring_sent(t):
        piece = x * 8 + nth(t)
        ring(2 * t, piece, x_send, 1).wait_send()
        ring(2 * t + 1, piece, x_send, 3).wait_send()

    def relay_sent(t):
        ring(2 * t, left + nth(2 * t), r_send, 1).wait_send()
        ring(2 * t + 1, right + nth(2 * t + 1), r_send, 3).wait_send()

    each(0, 8, kv_sent)
    each(1, 16, lambda e: count_copy(e).wait_send())
    each(1, 32, lambda n: q_copy(n).wait_send())
    each(0, 8, ring_sent)
    each(0, 4, relay_sent)
    each(0, 16, lambda n: pltpu.make_async_copy(cnts, cnt_out.at[n], c_recv.at[n]).wait())
    each(0, 32, lambda n: pltpu.make_async_copy(qs.at[0], q_out.at[n], q_recv.at[n]).wait())
    each(0, 32, lambda n: keep(n).wait())


def project(tokens, count, gain, bias, w_qkv):
    times, slots, width = tokens.shape
    rows = slots * SLOT
    bf16, i32 = jnp.bfloat16, jnp.int32
    dma = pltpu.SemaphoreType.DMA
    return pl.pallas_call(
        project_kernel,
        out_shape=(jax.ShapeDtypeStruct((32, rows // 2, 128), bf16),
                   jax.ShapeDtypeStruct((32, rows, 128), bf16),
                   jax.ShapeDtypeStruct((16, 1, 128), i32)),
        in_specs=[spec(VMEM), spec(SMEM), spec(VMEM), spec(VMEM), spec(ANY)],
        out_specs=(spec(ANY), spec(ANY), spec(ANY)),
        scratch_shapes=[
            VMEM(w_qkv.shape, bf16), VMEM((width // 128, rows, 128), jnp.float32), VMEM((rows, width), bf16),
            VMEM((HEADS, rows, 128), bf16), VMEM((HEADS, rows // 2, 128), bf16), VMEM((1, 128), i32),
            VMEM((32, rows, 128), bf16),
            dma((3,)), dma((8,)), dma((8,)), dma((32,)), dma((32,)), dma((16,)), dma((16,)),
            dma((16,)), dma((8,)), dma((32,)), dma((32,)),
        ],
        compiler_params=pltpu.CompilerParams(collective_id=0, has_side_effects=True),
        name="project",
    )(tokens, count, gain, bias, w_qkv)


def attention_kernel(cnt_ref, q_hbm, kv_hbm, o_ref, lse_ref, kvc, qc, vt, qt, acc, of, at_q, q_sem, k_sem, *held, times):
    base = (lax.axis_index("space") // 4) * 4
    kv_flat = kvc.reshape(kvc.shape[0] * SLOT, 128)
    q_flat = qc.reshape(qc.shape[0] * SLOT, 128)
    step_keys = KB

    def q_copy(j, l, unit):
        return pltpu.make_async_copy(
            q_hbm.at[:, l, pl.ds((j % 2) * SLOT, SLOT), :], qc.at[pl.ds(unit, 8)], q_sem.at[j * 4 + l])

    def k_copy(xs, l, j, unit):
        return pltpu.make_async_copy(
            kv_hbm.at[xs, :, l, pl.ds(j * SLOT, SLOT), :], kvc.at[pl.ds(unit, 2)], k_sem.at[(xs * 4 + l) * 4 + j])

    def start_keys(n, unit):
        count = cnt_ref[n, 0, 0]
        for j in range(4):
            @pl.when(j < count)
            def _(j=j):
                k_copy(n // 4, n % 4, j, unit + 2 * j).start()
        return unit + 2 * count

    key_units = lax.fori_loop(0, 16, start_keys, jnp.int32(0))
    fill = -(-step_keys // (2 * SLOT))

    def fill_copy(n):
        return pltpu.make_async_copy(
            kv_hbm.at[0, :, 0, pl.ds(0, SLOT), :], kvc.at[pl.ds(key_units + 2 * n, 2)], k_sem.at[64 + n])

    each(0, fill, lambda n: fill_copy(n).start())

    unit = jnp.int32(0)
    for j in range(4):
        if j == 2:
            low_units = unit
        for l in range(4):
            live = j < cnt_ref[base + l, 0, 0]
            at_q[j * 4 + l] = jnp.where(live, unit, 0)

            @pl.when(live)
            def _(j=j, l=l, unit=unit):
                q_copy(j, l, unit).start()
            unit = unit + jnp.where(live, 8, 0)
    query_rows = unit * SLOT
    query_tiles = (query_rows + QB - 1) // QB
    key_rows = key_units * SLOT
    key_steps = (key_rows + step_keys - 1) // step_keys

    def wait_keys(n, c):
        count = cnt_ref[n, 0, 0]
        for j in range(4):
            @pl.when(j < count)
            def _(j=j):
                k_copy(n // 4, n % 4, j, 0).wait()
        return c

    lax.fori_loop(0, 16, wait_keys, 0)
    each(0, fill, lambda n: fill_copy(n).wait())

    key_at = lax.broadcasted_iota(jnp.int32, (HD, KB), 1)
    row16 = lax.broadcasted_iota(jnp.int32, (16, KB), 0)

    def shape_keys(b, longest):
        turned = jnp.transpose(kv_flat[pl.ds(pl.multiple_of(b * KB, KB), KB), :].astype(jnp.float32))
        index = key_at + b * KB
        live = (index % SLOT < times) & (index < key_rows)
        vt[b, 0:HD, :] = jnp.where(live, turned[HD:], 0.0).astype(jnp.bfloat16)
        vt[b, HD:HD + 16, :] = jnp.where(live[:16] & (row16 == 0), 1.0, 0.0).astype(jnp.bfloat16)
        keys = turned[:HD]
        return jnp.maximum(longest, jnp.sum(keys * keys, axis=0, keepdims=True))

    longest_key = lax.fori_loop(0, key_steps, shape_keys, jnp.zeros((1, KB), jnp.float32))

    for j in range(4):
        for l in range(4):
            @pl.when(j < cnt_ref[base + l, 0, 0])
            def _(j=j, l=l):
                q_copy(j, l, 0).wait()

    col = lax.broadcasted_iota(jnp.int32, (HD, QB), 1)
    low_rows = low_units * SLOT

    def shape_queries(t, longest):
        turned = jnp.transpose(q_flat[pl.ds(pl.multiple_of(t * QB, QB), QB), :].astype(jnp.float32))
        index = col + t * QB
        query = jnp.where(index < low_rows, turned[:HD], turned[HD:])
        query = jnp.where(index < query_rows, query, 0.0)
        qt[t, 0:HD, :] = query.astype(jnp.bfloat16)
        qt[t, HD:, :] = jnp.zeros((HD, QB), jnp.bfloat16)
        return jnp.maximum(longest, jnp.sum(query * query, axis=0, keepdims=True))

    longest_query = lax.fori_loop(0, query_tiles, shape_queries, jnp.zeros((1, QB), jnp.float32))
    safe = jnp.max(longest_key) * jnp.max(longest_query) < SAFE * SAFE

    def put(t, total, best):
        weight_sum = total[HD:HD + 1, :]
        out = total[0:HD, :] / weight_sum
        lse = jnp.broadcast_to(best + jnp.log2(weight_sum), (HD, QB))
        low = col + t * QB < low_rows
        both = jnp.concatenate([jnp.where(low, out, lse), jnp.where(low, lse, out)], axis=0)
        of[pl.ds(pl.multiple_of(t * QB, QB), QB), :] = jnp.transpose(both)

    def block_scores(b, t):
        keys = kv_flat[pl.ds(pl.multiple_of(b * KB, KB), KB), :]
        return jnp.dot(keys, qt[t], preferred_element_type=jnp.float32)

    def clear(t):
        acc[t] = jnp.zeros((HD + 16, QB), jnp.float32)

    def after(item):
        t, b = item
        turn = b + 1 == key_steps
        return jnp.minimum(jnp.where(turn, t + 1, t), query_tiles), jnp.where(turn, 0, b + 1)

    def plain(i, carry):
        before, now = carry
        then = now[-1]
        later = []
        for u in range(UN):
            t, b = before[u]
            acc[t] += jnp.dot(vt[b], held[u][...], preferred_element_type=jnp.float32)
            t, b = now[u]
            held[u][...] = jnp.exp2(block_scores(b, t)).astype(jnp.bfloat16)
            then = after(then)
            later.append(then)
        return now, tuple(later)

    def plain_all():
        each(0, query_tiles, clear)
        first = [(jnp.int32(0), jnp.int32(0))]
        for _ in range(UN - 1):
            first.append(after(first[-1]))
        nowhere = ((query_tiles, jnp.int32(0)),) * UN
        steps = (query_tiles * key_steps + UN - 1) // UN + 1
        lax.fori_loop(0, steps, plain, (nowhere, tuple(first)))

        each(0, query_tiles, lambda t: put(t, acc[t], 0.0))

    def shifted_tile(t):
        def step(b, carry):
            best, total = carry
            scores = block_scores(b, t)
            best_next = jnp.maximum(best, jnp.max(scores, axis=0, keepdims=True))
            weights = jnp.exp2(scores - best_next).astype(jnp.bfloat16)
            total = total * jnp.exp2(best - best_next) + jnp.dot(
                vt[b], weights, preferred_element_type=jnp.float32)
            return best_next, total

        best, total = lax.fori_loop(
            0, key_steps, step,
            (jnp.full((1, QB), DEAD, jnp.float32), jnp.zeros((HD + 16, QB), jnp.float32)))
        put(t, total, best)

    @pl.when(safe)
    def _():
        plain_all()

    @pl.when(jnp.logical_not(safe))
    def _():
        each(0, query_tiles, shifted_tile)

    lane = lax.broadcasted_iota(jnp.int32, (SLOT, 128), 1)
    in_low = lane < HD

    def give_back(i, sizes):
        f, l = i % 8, ((i // 8) % 2) * 2 + i // 16
        sizes_next = []
        for j in range(2):
            first = of[pl.ds(pl.multiple_of((at_q[j * 4 + l] + f) * SLOT, 8), SLOT), :]
            second = of[pl.ds(pl.multiple_of((at_q[j * 4 + 8 + l] + f) * SLOT, 8), SLOT), :]
            o_ref[i, j * SLOT:j * SLOT + SLOT, :] = jnp.where(in_low, first, second).astype(jnp.bfloat16)
            sizes_next.append(jnp.where(lane % HD == i, jnp.where(in_low, second, first), sizes[j]))
        return tuple(sizes_next)

    sizes = lax.fori_loop(0, 32, give_back, (jnp.zeros((SLOT, 128), jnp.float32),) * 2)
    turned = jnp.transpose(jnp.concatenate([*sizes, jnp.zeros((128 - 2 * SLOT, 128), jnp.float32)], axis=0))
    lse_ref[0] = turned[HD:HD + 32]
    lse_ref[1] = turned[0:32]


def attention(counts, q_all, kv_all, times):
    sources, half_rows, _ = q_all.shape
    q_units, k_units = 4 * sources, 4 * sources
    q_rows = (q_units * SLOT + QB - 1) // QB * QB
    step = KB
    k_rows = (k_units * SLOT + step - 1) // step * step
    fill = -(-step // (2 * SLOT))
    dma = pltpu.SemaphoreType.DMA
    return pl.pallas_call(
        functools.partial(attention_kernel, times=times),
        out_shape=(jax.ShapeDtypeStruct((sources, half_rows, 128), jnp.bfloat16),
                   jax.ShapeDtypeStruct((2, sources, 128), jnp.float32)),
        in_specs=[spec(SMEM), spec(ANY), spec(ANY)],
        out_specs=(spec(VMEM), spec(VMEM)),
        scratch_shapes=[
            VMEM((k_units + 2 * fill, SLOT, 128), jnp.bfloat16),
            VMEM((q_rows // SLOT + 1, SLOT, 128), jnp.bfloat16),
            VMEM((k_rows // KB, HD + 16, KB), jnp.bfloat16),
            VMEM((q_rows // QB + 1, 128, QB), jnp.bfloat16),
            VMEM((q_rows // QB + 1, HD + 16, QB), jnp.float32),
            VMEM((q_rows, 128), jnp.float32),
            SMEM((16,), jnp.int32),
            dma((16,)), dma((64 + fill,)),
            *[VMEM((KB, QB), jnp.bfloat16) for _ in range(UN)],
        ],
        name="attention",
    )(counts, q_all.reshape(8, 4, half_rows, 128), kv_all.reshape(4, 2, 4, 2 * half_rows, 128))


def return_kernel(o_ref, lse_ref, back_ref, back_lse, mine, theirs, size_mine, size_theirs, both, size_both,
                  in_sem, t_send, t_recv, o_send, o_recv, l_send, l_recv):
    f, _, x, loc = place()
    hi, core = loc // 2, loc % 2
    half_rows = o_ref.shape[1]
    barrier = pltpu.get_barrier_semaphore()

    def greet(frame, there):
        pl.semaphore_signal(barrier, inc=1, device_id={"frame": frame, "space": x * 4 + there},
                            device_id_type=pl.DeviceIdType.MESH)

    greet(f, hi * 2 + 1 - core)
    each(1, 16, lambda n: greet((f + n // 2) % 8, ((hi + n) % 2) * 2 + core))

    keep = core * 16
    give = 16 - keep
    loads = [
        pltpu.make_async_copy(o_ref.at[pl.ds(keep, 16)], mine, in_sem.at[0]),
        pltpu.make_async_copy(lse_ref.at[:, pl.ds(keep, 16), :], size_mine, in_sem.at[1]),
    ]
    for copy in loads:
        copy.start()

    def twin(src, dst, n):
        return remote(src, dst, t_send.at[n], t_recv.at[n], f, x * 4 + hi * 2 + 1 - core)

    pl.semaphore_wait(barrier, 16)
    shares = [twin(lse_ref.at[:, pl.ds(give, 16), :], size_theirs, 0)]
    for n in range(2):
        shares.append(twin(o_ref.at[pl.ds(give + 8 * n, 8)], theirs.at[pl.ds(8 * n, 8)], 1 + n))
    for copy in shares:
        copy.start()
    for copy in loads:
        copy.wait()
    shares[0].wait_recv()

    turned = []
    for n in range(2):
        one, two = size_mine[n], size_theirs[n]
        top = jnp.maximum(one, two)
        one, two = jnp.exp2(one - top), jnp.exp2(two - top)
        total = one + two
        whole = top + jnp.log2(total)
        for r in range(16):
            size_both[r, n:n + 1, :] = whole[r:r + 1]
        turned.append(jnp.transpose(
            jnp.concatenate([one / total, two / total, jnp.zeros((96, 128), jnp.float32)], axis=0)))
    low = lax.broadcasted_iota(jnp.int32, (half_rows, 128), 1) < HD

    me = hi * 8 + f

    def copies(n):
        frame, there = (f + n // 2) % 8, (hi + n) % 2
        r = there * 8 + frame
        space = x * 4 + there * 2 + core
        return (remote(both.at[r], back_ref.at[me], o_send.at[n], o_recv.at[me], frame, space),
                remote(size_both.at[r], back_lse.at[me], l_send.at[n], l_recv.at[me], frame, space))

    def start(n):
        for copy in copies(n):
            copy.start()

    def sent(n):
        for copy in copies(n):
            copy.wait_send()

    for n in range(2):
        shares[1 + n].wait_recv()
        for r in range(8 * n, 8 * n + 8):
            one = jnp.where(low, turned[0][0:half_rows, r:r + 1], turned[1][0:half_rows, r:r + 1])
            two = jnp.where(low, turned[0][0:half_rows, 16 + r:17 + r], turned[1][0:half_rows, 16 + r:17 + r])
            both[r] = (mine[r].astype(jnp.float32) * one + theirs[r].astype(jnp.float32) * two).astype(jnp.bfloat16)

    each(1, 16, start)
    own = hi * 8 + f
    pltpu.make_async_copy(both.at[own], back_ref.at[me], o_recv.at[me]).start()
    pltpu.make_async_copy(size_both.at[own], back_lse.at[me], l_recv.at[me]).start()
    for copy in shares:
        copy.wait_send()
    each(1, 16, sent)
    each(0, 16, lambda n: pltpu.make_async_copy(both.at[0], back_ref.at[n], o_recv.at[n]).wait())
    each(0, 16, lambda n: pltpu.make_async_copy(size_both.at[0], back_lse.at[n], l_recv.at[n]).wait())


def give_results(partial, sizes):
    dma = pltpu.SemaphoreType.DMA
    half_rows = partial.shape[1]
    held = VMEM((16, half_rows, 128), partial.dtype)
    return pl.pallas_call(
        return_kernel,
        out_shape=(jax.ShapeDtypeStruct((16, half_rows, 128), partial.dtype),
                   jax.ShapeDtypeStruct((16, 2, 128), sizes.dtype)),
        in_specs=[spec(ANY), spec(ANY)],
        out_specs=(spec(ANY), spec(ANY)),
        scratch_shapes=[
            held, held, VMEM((2, 16, 128), sizes.dtype), VMEM((2, 16, 128), sizes.dtype),
            held, VMEM((16, 2, 128), sizes.dtype),
            dma((2,)), dma((3,)), dma((3,)), dma((16,)), dma((16,)), dma((16,)), dma((16,))],
        compiler_params=pltpu.CompilerParams(collective_id=1, has_side_effects=True),
        name="give_results",
    )(partial, sizes)


def finish_kernel(tok_ref, cnt_ref, back_ref, lse_ref, w_ref, o_ref, att, ys):
    times, slots, width = tok_ref.shape
    half = slots * SLOT // 2
    rows = slots * SLOT

    def shares(n):
        sizes = [lse_ref[p * 8:p * 8 + 8, n, :] for p in range(2)]
        top = jnp.maximum(sizes[0], sizes[1])
        powers = [jnp.exp2(v - top) for v in sizes]
        total = powers[0] + powers[1]
        return jnp.transpose(
            jnp.concatenate([v / total for v in powers] + [jnp.zeros((112, 128), jnp.float32)], axis=0))

    first, second = shares(0), shares(1)
    low = lax.broadcasted_iota(jnp.int32, (half, 128), 1) < HD

    def merged(h):
        out = jnp.zeros((half, 128), jnp.float32)
        for p in range(2):
            n = p * 8 + h
            share = jnp.where(low, first[0:half, n:n + 1], second[0:half, n:n + 1])
            out = out + back_ref[n].astype(jnp.float32) * share
        return out

    for j in range(HEADS // 2):
        a, b = merged(2 * j), merged(2 * j + 1)
        cols = slice(128 * j, 128 * j + 128)
        att[0:half, cols] = jnp.where(low, a, pltpu.roll(b, HD, 1)).astype(jnp.bfloat16)
        att[half:rows, cols] = jnp.where(low, pltpu.roll(a, HD, 1), b).astype(jnp.bfloat16)
    for c in range(width // 256):
        cols = slice(256 * c, 256 * c + 256)
        mixed = jnp.dot(att[...], w_ref[:, cols], preferred_element_type=jnp.float32)
        for i in range(slots):
            for e in range(2):
                ys[2 * c + e, pl.ds(i, SLOT, stride=slots), :] = (
                    mixed[i * SLOT:i * SLOT + SLOT, 128 * e:128 * e + 128])
    live = lax.broadcasted_iota(jnp.int32, (slots, width), 0) < cnt_ref[0]
    for t in range(times):
        mixed = jnp.concatenate([ys[c, t * slots:t * slots + slots, :] for c in range(width // 128)], axis=1)
        value = tok_ref[t].astype(jnp.float32) + mixed
        o_ref[t] = jnp.where(live, value, 0.0).astype(jnp.bfloat16)


def finish(tokens, count, back, sizes, w_out):
    times, slots, width = tokens.shape
    rows = slots * SLOT
    return pl.pallas_call(
        finish_kernel,
        out_shape=jax.ShapeDtypeStruct(tokens.shape, tokens.dtype),
        in_specs=[spec(VMEM), spec(SMEM), spec(VMEM), spec(VMEM), spec(VMEM)],
        out_specs=spec(VMEM),
        scratch_shapes=[VMEM((rows, w_out.shape[0]), jnp.bfloat16), VMEM((width // 128, rows, 128), jnp.float32)],
        name="finish",
    )(tokens, count, back, sizes, w_out)


def on_device(tokens, tube_count, ln_gain, ln_bias, w_qkv, w_out):
    tokens = jnp.transpose(tokens, (1, 0, 2))
    q_all, kv_all, counts = project(
        tokens, tube_count, ln_gain.reshape(1, -1), ln_bias.reshape(1, -1), w_qkv)
    partial, sizes = attention(counts, q_all, kv_all, tokens.shape[0])
    mixed = finish(tokens, tube_count, *give_results(partial, sizes), w_out)
    return jnp.transpose(mixed, (1, 0, 2))


def solution(mesh):
    in_specs = (P("space", "frame", None), P("space"), P(), P(), P(), P())
    return jax.shard_map(
        on_device, mesh=mesh, in_specs=in_specs, out_specs=P("space", "frame", None), check_vma=False)
```

```python
import functools

import jax
import jax.numpy as jnp
from jax import lax
from jax.experimental import pallas as pl
from jax.experimental.pallas import tpu as pltpu
from jax.sharding import PartitionSpec as P

HEADS = 8
HD = 64
SLOT = 40
KB = 256
UN = 8
QB = 512
DEAD = -1e30
Q_AFTER = 2
SAFE = 100.0
EPSILON = 1e-06
SCALE = 1.4426950408889634 / 8.0
ANY = pl.ANY
VMEM = pltpu.VMEM
SMEM = pltpu.SMEM


def spec(space):
    return pl.BlockSpec(memory_space=space)


def near(array):
    return pltpu.with_memory_space_constraint(array, VMEM)


def place():
    f, s = lax.axis_index("frame"), lax.axis_index("space")
    return f, s, s // 4, s % 4


def remote(src, dst, send, recv, frame, space):
    return pltpu.make_async_remote_copy(
        src_ref=src, dst_ref=dst, send_sem=send, recv_sem=recv,
        device_id={"frame": frame, "space": space}, device_id_type=pl.DeviceIdType.MESH)


def each(lo, hi, body):
    def step(i, c):
        body(i)
        return c
    lax.fori_loop(lo, hi, step, 0)


def project_kernel(tok_in, cnt_ref, gain_ref, bias_ref, w_ref, w_last, q_out, kv_out, cnt_out, tok_ref, w_next,
                   w_v, xs, nb, kvs, qs, cnts,
                   w_sem, kv_send, kv_recv, q_send, q_recv, c_send, c_recv, x_send, r_send, x_recv):
    f, s, x, loc = place()
    times, slots, width = tok_ref.shape
    inner = HEADS * HD

    tok_copy = pltpu.make_async_copy(tok_in, tok_ref, w_sem.at[3])
    tok_copy.start()
    last_copy = pltpu.make_async_copy(w_last, w_next, w_sem.at[4])
    copies = []
    for n, at in enumerate((inner, 2 * inner, 0)):
        cols = pl.ds(at, inner)
        copy = pltpu.make_async_copy(w_ref.at[:, cols], w_v.at[:, cols], w_sem.at[n])
        copy.start()
        copies.append(copy)

    barrier = pltpu.get_barrier_semaphore()

    def greet(frame, space):
        pl.semaphore_signal(barrier, inc=1, device_id={"frame": frame, "space": space},
                            device_id_type=pl.DeviceIdType.MESH)

    each(1, 32, lambda n: greet((f + n // 4) % 8, x * 4 + (loc + n % 4) % 4))
    each(0, 12, lambda n: greet(f, ((x + 1 + n // 4) % 4) * 4 + n % 4))

    cnts[...] = jnp.full(cnts.shape, cnt_ref[0], jnp.int32)

    tok_copy.wait()
    for t in range(SLOT):
        values = tok_ref[t % times].astype(jnp.float32)
        for c in range(width // 128):
            xs[c, t * slots:t * slots + slots, :] = values[:, 128 * c:128 * c + 128]
    for i in range(slots):
        values = jnp.concatenate(
            [xs[c, pl.ds(i, SLOT, stride=slots), :] for c in range(width // 128)], axis=1)
        center = values - jnp.mean(values, axis=-1, keepdims=True)
        spread = jnp.mean(center * center, axis=-1, keepdims=True)
        normed = center * lax.rsqrt(spread + EPSILON) * gain_ref[...] + bias_ref[...]
        nb[i * SLOT:i * SLOT + SLOT, :] = normed.astype(jnp.bfloat16)

    rows_all = slots * SLOT
    half = rows_all // 2
    low = lax.broadcasted_iota(jnp.int32, (rows_all, 128), 1) < HD
    low_half = lax.broadcasted_iota(jnp.int32, (half, 128), 1) < HD

    copies[0].wait()
    copies[1].wait()
    for g in range(2):
        k4 = jnp.dot(nb[...], w_v[:, inner + 256 * g:inner + 256 * g + 256], preferred_element_type=jnp.float32)
        v4 = jnp.dot(nb[...], w_v[:, 2 * inner + 256 * g:2 * inner + 256 * g + 256],
                     preferred_element_type=jnp.float32)
        for j in range(2):
            k2, v2 = k4[:, 128 * j:128 * j + 128], v4[:, 128 * j:128 * j + 128]
            h = 4 * g + 2 * j
            kvs[h] = jnp.where(low, k2, pltpu.roll(v2, HD, 1)).astype(jnp.bfloat16)
            kvs[h + 1] = jnp.where(low, pltpu.roll(k2, HD, 1), v2).astype(jnp.bfloat16)

    part = f // 2
    source = x * 8 + (f % 2) * 4 + loc
    mine = (f % 2) * 4 + loc
    pl.semaphore_wait(barrier, 43)

    def kv_copy(d):
        h = (f + d + 2 * loc) % 8
        stays = (h == f) & (part == loc)
        return stays, h, remote(
            kvs.at[h], kv_out.at[source], kv_send.at[d], kv_recv.at[mine], h, x * 4 + part)

    def kv_start(d):
        stays, h, copy = kv_copy(d)

        @pl.when(stays)
        def _():
            pltpu.make_async_copy(kvs.at[h], kv_out.at[source], kv_recv.at[mine]).start()

        @pl.when(jnp.logical_not(stays))
        def _():
            copy.start()

    each(0, 8, kv_start)

    def count_copy(e):
        return remote(cnts, cnt_out.at[s], c_send.at[e], c_recv.at[s], f, (s + e) % 16)

    each(1, 16, lambda e: count_copy(e).start())
    pltpu.make_async_copy(cnts, cnt_out.at[s], c_recv.at[s]).start()

    copies[2].wait()
    last_copy.start()
    for g in range(2):
        q4 = jnp.dot(nb[...], w_v[:, 256 * g:256 * g + 256], preferred_element_type=jnp.float32) * SCALE
        for j in range(2):
            q2 = q4[:, 128 * j:128 * j + 128]
            h = 4 * g + 2 * j
            qs[h] = jnp.where(low_half, q2[:half], pltpu.roll(q2[half:], HD, 1)).astype(jnp.bfloat16)
            qs[h + 1] = jnp.where(low_half, pltpu.roll(q2[:half], HD, 1), q2[half:]).astype(jnp.bfloat16)

    me = f * 4 + loc

    def q_copy(n):
        h = (f + n // 4) % 8
        return remote(qs.at[h], q_out.at[me], q_send.at[n], q_recv.at[me], h, x * 4 + (loc + n % 4) % 4)

    def ring(n, piece, send, step):
        there = (x + step) % 4
        return remote(kv_out.at[piece], kv_out.at[piece], send.at[n], x_recv.at[piece], f, there * 4 + loc)

    def nth(t):
        u = (f - 2 * loc - t + 16) % 8
        return (u % 2) * 4 + u // 2

    right, left, over = ((x + 1) % 4) * 8, ((x + 3) % 4) * 8, ((x + 2) % 4) * 8

    def landed(sem, index, piece):
        pltpu.make_async_copy(kv_out.at[piece], kv_out.at[piece], sem.at[index]).wait()

    def arrived(t):
        i = nth(t)
        piece = x * 8 + i
        landed(kv_recv, i, piece)
        ring(2 * t, piece, x_send, 1).start()
        ring(2 * t + 1, piece, x_send, 3).start()

    each(0, Q_AFTER, arrived)
    each(1, 32, lambda n: q_copy(n).start())
    pltpu.make_async_copy(qs.at[f], q_out.at[me], q_recv.at[me]).start()
    each(Q_AFTER, 8, arrived)

    def relay(t):
        i = nth(2 * t)
        landed(x_recv, left + i, left + i)
        ring(2 * t, left + i, r_send, 1).start()
        i = nth(2 * t + 1)
        landed(x_recv, right + i, right + i)
        ring(2 * t + 1, right + i, r_send, 3).start()

    each(0, 4, relay)

    def rest(t):
        i = nth(2 * t + 1)
        landed(x_recv, left + i, left + i)
        i = nth(2 * t)
        landed(x_recv, right + i, right + i)

    each(0, 4, rest)

    def last(t):
        i = nth(t)
        landed(x_recv, over + i, over + i)

    each(0, 8, last)

    def kv_sent(d):
        stays, _, copy = kv_copy(d)

        @pl.when(jnp.logical_not(stays))
        def _():
            copy.wait_send()

    def ring_sent(t):
        piece = x * 8 + nth(t)
        ring(2 * t, piece, x_send, 1).wait_send()
        ring(2 * t + 1, piece, x_send, 3).wait_send()

    def relay_sent(t):
        ring(2 * t, left + nth(2 * t), r_send, 1).wait_send()
        ring(2 * t + 1, right + nth(2 * t + 1), r_send, 3).wait_send()

    last_copy.wait()
    each(0, 8, kv_sent)
    each(1, 16, lambda e: count_copy(e).wait_send())
    each(1, 32, lambda n: q_copy(n).wait_send())
    each(0, 8, ring_sent)
    each(0, 4, relay_sent)
    each(0, 16, lambda n: pltpu.make_async_copy(cnts, cnt_out.at[n], c_recv.at[n]).wait())
    each(0, 32, lambda n: pltpu.make_async_copy(qs.at[0], q_out.at[n], q_recv.at[n]).wait())


def project(tokens, count, gain, bias, w_qkv, w_out):
    times, slots, width = tokens.shape
    rows = slots * SLOT
    bf16, i32 = jnp.bfloat16, jnp.int32
    dma = pltpu.SemaphoreType.DMA
    return pl.pallas_call(
        project_kernel,
        out_shape=(VMEM((32, rows // 2, 128), bf16),
                   VMEM((32, rows, 128), bf16),
                   jax.ShapeDtypeStruct((16, 1, 128), i32),
                   VMEM(tokens.shape, bf16), VMEM(w_out.shape, bf16)),
        in_specs=[spec(ANY), spec(SMEM), spec(VMEM), spec(VMEM), spec(ANY), spec(ANY)],
        out_specs=(spec(ANY), spec(ANY), spec(ANY), spec(VMEM), spec(ANY)),
        scratch_shapes=[
            VMEM(w_qkv.shape, bf16), VMEM((width // 128, rows, 128), jnp.float32), VMEM((rows, width), bf16),
            VMEM((HEADS, rows, 128), bf16), VMEM((HEADS, rows // 2, 128), bf16), VMEM((1, 128), i32),
            dma((5,)), dma((8,)), dma((8,)), dma((32,)), dma((32,)), dma((16,)), dma((16,)),
            dma((16,)), dma((8,)), dma((32,)),
        ],
        compiler_params=pltpu.CompilerParams(collective_id=0, has_side_effects=True),
        name="project",
    )(tokens, count, gain, bias, w_qkv, w_out)


def attention_kernel(cnt_ref, q_hbm, kv_hbm, o_ref, lse_ref, kvc, qc, vt, qt, acc, of, at_q, q_sem, k_sem, *held, times):
    base = (lax.axis_index("space") // 4) * 4
    kv_flat = kvc.reshape(kvc.shape[0] * SLOT, 128)
    q_flat = qc.reshape(qc.shape[0] * SLOT, 128)
    step_keys = KB

    def q_copy(j, l, unit):
        return pltpu.make_async_copy(
            q_hbm.at[:, l, pl.ds((j % 2) * SLOT, SLOT), :], qc.at[pl.ds(unit, 8)], q_sem.at[j * 4 + l])

    def k_copy(xs, l, j, unit):
        return pltpu.make_async_copy(
            kv_hbm.at[xs, :, l, pl.ds(j * SLOT, SLOT), :], kvc.at[pl.ds(unit, 2)], k_sem.at[(xs * 4 + l) * 4 + j])

    def start_keys(n, unit):
        count = cnt_ref[n, 0, 0]
        for j in range(4):
            @pl.when(j < count)
            def _(j=j):
                k_copy(n // 4, n % 4, j, unit + 2 * j).start()
        return unit + 2 * count

    key_units = lax.fori_loop(0, 16, start_keys, jnp.int32(0))
    fill = -(-step_keys // (2 * SLOT))

    def fill_copy(n):
        return pltpu.make_async_copy(
            kv_hbm.at[0, :, 0, pl.ds(0, SLOT), :], kvc.at[pl.ds(key_units + 2 * n, 2)], k_sem.at[64 + n])

    each(0, fill, lambda n: fill_copy(n).start())

    unit = jnp.int32(0)
    for j in range(4):
        if j == 2:
            low_units = unit
        for l in range(4):
            live = j < cnt_ref[base + l, 0, 0]
            at_q[j * 4 + l] = jnp.where(live, unit, 0)

            @pl.when(live)
            def _(j=j, l=l, unit=unit):
                q_copy(j, l, unit).start()
            unit = unit + jnp.where(live, 8, 0)
    query_rows = unit * SLOT
    query_tiles = (query_rows + QB - 1) // QB
    key_rows = key_units * SLOT
    key_steps = (key_rows + step_keys - 1) // step_keys

    def wait_keys(n, c):
        count = cnt_ref[n, 0, 0]
        for j in range(4):
            @pl.when(j < count)
            def _(j=j):
                k_copy(n // 4, n % 4, j, 0).wait()
        return c

    lax.fori_loop(0, 16, wait_keys, 0)
    each(0, fill, lambda n: fill_copy(n).wait())

    key_at = lax.broadcasted_iota(jnp.int32, (HD, KB), 1)
    row16 = lax.broadcasted_iota(jnp.int32, (16, KB), 0)

    def shape_keys(b, longest):
        turned = jnp.transpose(kv_flat[pl.ds(pl.multiple_of(b * KB, KB), KB), :].astype(jnp.float32))
        index = key_at + b * KB
        live = (index % SLOT < times) & (index < key_rows)
        vt[b, 0:HD, :] = jnp.where(live, turned[HD:], 0.0).astype(jnp.bfloat16)
        vt[b, HD:HD + 16, :] = jnp.where(live[:16] & (row16 == 0), 1.0, 0.0).astype(jnp.bfloat16)
        keys = turned[:HD]
        return jnp.maximum(longest, jnp.sum(keys * keys, axis=0, keepdims=True))

    longest_key = lax.fori_loop(0, key_steps, shape_keys, jnp.zeros((1, KB), jnp.float32))

    for j in range(4):
        for l in range(4):
            @pl.when(j < cnt_ref[base + l, 0, 0])
            def _(j=j, l=l):
                q_copy(j, l, 0).wait()

    col = lax.broadcasted_iota(jnp.int32, (HD, QB), 1)
    low_rows = low_units * SLOT

    def shape_queries(t, longest):
        turned = jnp.transpose(q_flat[pl.ds(pl.multiple_of(t * QB, QB), QB), :].astype(jnp.float32))
        index = col + t * QB
        query = jnp.where(index < low_rows, turned[:HD], turned[HD:])
        query = jnp.where(index < query_rows, query, 0.0)
        qt[t, 0:HD, :] = query.astype(jnp.bfloat16)
        qt[t, HD:, :] = jnp.zeros((HD, QB), jnp.bfloat16)
        return jnp.maximum(longest, jnp.sum(query * query, axis=0, keepdims=True))

    longest_query = lax.fori_loop(0, query_tiles, shape_queries, jnp.zeros((1, QB), jnp.float32))
    safe = jnp.max(longest_key) * jnp.max(longest_query) < SAFE * SAFE

    def put(t, total, best):
        weight_sum = total[HD:HD + 1, :]
        out = total[0:HD, :] / weight_sum
        lse = jnp.broadcast_to(best + jnp.log2(weight_sum), (HD, QB))
        low = col + t * QB < low_rows
        both = jnp.concatenate([jnp.where(low, out, lse), jnp.where(low, lse, out)], axis=0)
        of[pl.ds(pl.multiple_of(t * QB, QB), QB), :] = jnp.transpose(both)

    def block_scores(b, t):
        keys = kv_flat[pl.ds(pl.multiple_of(b * KB, KB), KB), :]
        return jnp.dot(keys, qt[t], preferred_element_type=jnp.float32)

    def clear(t):
        acc[t] = jnp.zeros((HD + 16, QB), jnp.float32)

    def after(item):
        t, b = item
        turn = b + 1 == key_steps
        return jnp.minimum(jnp.where(turn, t + 1, t), query_tiles), jnp.where(turn, 0, b + 1)

    def plain(i, carry):
        before, now = carry
        then = now[-1]
        later = []
        for u in range(UN):
            t, b = before[u]
            acc[t] += jnp.dot(vt[b], held[u][...], preferred_element_type=jnp.float32)
            t, b = now[u]
            held[u][...] = jnp.exp2(block_scores(b, t)).astype(jnp.bfloat16)
            then = after(then)
            later.append(then)
        return now, tuple(later)

    def plain_all():
        each(0, query_tiles, clear)
        first = [(jnp.int32(0), jnp.int32(0))]
        for _ in range(UN - 1):
            first.append(after(first[-1]))
        nowhere = ((query_tiles, jnp.int32(0)),) * UN
        steps = (query_tiles * key_steps + UN - 1) // UN + 1
        lax.fori_loop(0, steps, plain, (nowhere, tuple(first)))

        each(0, query_tiles, lambda t: put(t, acc[t], 0.0))

    def shifted_tile(t):
        def step(b, carry):
            best, total = carry
            scores = block_scores(b, t)
            best_next = jnp.maximum(best, jnp.max(scores, axis=0, keepdims=True))
            weights = jnp.exp2(scores - best_next).astype(jnp.bfloat16)
            total = total * jnp.exp2(best - best_next) + jnp.dot(
                vt[b], weights, preferred_element_type=jnp.float32)
            return best_next, total

        best, total = lax.fori_loop(
            0, key_steps, step,
            (jnp.full((1, QB), DEAD, jnp.float32), jnp.zeros((HD + 16, QB), jnp.float32)))
        put(t, total, best)

    @pl.when(safe)
    def _():
        plain_all()

    @pl.when(jnp.logical_not(safe))
    def _():
        each(0, query_tiles, shifted_tile)

    lane = lax.broadcasted_iota(jnp.int32, (SLOT, 128), 1)
    in_low = lane < HD

    def give_back(i, sizes):
        f, l = i % 8, ((i // 8) % 2) * 2 + i // 16
        sizes_next = []
        for j in range(2):
            first = of[pl.ds(pl.multiple_of((at_q[j * 4 + l] + f) * SLOT, 8), SLOT), :]
            second = of[pl.ds(pl.multiple_of((at_q[j * 4 + 8 + l] + f) * SLOT, 8), SLOT), :]
            o_ref[i, j * SLOT:j * SLOT + SLOT, :] = jnp.where(in_low, first, second).astype(jnp.bfloat16)
            sizes_next.append(jnp.where(lane % HD == i, jnp.where(in_low, second, first), sizes[j]))
        return tuple(sizes_next)

    sizes = lax.fori_loop(0, 32, give_back, (jnp.zeros((SLOT, 128), jnp.float32),) * 2)
    turned = jnp.transpose(jnp.concatenate([*sizes, jnp.zeros((128 - 2 * SLOT, 128), jnp.float32)], axis=0))
    lse_ref[0] = turned[HD:HD + 32]
    lse_ref[1] = turned[0:32]


def attention(counts, q_all, kv_all, times):
    sources, half_rows, _ = q_all.shape
    q_units, k_units = 4 * sources, 4 * sources
    q_rows = (q_units * SLOT + QB - 1) // QB * QB
    step = KB
    k_rows = (k_units * SLOT + step - 1) // step * step
    fill = -(-step // (2 * SLOT))
    dma = pltpu.SemaphoreType.DMA
    return pl.pallas_call(
        functools.partial(attention_kernel, times=times),
        out_shape=(VMEM((sources, half_rows, 128), jnp.bfloat16),
                   VMEM((2, sources, 128), jnp.float32)),
        in_specs=[spec(SMEM), spec(ANY), spec(ANY)],
        out_specs=(spec(VMEM), spec(VMEM)),
        scratch_shapes=[
            VMEM((k_units + 2 * fill, SLOT, 128), jnp.bfloat16),
            VMEM((q_rows // SLOT + 1, SLOT, 128), jnp.bfloat16),
            VMEM((k_rows // KB, HD + 16, KB), jnp.bfloat16),
            VMEM((q_rows // QB + 1, 128, QB), jnp.bfloat16),
            VMEM((q_rows // QB + 1, HD + 16, QB), jnp.float32),
            VMEM((q_rows, 128), jnp.float32),
            SMEM((16,), jnp.int32),
            dma((16,)), dma((64 + fill,)),
            *[VMEM((KB, QB), jnp.bfloat16) for _ in range(UN)],
        ],
        name="attention",
    )(counts, near(q_all.reshape(8, 4, half_rows, 128)),
      near(kv_all.reshape(4, 2, 4, 2 * half_rows, 128)))


def return_kernel(o_ref, lse_ref, back_ref, back_lse, mine, theirs, size_mine, size_theirs, both, size_both,
                  in_sem, t_send, t_recv, o_send, o_recv, l_send, l_recv):
    f, _, x, loc = place()
    hi, core = loc // 2, loc % 2
    half_rows = o_ref.shape[1]
    barrier = pltpu.get_barrier_semaphore()

    def greet(frame, there):
        pl.semaphore_signal(barrier, inc=1, device_id={"frame": frame, "space": x * 4 + there},
                            device_id_type=pl.DeviceIdType.MESH)

    greet(f, hi * 2 + 1 - core)
    each(1, 16, lambda n: greet((f + n // 2) % 8, ((hi + n) % 2) * 2 + core))

    keep = core * 16
    give = 16 - keep
    loads = [
        pltpu.make_async_copy(o_ref.at[pl.ds(keep, 16)], mine, in_sem.at[0]),
        pltpu.make_async_copy(lse_ref.at[:, pl.ds(keep, 16), :], size_mine, in_sem.at[1]),
    ]
    for copy in loads:
        copy.start()

    def twin(src, dst, n):
        return remote(src, dst, t_send.at[n], t_recv.at[n], f, x * 4 + hi * 2 + 1 - core)

    pl.semaphore_wait(barrier, 16)
    shares = [twin(lse_ref.at[:, pl.ds(give, 16), :], size_theirs, 0)]
    for n in range(2):
        shares.append(twin(o_ref.at[pl.ds(give + 8 * n, 8)], theirs.at[pl.ds(8 * n, 8)], 1 + n))
    for copy in shares:
        copy.start()
    for copy in loads:
        copy.wait()
    shares[0].wait_recv()

    turned = []
    for n in range(2):
        one, two = size_mine[n], size_theirs[n]
        top = jnp.maximum(one, two)
        one, two = jnp.exp2(one - top), jnp.exp2(two - top)
        total = one + two
        whole = top + jnp.log2(total)
        for r in range(16):
            size_both[r, n:n + 1, :] = whole[r:r + 1]
        turned.append(jnp.transpose(
            jnp.concatenate([one / total, two / total, jnp.zeros((96, 128), jnp.float32)], axis=0)))
    low = lax.broadcasted_iota(jnp.int32, (half_rows, 128), 1) < HD

    me = hi * 8 + f

    def copies(n):
        frame, there = (f + n // 2) % 8, (hi + n) % 2
        r = there * 8 + frame
        space = x * 4 + there * 2 + core
        return (remote(both.at[r], back_ref.at[me], o_send.at[n], o_recv.at[me], frame, space),
                remote(size_both.at[r], back_lse.at[me], l_send.at[n], l_recv.at[me], frame, space))

    def start(n):
        for copy in copies(n):
            copy.start()

    def sent(n):
        for copy in copies(n):
            copy.wait_send()

    for n in range(2):
        shares[1 + n].wait_recv()
        for r in range(8 * n, 8 * n + 8):
            one = jnp.where(low, turned[0][0:half_rows, r:r + 1], turned[1][0:half_rows, r:r + 1])
            two = jnp.where(low, turned[0][0:half_rows, 16 + r:17 + r], turned[1][0:half_rows, 16 + r:17 + r])
            both[r] = (mine[r].astype(jnp.float32) * one + theirs[r].astype(jnp.float32) * two).astype(jnp.bfloat16)

    each(1, 16, start)
    own = hi * 8 + f
    pltpu.make_async_copy(both.at[own], back_ref.at[me], o_recv.at[me]).start()
    pltpu.make_async_copy(size_both.at[own], back_lse.at[me], l_recv.at[me]).start()
    for copy in shares:
        copy.wait_send()
    each(1, 16, sent)
    each(0, 16, lambda n: pltpu.make_async_copy(both.at[0], back_ref.at[n], o_recv.at[n]).wait())
    each(0, 16, lambda n: pltpu.make_async_copy(size_both.at[0], back_lse.at[n], l_recv.at[n]).wait())


def give_results(partial, sizes):
    dma = pltpu.SemaphoreType.DMA
    half_rows = partial.shape[1]
    held = VMEM((16, half_rows, 128), partial.dtype)
    return pl.pallas_call(
        return_kernel,
        out_shape=(VMEM((16, half_rows, 128), partial.dtype),
                   VMEM((16, 2, 128), sizes.dtype)),
        in_specs=[spec(ANY), spec(ANY)],
        out_specs=(spec(ANY), spec(ANY)),
        scratch_shapes=[
            held, held, VMEM((2, 16, 128), sizes.dtype), VMEM((2, 16, 128), sizes.dtype),
            held, VMEM((16, 2, 128), sizes.dtype),
            dma((2,)), dma((3,)), dma((3,)), dma((16,)), dma((16,)), dma((16,)), dma((16,))],
        compiler_params=pltpu.CompilerParams(collective_id=1, has_side_effects=True),
        name="give_results",
    )(near(partial), near(sizes))


def finish_kernel(tok_ref, cnt_ref, back_ref, lse_ref, w_ref, o_ref, att, ys):
    times, slots, width = tok_ref.shape
    half = slots * SLOT // 2
    rows = slots * SLOT

    def shares(n):
        sizes = [lse_ref[p * 8:p * 8 + 8, n, :] for p in range(2)]
        top = jnp.maximum(sizes[0], sizes[1])
        powers = [jnp.exp2(v - top) for v in sizes]
        total = powers[0] + powers[1]
        return jnp.transpose(
            jnp.concatenate([v / total for v in powers] + [jnp.zeros((112, 128), jnp.float32)], axis=0))

    first, second = shares(0), shares(1)
    low = lax.broadcasted_iota(jnp.int32, (half, 128), 1) < HD

    def merged(h):
        out = jnp.zeros((half, 128), jnp.float32)
        for p in range(2):
            n = p * 8 + h
            share = jnp.where(low, first[0:half, n:n + 1], second[0:half, n:n + 1])
            out = out + back_ref[n].astype(jnp.float32) * share
        return out

    for j in range(HEADS // 2):
        a, b = merged(2 * j), merged(2 * j + 1)
        cols = slice(128 * j, 128 * j + 128)
        att[0:half, cols] = jnp.where(low, a, pltpu.roll(b, HD, 1)).astype(jnp.bfloat16)
        att[half:rows, cols] = jnp.where(low, pltpu.roll(a, HD, 1), b).astype(jnp.bfloat16)
    for c in range(width // 256):
        cols = slice(256 * c, 256 * c + 256)
        mixed = jnp.dot(att[...], w_ref[:, cols], preferred_element_type=jnp.float32)
        for i in range(slots):
            for e in range(2):
                ys[2 * c + e, pl.ds(i, SLOT, stride=slots), :] = (
                    mixed[i * SLOT:i * SLOT + SLOT, 128 * e:128 * e + 128])
    live = lax.broadcasted_iota(jnp.int32, (slots, width), 0) < cnt_ref[0]
    for t in range(times):
        mixed = jnp.concatenate([ys[c, t * slots:t * slots + slots, :] for c in range(width // 128)], axis=1)
        value = tok_ref[t].astype(jnp.float32) + mixed
        o_ref[t] = jnp.where(live, value, 0.0).astype(jnp.bfloat16)


def finish(tokens, count, back, sizes, w_out):
    times, slots, width = tokens.shape
    rows = slots * SLOT
    return pl.pallas_call(
        finish_kernel,
        out_shape=jax.ShapeDtypeStruct(tokens.shape, tokens.dtype),
        in_specs=[spec(VMEM), spec(SMEM), spec(VMEM), spec(VMEM), spec(VMEM)],
        out_specs=spec(VMEM),
        scratch_shapes=[VMEM((rows, w_out.shape[0]), jnp.bfloat16), VMEM((width // 128, rows, 128), jnp.float32)],
        name="finish",
    )(near(tokens), count, near(back), near(sizes), near(w_out))


def on_device(tokens, tube_count, ln_gain, ln_bias, w_qkv, w_out):
    tokens = jnp.transpose(tokens, (1, 0, 2))
    q_all, kv_all, counts, tokens, w_out = project(
        tokens, tube_count, ln_gain.reshape(1, -1), ln_bias.reshape(1, -1), w_qkv, w_out)
    partial, sizes = attention(counts, q_all, kv_all, tokens.shape[0])
    mixed = finish(tokens, tube_count, *give_results(partial, sizes), w_out)
    return jnp.transpose(mixed, (1, 0, 2))


def solution(mesh):
    in_specs = (P("space", "frame", None), P("space"), P(), P(), P(), P())
    return jax.shard_map(
        on_device, mesh=mesh, in_specs=in_specs, out_specs=P("space", "frame", None), check_vma=False)
```

```python
import functools

import jax
import jax.numpy as jnp
from jax import lax
from jax.experimental import pallas as pl
from jax.experimental.pallas import tpu as pltpu
from jax.sharding import PartitionSpec as P

HEADS = 8
HD = 64
SLOT = 40
KB = 256
UN = 8
QB = 512
DEAD = -1e30
Q_AFTER = 2
SAFE = 100.0
EPSILON = 1e-06
SCALE = 1.4426950408889634 / 8.0
ANY = pl.ANY
VMEM = pltpu.VMEM
SMEM = pltpu.SMEM


def spec(space):
    return pl.BlockSpec(memory_space=space)


def near(array):
    return pltpu.with_memory_space_constraint(array, VMEM)


def place():
    f, s = lax.axis_index("frame"), lax.axis_index("space")
    return f, s, s // 4, s % 4


def remote(src, dst, send, recv, frame, space):
    return pltpu.make_async_remote_copy(
        src_ref=src, dst_ref=dst, send_sem=send, recv_sem=recv,
        device_id={"frame": frame, "space": space}, device_id_type=pl.DeviceIdType.MESH)


def each(lo, hi, body):
    def step(i, c):
        body(i)
        return c
    lax.fori_loop(lo, hi, step, 0)


def project_kernel(tok_in, cnt_ref, gain_ref, bias_ref, w_ref, w_last, q_out, kv_out, cnt_out, tok_ref, w_next,
                   w_v, xs, nb, kvs, qs, cnts,
                   w_sem, kv_send, kv_recv, q_send, q_recv, c_send, c_recv, x_send, r_send, x_recv):
    f, s, x, loc = place()
    times, slots, width = tok_ref.shape
    inner = HEADS * HD

    tok_copy = pltpu.make_async_copy(tok_in, tok_ref, w_sem.at[3])
    tok_copy.start()
    last_copy = pltpu.make_async_copy(w_last, w_next, w_sem.at[4])
    copies = []
    for n, at in enumerate((inner, 2 * inner, 0)):
        cols = pl.ds(at, inner)
        copy = pltpu.make_async_copy(w_ref.at[:, cols], w_v.at[:, cols], w_sem.at[n])
        copy.start()
        copies.append(copy)

    barrier = pltpu.get_barrier_semaphore()

    def greet(frame, space):
        pl.semaphore_signal(barrier, inc=1, device_id={"frame": frame, "space": space},
                            device_id_type=pl.DeviceIdType.MESH)

    each(1, 32, lambda n: greet((f + n // 4) % 8, x * 4 + (loc + n % 4) % 4))
    each(0, 12, lambda n: greet(f, ((x + 1 + n // 4) % 4) * 4 + n % 4))

    cnts[...] = jnp.full(cnts.shape, cnt_ref[0], jnp.int32)

    tok_copy.wait()
    for t in range(SLOT):
        values = tok_ref[t % times].astype(jnp.float32)
        for c in range(width // 128):
            xs[c, t * slots:t * slots + slots, :] = values[:, 128 * c:128 * c + 128]
    for i in range(slots):
        values = jnp.concatenate(
            [xs[c, pl.ds(i, SLOT, stride=slots), :] for c in range(width // 128)], axis=1)
        center = values - jnp.mean(values, axis=-1, keepdims=True)
        spread = jnp.mean(center * center, axis=-1, keepdims=True)
        normed = center * lax.rsqrt(spread + EPSILON) * gain_ref[...] + bias_ref[...]
        nb[i * SLOT:i * SLOT + SLOT, :] = normed.astype(jnp.bfloat16)

    rows_all = slots * SLOT
    half = rows_all // 2
    low = lax.broadcasted_iota(jnp.int32, (rows_all, 128), 1) < HD
    low_half = lax.broadcasted_iota(jnp.int32, (half, 128), 1) < HD

    copies[0].wait()
    copies[1].wait()
    for g in range(2):
        k4 = jnp.dot(nb[...], w_v[:, inner + 256 * g:inner + 256 * g + 256], preferred_element_type=jnp.float32)
        v4 = jnp.dot(nb[...], w_v[:, 2 * inner + 256 * g:2 * inner + 256 * g + 256],
                     preferred_element_type=jnp.float32)
        for j in range(2):
            k2, v2 = k4[:, 128 * j:128 * j + 128], v4[:, 128 * j:128 * j + 128]
            h = 4 * g + 2 * j
            kvs[h] = jnp.where(low, k2, pltpu.roll(v2, HD, 1)).astype(jnp.bfloat16)
            kvs[h + 1] = jnp.where(low, pltpu.roll(k2, HD, 1), v2).astype(jnp.bfloat16)

    part = f // 2
    source = x * 8 + (f % 2) * 4 + loc
    mine = (f % 2) * 4 + loc
    pl.semaphore_wait(barrier, 43)

    def kv_copy(d):
        h = (f + d + 2 * loc) % 8
        stays = (h == f) & (part == loc)
        return stays, h, remote(
            kvs.at[h], kv_out.at[source], kv_send.at[d], kv_recv.at[mine], h, x * 4 + part)

    def kv_start(d):
        stays, h, copy = kv_copy(d)

        @pl.when(stays)
        def _():
            pltpu.make_async_copy(kvs.at[h], kv_out.at[source], kv_recv.at[mine]).start()

        @pl.when(jnp.logical_not(stays))
        def _():
            copy.start()

    each(0, 8, kv_start)

    def count_copy(e):
        return remote(cnts, cnt_out.at[s], c_send.at[e], c_recv.at[s], f, (s + e) % 16)

    each(1, 16, lambda e: count_copy(e).start())
    pltpu.make_async_copy(cnts, cnt_out.at[s], c_recv.at[s]).start()

    copies[2].wait()
    last_copy.start()
    for g in range(2):
        q4 = jnp.dot(nb[...], w_v[:, 256 * g:256 * g + 256], preferred_element_type=jnp.float32) * SCALE
        for j in range(2):
            q2 = q4[:, 128 * j:128 * j + 128]
            h = 4 * g + 2 * j
            qs[h] = jnp.where(low_half, q2[:half], pltpu.roll(q2[half:], HD, 1)).astype(jnp.bfloat16)
            qs[h + 1] = jnp.where(low_half, pltpu.roll(q2[:half], HD, 1), q2[half:]).astype(jnp.bfloat16)

    me = f * 4 + loc

    def q_copy(n):
        h = (f + n // 4) % 8
        return remote(qs.at[h], q_out.at[me], q_send.at[n], q_recv.at[me], h, x * 4 + (loc + n % 4) % 4)

    def ring(n, piece, send, step):
        there = (x + step) % 4
        return remote(kv_out.at[piece], kv_out.at[piece], send.at[n], x_recv.at[piece], f, there * 4 + loc)

    def nth(t):
        u = (f - 2 * loc - t + 16) % 8
        return (u % 2) * 4 + u // 2

    right, left, over = ((x + 1) % 4) * 8, ((x + 3) % 4) * 8, ((x + 2) % 4) * 8

    def landed(sem, index, piece):
        pltpu.make_async_copy(kv_out.at[piece], kv_out.at[piece], sem.at[index]).wait()

    def arrived(t):
        i = nth(t)
        piece = x * 8 + i
        landed(kv_recv, i, piece)
        ring(2 * t, piece, x_send, 1).start()
        ring(2 * t + 1, piece, x_send, 3).start()

    each(0, Q_AFTER, arrived)
    each(1, 32, lambda n: q_copy(n).start())
    pltpu.make_async_copy(qs.at[f], q_out.at[me], q_recv.at[me]).start()
    each(Q_AFTER, 8, arrived)

    def relay(t):
        i = nth(2 * t)
        landed(x_recv, left + i, left + i)
        ring(2 * t, left + i, r_send, 1).start()
        i = nth(2 * t + 1)
        landed(x_recv, right + i, right + i)
        ring(2 * t + 1, right + i, r_send, 3).start()

    each(0, 4, relay)

    def rest(t):
        i = nth(2 * t + 1)
        landed(x_recv, left + i, left + i)
        i = nth(2 * t)
        landed(x_recv, right + i, right + i)

    each(0, 4, rest)

    def last(t):
        i = nth(t)
        landed(x_recv, over + i, over + i)

    each(0, 8, last)

    def kv_sent(d):
        stays, _, copy = kv_copy(d)

        @pl.when(jnp.logical_not(stays))
        def _():
            copy.wait_send()

    def ring_sent(t):
        piece = x * 8 + nth(t)
        ring(2 * t, piece, x_send, 1).wait_send()
        ring(2 * t + 1, piece, x_send, 3).wait_send()

    def relay_sent(t):
        ring(2 * t, left + nth(2 * t), r_send, 1).wait_send()
        ring(2 * t + 1, right + nth(2 * t + 1), r_send, 3).wait_send()

    last_copy.wait()
    each(0, 8, kv_sent)
    each(1, 16, lambda e: count_copy(e).wait_send())
    each(1, 32, lambda n: q_copy(n).wait_send())
    each(0, 8, ring_sent)
    each(0, 4, relay_sent)
    each(0, 16, lambda n: pltpu.make_async_copy(cnts, cnt_out.at[n], c_recv.at[n]).wait())
    each(0, 32, lambda n: pltpu.make_async_copy(qs.at[0], q_out.at[n], q_recv.at[n]).wait())


def project(tokens, count, gain, bias, w_qkv, w_out):
    times, slots, width = tokens.shape
    rows = slots * SLOT
    bf16, i32 = jnp.bfloat16, jnp.int32
    dma = pltpu.SemaphoreType.DMA
    return pl.pallas_call(
        project_kernel,
        out_shape=(VMEM((32, rows // 2, 128), bf16),
                   VMEM((32, rows, 128), bf16),
                   VMEM((16, 1, 128), i32),
                   VMEM(tokens.shape, bf16), VMEM(w_out.shape, bf16)),
        in_specs=[spec(pltpu.HBM), spec(SMEM), spec(VMEM), spec(VMEM), spec(pltpu.HBM), spec(pltpu.HBM)],
        out_specs=(spec(ANY), spec(ANY), spec(ANY), spec(VMEM), spec(ANY)),
        scratch_shapes=[
            VMEM(w_qkv.shape, bf16), VMEM((width // 128, rows, 128), jnp.float32), VMEM((rows, width), bf16),
            VMEM((HEADS, rows, 128), bf16), VMEM((HEADS, rows // 2, 128), bf16), VMEM((1, 128), i32),
            dma((5,)), dma((8,)), dma((8,)), dma((32,)), dma((32,)), dma((16,)), dma((16,)),
            dma((16,)), dma((8,)), dma((32,)),
        ],
        compiler_params=pltpu.CompilerParams(collective_id=0, has_side_effects=True),
        name="project",
    )(tokens, count, gain, bias, w_qkv, w_out)


def attention_kernel(cnt_ref, q_hbm, kv_hbm, o_ref, lse_ref, kvc, qc, vt, qt, acc, of, at_q, q_sem, k_sem, *held, times):
    base = (lax.axis_index("space") // 4) * 4
    kv_flat = kvc.reshape(kvc.shape[0] * SLOT, 128)
    q_flat = qc.reshape(qc.shape[0] * SLOT, 128)
    step_keys = KB

    def q_copy(j, l, unit):
        return pltpu.make_async_copy(
            q_hbm.at[:, l, pl.ds((j % 2) * SLOT, SLOT), :], qc.at[pl.ds(unit, 8)], q_sem.at[j * 4 + l])

    def k_copy(xs, l, j, unit):
        return pltpu.make_async_copy(
            kv_hbm.at[xs, :, l, pl.ds(j * SLOT, SLOT), :], kvc.at[pl.ds(unit, 2)], k_sem.at[(xs * 4 + l) * 4 + j])

    def start_keys(n, unit):
        count = cnt_ref[n, 0, 0]
        for j in range(4):
            @pl.when(j < count)
            def _(j=j):
                k_copy(n // 4, n % 4, j, unit + 2 * j).start()
        return unit + 2 * count

    key_units = lax.fori_loop(0, 16, start_keys, jnp.int32(0))
    fill = -(-step_keys // (2 * SLOT))

    def fill_copy(n):
        return pltpu.make_async_copy(
            kv_hbm.at[0, :, 0, pl.ds(0, SLOT), :], kvc.at[pl.ds(key_units + 2 * n, 2)], k_sem.at[64 + n])

    each(0, fill, lambda n: fill_copy(n).start())

    unit = jnp.int32(0)
    for j in range(4):
        if j == 2:
            low_units = unit
        for l in range(4):
            live = j < cnt_ref[base + l, 0, 0]
            at_q[j * 4 + l] = jnp.where(live, unit, 0)

            @pl.when(live)
            def _(j=j, l=l, unit=unit):
                q_copy(j, l, unit).start()
            unit = unit + jnp.where(live, 8, 0)
    query_rows = unit * SLOT
    query_tiles = (query_rows + QB - 1) // QB
    key_rows = key_units * SLOT
    key_steps = (key_rows + step_keys - 1) // step_keys

    def wait_keys(n, c):
        count = cnt_ref[n, 0, 0]
        for j in range(4):
            @pl.when(j < count)
            def _(j=j):
                k_copy(n // 4, n % 4, j, 0).wait()
        return c

    lax.fori_loop(0, 16, wait_keys, 0)
    each(0, fill, lambda n: fill_copy(n).wait())

    key_at = lax.broadcasted_iota(jnp.int32, (HD, KB), 1)
    row16 = lax.broadcasted_iota(jnp.int32, (16, KB), 0)

    def shape_keys(b, longest):
        turned = jnp.transpose(kv_flat[pl.ds(pl.multiple_of(b * KB, KB), KB), :].astype(jnp.float32))
        index = key_at + b * KB
        live = (index % SLOT < times) & (index < key_rows)
        vt[b, 0:HD, :] = jnp.where(live, turned[HD:], 0.0).astype(jnp.bfloat16)
        vt[b, HD:HD + 16, :] = jnp.where(live[:16] & (row16 == 0), 1.0, 0.0).astype(jnp.bfloat16)
        keys = turned[:HD]
        return jnp.maximum(longest, jnp.sum(keys * keys, axis=0, keepdims=True))

    longest_key = lax.fori_loop(0, key_steps, shape_keys, jnp.zeros((1, KB), jnp.float32))

    for j in range(4):
        for l in range(4):
            @pl.when(j < cnt_ref[base + l, 0, 0])
            def _(j=j, l=l):
                q_copy(j, l, 0).wait()

    col = lax.broadcasted_iota(jnp.int32, (HD, QB), 1)
    low_rows = low_units * SLOT

    def shape_queries(t, longest):
        turned = jnp.transpose(q_flat[pl.ds(pl.multiple_of(t * QB, QB), QB), :].astype(jnp.float32))
        index = col + t * QB
        query = jnp.where(index < low_rows, turned[:HD], turned[HD:])
        query = jnp.where(index < query_rows, query, 0.0)
        qt[t, 0:HD, :] = query.astype(jnp.bfloat16)
        qt[t, HD:, :] = jnp.zeros((HD, QB), jnp.bfloat16)
        return jnp.maximum(longest, jnp.sum(query * query, axis=0, keepdims=True))

    longest_query = lax.fori_loop(0, query_tiles, shape_queries, jnp.zeros((1, QB), jnp.float32))
    safe = jnp.max(longest_key) * jnp.max(longest_query) < SAFE * SAFE

    def put(t, total, best):
        weight_sum = total[HD:HD + 1, :]
        out = total[0:HD, :] / weight_sum
        lse = jnp.broadcast_to(best + jnp.log2(weight_sum), (HD, QB))
        low = col + t * QB < low_rows
        both = jnp.concatenate([jnp.where(low, out, lse), jnp.where(low, lse, out)], axis=0)
        of[pl.ds(pl.multiple_of(t * QB, QB), QB), :] = jnp.transpose(both)

    def block_scores(b, t):
        keys = kv_flat[pl.ds(pl.multiple_of(b * KB, KB), KB), :]
        return jnp.dot(keys, qt[t], preferred_element_type=jnp.float32)

    def clear(t):
        acc[t] = jnp.zeros((HD + 16, QB), jnp.float32)

    def after(item):
        t, b = item
        turn = b + 1 == key_steps
        return jnp.minimum(jnp.where(turn, t + 1, t), query_tiles), jnp.where(turn, 0, b + 1)

    def plain(i, carry):
        before, now = carry
        then = now[-1]
        later = []
        for u in range(UN):
            t, b = before[u]
            acc[t] += jnp.dot(vt[b], held[u][...], preferred_element_type=jnp.float32)
            t, b = now[u]
            held[u][...] = jnp.exp2(block_scores(b, t)).astype(jnp.bfloat16)
            then = after(then)
            later.append(then)
        return now, tuple(later)

    def plain_all():
        each(0, query_tiles, clear)
        first = [(jnp.int32(0), jnp.int32(0))]
        for _ in range(UN - 1):
            first.append(after(first[-1]))
        nowhere = ((query_tiles, jnp.int32(0)),) * UN
        steps = (query_tiles * key_steps + UN - 1) // UN + 1
        lax.fori_loop(0, steps, plain, (nowhere, tuple(first)))

        each(0, query_tiles, lambda t: put(t, acc[t], 0.0))

    def shifted_tile(t):
        def step(b, carry):
            best, total = carry
            scores = block_scores(b, t)
            best_next = jnp.maximum(best, jnp.max(scores, axis=0, keepdims=True))
            weights = jnp.exp2(scores - best_next).astype(jnp.bfloat16)
            total = total * jnp.exp2(best - best_next) + jnp.dot(
                vt[b], weights, preferred_element_type=jnp.float32)
            return best_next, total

        best, total = lax.fori_loop(
            0, key_steps, step,
            (jnp.full((1, QB), DEAD, jnp.float32), jnp.zeros((HD + 16, QB), jnp.float32)))
        put(t, total, best)

    @pl.when(safe)
    def _():
        plain_all()

    @pl.when(jnp.logical_not(safe))
    def _():
        each(0, query_tiles, shifted_tile)

    lane = lax.broadcasted_iota(jnp.int32, (SLOT, 128), 1)
    in_low = lane < HD

    def give_back(i, sizes):
        f, l = i % 8, ((i // 8) % 2) * 2 + i // 16
        sizes_next = []
        for j in range(2):
            first = of[pl.ds(pl.multiple_of((at_q[j * 4 + l] + f) * SLOT, 8), SLOT), :]
            second = of[pl.ds(pl.multiple_of((at_q[j * 4 + 8 + l] + f) * SLOT, 8), SLOT), :]
            o_ref[i, j * SLOT:j * SLOT + SLOT, :] = jnp.where(in_low, first, second).astype(jnp.bfloat16)
            sizes_next.append(jnp.where(lane % HD == i, jnp.where(in_low, second, first), sizes[j]))
        return tuple(sizes_next)

    sizes = lax.fori_loop(0, 32, give_back, (jnp.zeros((SLOT, 128), jnp.float32),) * 2)
    turned = jnp.transpose(jnp.concatenate([*sizes, jnp.zeros((128 - 2 * SLOT, 128), jnp.float32)], axis=0))
    lse_ref[0] = turned[HD:HD + 32]
    lse_ref[1] = turned[0:32]


def attention(counts, q_all, kv_all, times):
    sources, half_rows, _ = q_all.shape
    q_units, k_units = 4 * sources, 4 * sources
    q_rows = (q_units * SLOT + QB - 1) // QB * QB
    step = KB
    k_rows = (k_units * SLOT + step - 1) // step * step
    fill = -(-step // (2 * SLOT))
    dma = pltpu.SemaphoreType.DMA
    return pl.pallas_call(
        functools.partial(attention_kernel, times=times),
        out_shape=(VMEM((sources, half_rows, 128), jnp.bfloat16),
                   VMEM((2, sources, 128), jnp.float32)),
        in_specs=[spec(SMEM), spec(ANY), spec(ANY)],
        out_specs=(spec(VMEM), spec(VMEM)),
        scratch_shapes=[
            VMEM((k_units + 2 * fill, SLOT, 128), jnp.bfloat16),
            VMEM((q_rows // SLOT + 1, SLOT, 128), jnp.bfloat16),
            VMEM((k_rows // KB, HD + 16, KB), jnp.bfloat16),
            VMEM((q_rows // QB + 1, 128, QB), jnp.bfloat16),
            VMEM((q_rows // QB + 1, HD + 16, QB), jnp.float32),
            VMEM((q_rows, 128), jnp.float32),
            SMEM((16,), jnp.int32),
            dma((16,)), dma((64 + fill,)),
            *[VMEM((KB, QB), jnp.bfloat16) for _ in range(UN)],
        ],
        compiler_params=pltpu.CompilerParams(vmem_limit_bytes=32 << 20),
        name="attention",
    )(counts, near(q_all.reshape(8, 4, half_rows, 128)),
      near(kv_all.reshape(4, 2, 4, 2 * half_rows, 128)))


def return_kernel(o_ref, lse_ref, back_ref, back_lse, mine, theirs, size_mine, size_theirs, both, size_both,
                  in_sem, t_send, t_recv, o_send, o_recv, l_send, l_recv):
    f, _, x, loc = place()
    hi, core = loc // 2, loc % 2
    half_rows = o_ref.shape[1]
    barrier = pltpu.get_barrier_semaphore()

    def greet(frame, there):
        pl.semaphore_signal(barrier, inc=1, device_id={"frame": frame, "space": x * 4 + there},
                            device_id_type=pl.DeviceIdType.MESH)

    greet(f, hi * 2 + 1 - core)
    each(1, 16, lambda n: greet((f + n // 2) % 8, ((hi + n) % 2) * 2 + core))

    keep = core * 16
    give = 16 - keep
    loads = [
        pltpu.make_async_copy(o_ref.at[pl.ds(keep, 16)], mine, in_sem.at[0]),
        pltpu.make_async_copy(lse_ref.at[:, pl.ds(keep, 16), :], size_mine, in_sem.at[1]),
    ]
    for copy in loads:
        copy.start()

    def twin(src, dst, n):
        return remote(src, dst, t_send.at[n], t_recv.at[n], f, x * 4 + hi * 2 + 1 - core)

    pl.semaphore_wait(barrier, 16)
    shares = [twin(lse_ref.at[:, pl.ds(give, 16), :], size_theirs, 0)]
    for n in range(2):
        shares.append(twin(o_ref.at[pl.ds(give + 8 * n, 8)], theirs.at[pl.ds(8 * n, 8)], 1 + n))
    for copy in shares:
        copy.start()
    for copy in loads:
        copy.wait()
    shares[0].wait_recv()

    turned = []
    for n in range(2):
        one, two = size_mine[n], size_theirs[n]
        top = jnp.maximum(one, two)
        one, two = jnp.exp2(one - top), jnp.exp2(two - top)
        total = one + two
        whole = top + jnp.log2(total)
        for r in range(16):
            size_both[r, n:n + 1, :] = whole[r:r + 1]
        turned.append(jnp.transpose(
            jnp.concatenate([one / total, two / total, jnp.zeros((96, 128), jnp.float32)], axis=0)))
    low = lax.broadcasted_iota(jnp.int32, (half_rows, 128), 1) < HD

    me = hi * 8 + f

    def copies(n):
        frame, there = (f + n // 2) % 8, (hi + n) % 2
        r = there * 8 + frame
        space = x * 4 + there * 2 + core
        return (remote(both.at[r], back_ref.at[me], o_send.at[n], o_recv.at[me], frame, space),
                remote(size_both.at[r], back_lse.at[me], l_send.at[n], l_recv.at[me], frame, space))

    def start(n):
        for copy in copies(n):
            copy.start()

    def sent(n):
        for copy in copies(n):
            copy.wait_send()

    for n in range(2):
        shares[1 + n].wait_recv()
        for r in range(8 * n, 8 * n + 8):
            one = jnp.where(low, turned[0][0:half_rows, r:r + 1], turned[1][0:half_rows, r:r + 1])
            two = jnp.where(low, turned[0][0:half_rows, 16 + r:17 + r], turned[1][0:half_rows, 16 + r:17 + r])
            both[r] = (mine[r].astype(jnp.float32) * one + theirs[r].astype(jnp.float32) * two).astype(jnp.bfloat16)

    each(1, 16, start)
    own = hi * 8 + f
    pltpu.make_async_copy(both.at[own], back_ref.at[me], o_recv.at[me]).start()
    pltpu.make_async_copy(size_both.at[own], back_lse.at[me], l_recv.at[me]).start()
    for copy in shares:
        copy.wait_send()
    each(1, 16, sent)
    each(0, 16, lambda n: pltpu.make_async_copy(both.at[0], back_ref.at[n], o_recv.at[n]).wait())
    each(0, 16, lambda n: pltpu.make_async_copy(size_both.at[0], back_lse.at[n], l_recv.at[n]).wait())


def give_results(partial, sizes):
    dma = pltpu.SemaphoreType.DMA
    half_rows = partial.shape[1]
    held = VMEM((16, half_rows, 128), partial.dtype)
    return pl.pallas_call(
        return_kernel,
        out_shape=(VMEM((16, half_rows, 128), partial.dtype),
                   VMEM((16, 2, 128), sizes.dtype)),
        in_specs=[spec(ANY), spec(ANY)],
        out_specs=(spec(ANY), spec(ANY)),
        scratch_shapes=[
            held, held, VMEM((2, 16, 128), sizes.dtype), VMEM((2, 16, 128), sizes.dtype),
            held, VMEM((16, 2, 128), sizes.dtype),
            dma((2,)), dma((3,)), dma((3,)), dma((16,)), dma((16,)), dma((16,)), dma((16,))],
        compiler_params=pltpu.CompilerParams(
            collective_id=1, has_side_effects=True, vmem_limit_bytes=16 << 20),
        name="give_results",
    )(near(partial), near(sizes))


def finish_kernel(tok_ref, cnt_ref, back_ref, lse_ref, w_ref, o_ref, att, ys):
    times, slots, width = tok_ref.shape
    half = slots * SLOT // 2
    rows = slots * SLOT

    def shares(n):
        sizes = [lse_ref[p * 8:p * 8 + 8, n, :] for p in range(2)]
        top = jnp.maximum(sizes[0], sizes[1])
        powers = [jnp.exp2(v - top) for v in sizes]
        total = powers[0] + powers[1]
        return jnp.transpose(
            jnp.concatenate([v / total for v in powers] + [jnp.zeros((112, 128), jnp.float32)], axis=0))

    first, second = shares(0), shares(1)
    low = lax.broadcasted_iota(jnp.int32, (half, 128), 1) < HD

    def merged(h):
        out = jnp.zeros((half, 128), jnp.float32)
        for p in range(2):
            n = p * 8 + h
            share = jnp.where(low, first[0:half, n:n + 1], second[0:half, n:n + 1])
            out = out + back_ref[n].astype(jnp.float32) * share
        return out

    for j in range(HEADS // 2):
        a, b = merged(2 * j), merged(2 * j + 1)
        cols = slice(128 * j, 128 * j + 128)
        att[0:half, cols] = jnp.where(low, a, pltpu.roll(b, HD, 1)).astype(jnp.bfloat16)
        att[half:rows, cols] = jnp.where(low, pltpu.roll(a, HD, 1), b).astype(jnp.bfloat16)
    for c in range(width // 256):
        cols = slice(256 * c, 256 * c + 256)
        mixed = jnp.dot(att[...], w_ref[:, cols], preferred_element_type=jnp.float32)
        for i in range(slots):
            for e in range(2):
                ys[2 * c + e, pl.ds(i, SLOT, stride=slots), :] = (
                    mixed[i * SLOT:i * SLOT + SLOT, 128 * e:128 * e + 128])
    live = lax.broadcasted_iota(jnp.int32, (slots, width), 0) < cnt_ref[0]
    for t in range(times):
        mixed = jnp.concatenate([ys[c, t * slots:t * slots + slots, :] for c in range(width // 128)], axis=1)
        value = tok_ref[t].astype(jnp.float32) + mixed
        o_ref[t] = jnp.where(live, value, 0.0).astype(jnp.bfloat16)


def finish(tokens, count, back, sizes, w_out):
    times, slots, width = tokens.shape
    rows = slots * SLOT
    return pl.pallas_call(
        finish_kernel,
        out_shape=jax.ShapeDtypeStruct(tokens.shape, tokens.dtype),
        in_specs=[spec(VMEM), spec(SMEM), spec(VMEM), spec(VMEM), spec(VMEM)],
        out_specs=spec(VMEM),
        scratch_shapes=[VMEM((rows, w_out.shape[0]), jnp.bfloat16), VMEM((width // 128, rows, 128), jnp.float32)],
        compiler_params=pltpu.CompilerParams(vmem_limit_bytes=16 << 20),
        name="finish",
    )(near(tokens), count, near(back), near(sizes), near(w_out))


def on_device(tokens, tube_count, ln_gain, ln_bias, w_qkv, w_out):
    tokens = jnp.transpose(tokens, (1, 0, 2))
    q_all, kv_all, counts, tokens, w_out = project(
        tokens, tube_count, ln_gain.reshape(1, -1), ln_bias.reshape(1, -1), w_qkv, w_out)
    partial, sizes = attention(counts, q_all, kv_all, tokens.shape[0])
    mixed = finish(tokens, tube_count, *give_results(partial, sizes), w_out)
    return jnp.transpose(mixed, (1, 0, 2))


def solution(mesh):
    in_specs = (P("space", "frame", None), P("space"), P(), P(), P(), P())
    return jax.shard_map(
        on_device, mesh=mesh, in_specs=in_specs, out_specs=P("space", "frame", None), check_vma=False)
```

```python
import functools

import jax
import jax.numpy as jnp
from jax import lax
from jax.experimental import pallas as pl
from jax.experimental.pallas import tpu as pltpu
from jax.sharding import PartitionSpec as P

HEADS = 8
HD = 64
SLOT = 40
KB = 256
UN = 8
QB = 512
DEAD = -1e30
Q_AFTER = 2
SAFE = 100.0
EPSILON = 1e-06
SCALE = 1.4426950408889634 / 8.0
ANY = pl.ANY
VMEM = pltpu.VMEM
SMEM = pltpu.SMEM


def spec(space):
    return pl.BlockSpec(memory_space=space)


def near(array):
    return pltpu.with_memory_space_constraint(array, VMEM)


def place():
    f, s = lax.axis_index("frame"), lax.axis_index("space")
    return f, s, div(s, 4), rem(s, 4)


def remote(src, dst, send, recv, frame, space):
    return pltpu.make_async_remote_copy(
        src_ref=src, dst_ref=dst, send_sem=send, recv_sem=recv,
        device_id={"frame": frame, "space": space}, device_id_type=pl.DeviceIdType.MESH)


def rem(a, n):
    return lax.rem(a, jnp.int32(n))


def div(a, n):
    return lax.div(a, jnp.int32(n))


def each(lo, hi, body):
    def step(i, c):
        body(i)
        return c
    lax.fori_loop(lo, hi, step, 0)


def project_kernel(tok_in, cnt_ref, gain_ref, bias_ref, w_ref, w_last, q_out, kv_out, cnt_out, tok_ref, w_next,
                   w_v, xs, nb, kvs, qs, cnts,
                   w_sem, kv_send, kv_recv, q_send, q_recv, c_send, c_recv, x_send, r_send, pass_recv, rest_recv):
    f, s, x, loc = place()
    times, slots, width = tok_ref.shape
    inner = HEADS * HD

    tok_copy = pltpu.make_async_copy(tok_in, tok_ref, w_sem.at[3])
    tok_copy.start()
    last_copy = pltpu.make_async_copy(w_last, w_next, w_sem.at[4])
    copies = []
    for n, at in enumerate((inner, 2 * inner, 0)):
        cols = pl.ds(at, inner)
        copy = pltpu.make_async_copy(w_ref.at[:, cols], w_v.at[:, cols], w_sem.at[n])
        copy.start()
        copies.append(copy)

    barrier = pltpu.get_barrier_semaphore()

    def greet(frame, space):
        pl.semaphore_signal(barrier, inc=1, device_id={"frame": frame, "space": space},
                            device_id_type=pl.DeviceIdType.MESH)

    each(1, 32, lambda n: greet(rem(f + div(n, 4), 8), x * 4 + rem(loc + n, 4)))
    each(4, 16, lambda n: greet(f, rem(x * 4 + n, 16)))

    cnts[...] = jnp.full(cnts.shape, cnt_ref[0], jnp.int32)

    tok_copy.wait()
    for t in range(SLOT):
        values = tok_ref[t % times].astype(jnp.float32)
        for c in range(width // 128):
            xs[c, t * slots:t * slots + slots, :] = values[:, 128 * c:128 * c + 128]
    for i in range(slots):
        values = jnp.concatenate(
            [xs[c, pl.ds(i, SLOT, stride=slots), :] for c in range(width // 128)], axis=1)
        center = values - jnp.mean(values, axis=-1, keepdims=True)
        spread = jnp.mean(center * center, axis=-1, keepdims=True)
        normed = center * lax.rsqrt(spread + EPSILON) * gain_ref[...] + bias_ref[...]
        nb[i * SLOT:i * SLOT + SLOT, :] = normed.astype(jnp.bfloat16)

    rows_all = slots * SLOT
    half = rows_all // 2
    low = lax.broadcasted_iota(jnp.int32, (rows_all, 128), 1) < HD
    low_half = lax.broadcasted_iota(jnp.int32, (half, 128), 1) < HD

    copies[0].wait()
    copies[1].wait()
    for g in range(2):
        k4 = jnp.dot(nb[...], w_v[:, inner + 256 * g:inner + 256 * g + 256], preferred_element_type=jnp.float32)
        v4 = jnp.dot(nb[...], w_v[:, 2 * inner + 256 * g:2 * inner + 256 * g + 256],
                     preferred_element_type=jnp.float32)
        for j in range(2):
            k2, v2 = k4[:, 128 * j:128 * j + 128], v4[:, 128 * j:128 * j + 128]
            h = 4 * g + 2 * j
            kvs[h] = jnp.where(low, k2, pltpu.roll(v2, HD, 1)).astype(jnp.bfloat16)
            kvs[h + 1] = jnp.where(low, pltpu.roll(k2, HD, 1), v2).astype(jnp.bfloat16)

    part = div(f, 2)
    mine = rem(f, 2) * 4 + loc
    source = x * 8 + mine
    pl.semaphore_wait(barrier, 43)

    def kv_copy(d):
        h = rem(f + d + 2 * loc, 8)
        stays = (h == f) & (part == loc)
        return stays, h, remote(
            kvs.at[h], kv_out.at[source], kv_send.at[0], kv_recv.at[mine], h, x * 4 + part)

    def kv_start(d):
        stays, h, copy = kv_copy(d)

        @pl.when(stays)
        def _():
            pltpu.make_async_copy(kvs.at[h], kv_out.at[source], kv_recv.at[mine]).start()

        @pl.when(jnp.logical_not(stays))
        def _():
            copy.start()

    each(0, 8, kv_start)

    def count_copy(e):
        return remote(cnts, cnt_out.at[s], c_send.at[0], c_recv.at[0], f, rem(s + e, 16))

    each(1, 16, lambda e: count_copy(e).start())
    pltpu.make_async_copy(cnts, cnt_out.at[s], c_recv.at[0]).start()

    copies[2].wait()
    last_copy.start()
    for g in range(2):
        q4 = jnp.dot(nb[...], w_v[:, 256 * g:256 * g + 256], preferred_element_type=jnp.float32) * SCALE
        for j in range(2):
            q2 = q4[:, 128 * j:128 * j + 128]
            h = 4 * g + 2 * j
            qs[h] = jnp.where(low_half, q2[:half], pltpu.roll(q2[half:], HD, 1)).astype(jnp.bfloat16)
            qs[h + 1] = jnp.where(low_half, pltpu.roll(q2[:half], HD, 1), q2[half:]).astype(jnp.bfloat16)

    me = f * 4 + loc

    def q_copy(n):
        h = rem(f + div(n, 4), 8)
        return remote(qs.at[h], q_out.at[me], q_send.at[0], q_recv.at[0], h, x * 4 + rem(loc + n, 4))

    def ring(piece, send, recv, step):
        return remote(kv_out.at[piece], kv_out.at[piece], send.at[0], recv, f, rem(x + step, 4) * 4 + loc)

    def nth(t):
        u = rem(f - 2 * loc - t + 16, 8)
        return rem(u, 2) * 4 + div(u, 2)

    right, left = rem(x + 1, 4) * 8, rem(x + 3, 4) * 8

    def landed(sem, ref):
        pltpu.make_async_copy(ref, ref, sem).wait()

    def to_right(t, piece):
        even = rem(t, 2) == 0

        @pl.when(even)
        def _():
            ring(piece, x_send, pass_recv.at[t], 1).start()

        @pl.when(jnp.logical_not(even))
        def _():
            ring(piece, x_send, rest_recv.at[0], 1).start()

    def to_left(t, piece):
        odd = rem(t, 2) == 1

        @pl.when(odd)
        def _():
            ring(piece, x_send, pass_recv.at[t], 3).start()

        @pl.when(jnp.logical_not(odd))
        def _():
            ring(piece, x_send, rest_recv.at[0], 3).start()

    def arrived(t):
        i = nth(t)
        piece = x * 8 + i
        landed(kv_recv.at[i], kv_out.at[piece])
        to_right(t, piece)
        to_left(t, piece)

    each(0, Q_AFTER, arrived)
    each(1, 32, lambda n: q_copy(n).start())
    pltpu.make_async_copy(qs.at[f], q_out.at[me], q_recv.at[0]).start()
    each(Q_AFTER, 8, arrived)

    def relay(t):
        piece = left + nth(2 * t)
        landed(pass_recv.at[2 * t], kv_out.at[piece])
        ring(piece, r_send, rest_recv.at[0], 1).start()
        piece = right + nth(2 * t + 1)
        landed(pass_recv.at[2 * t + 1], kv_out.at[piece])
        ring(piece, r_send, rest_recv.at[0], 3).start()

    each(0, 4, relay)

    last_copy.wait()
    landed(kv_send.at[0], kv_out.at[pl.ds(0, 7)])

    @pl.when(part != loc)
    def _():
        landed(kv_send.at[0], kv_out.at[0])

    landed(c_send.at[0], cnt_out.at[pl.ds(0, 15)])
    landed(q_send.at[0], q_out.at[pl.ds(0, 31)])
    landed(x_send.at[0], kv_out.at[pl.ds(0, 16)])
    landed(r_send.at[0], kv_out.at[pl.ds(0, 8)])
    landed(c_recv.at[0], cnt_out)
    landed(q_recv.at[0], q_out)
    landed(rest_recv.at[0], kv_out.at[pl.ds(0, 16)])


def project(tokens, count, gain, bias, w_qkv, w_out):
    times, slots, width = tokens.shape
    rows = slots * SLOT
    bf16, i32 = jnp.bfloat16, jnp.int32
    dma = pltpu.SemaphoreType.DMA
    return pl.pallas_call(
        project_kernel,
        out_shape=(VMEM((32, rows // 2, 128), bf16),
                   VMEM((32, rows, 128), bf16),
                   VMEM((16, 1, 128), i32),
                   VMEM(tokens.shape, bf16), VMEM(w_out.shape, bf16)),
        in_specs=[spec(pltpu.HBM), spec(SMEM), spec(VMEM), spec(VMEM), spec(pltpu.HBM), spec(pltpu.HBM)],
        out_specs=(spec(ANY), spec(ANY), spec(ANY), spec(VMEM), spec(ANY)),
        scratch_shapes=[
            VMEM(w_qkv.shape, bf16), VMEM((width // 128, rows, 128), jnp.float32), VMEM((rows, width), bf16),
            VMEM((HEADS, rows, 128), bf16), VMEM((HEADS, rows // 2, 128), bf16), VMEM((1, 128), i32),
            dma((5,)), dma((1,)), dma((8,)), dma((1,)), dma((1,)), dma((1,)), dma((1,)),
            dma((1,)), dma((1,)), dma((8,)), dma((1,)),
        ],
        compiler_params=pltpu.CompilerParams(collective_id=0, has_side_effects=True),
        name="project",
    )(tokens, count, gain, bias, w_qkv, w_out)


def attention_kernel(cnt_ref, q_ref, kv_ref, o_ref, lse_ref, kvc, qc, vt, qt, acc, of, at_q, *held, times):
    base = (lax.axis_index("space") // 4) * 4
    kv_flat = kvc.reshape(kvc.shape[0] * SLOT, 128)
    q_flat = qc.reshape(qc.shape[0] * SLOT, 128)
    step_keys = KB

    def take_keys(n, unit):
        for j in range(4):
            for sub in range(2):
                kvc[unit + 2 * j + sub] = kv_ref[n // 4, sub, n % 4, j * SLOT:j * SLOT + SLOT, :]
        return unit + 2 * cnt_ref[n, 0, 0]

    unit = jnp.int32(0)
    for n in range(16):
        unit = take_keys(n, unit)
    key_units = unit
    for n in range(-(-step_keys // SLOT)):
        kvc[key_units + n] = kv_ref[0, 0, 0, 0:SLOT, :]

    unit = jnp.int32(0)
    for j in range(4):
        if j == 2:
            low_units = unit
        for l in range(4):
            live = j < cnt_ref[base + l, 0, 0]
            at_q[j * 4 + l] = jnp.where(live, unit, 0)
            for f in range(8):
                qc[unit + f] = q_ref[f, l, (j % 2) * SLOT:(j % 2) * SLOT + SLOT, :]
            unit = unit + jnp.where(live, 8, 0)
    query_rows = unit * SLOT
    query_tiles = (query_rows + QB - 1) // QB
    key_rows = key_units * SLOT
    key_steps = (key_rows + step_keys - 1) // step_keys

    key_at = lax.broadcasted_iota(jnp.int32, (HD, KB), 1)
    row16 = lax.broadcasted_iota(jnp.int32, (16, KB), 0)

    def shape_keys(b, longest):
        turned = jnp.transpose(kv_flat[pl.ds(pl.multiple_of(b * KB, KB), KB), :].astype(jnp.float32))
        index = key_at + b * KB
        live = (index % SLOT < times) & (index < key_rows)
        vt[b, 0:HD, :] = jnp.where(live, turned[HD:], 0.0).astype(jnp.bfloat16)
        vt[b, HD:HD + 16, :] = jnp.where(live[:16] & (row16 == 0), 1.0, 0.0).astype(jnp.bfloat16)
        keys = turned[:HD]
        return jnp.maximum(longest, jnp.sum(keys * keys, axis=0, keepdims=True))

    longest_key = lax.fori_loop(0, key_steps, shape_keys, jnp.zeros((1, KB), jnp.float32))

    col = lax.broadcasted_iota(jnp.int32, (HD, QB), 1)
    low_rows = low_units * SLOT

    def shape_queries(t, longest):
        turned = jnp.transpose(q_flat[pl.ds(pl.multiple_of(t * QB, QB), QB), :].astype(jnp.float32))
        index = col + t * QB
        query = jnp.where(index < low_rows, turned[:HD], turned[HD:])
        query = jnp.where(index < query_rows, query, 0.0)
        qt[t, 0:HD, :] = query.astype(jnp.bfloat16)
        qt[t, HD:, :] = jnp.zeros((HD, QB), jnp.bfloat16)
        return jnp.maximum(longest, jnp.sum(query * query, axis=0, keepdims=True))

    longest_query = lax.fori_loop(0, query_tiles, shape_queries, jnp.zeros((1, QB), jnp.float32))
    safe = jnp.max(longest_key) * jnp.max(longest_query) < SAFE * SAFE

    def put(t, total, best):
        weight_sum = total[HD:HD + 1, :]
        out = total[0:HD, :] / weight_sum
        lse = jnp.broadcast_to(best + jnp.log2(weight_sum), (HD, QB))
        low = col + t * QB < low_rows
        both = jnp.concatenate([jnp.where(low, out, lse), jnp.where(low, lse, out)], axis=0)
        of[pl.ds(pl.multiple_of(t * QB, QB), QB), :] = jnp.transpose(both)

    def block_scores(b, t):
        keys = kv_flat[pl.ds(pl.multiple_of(b * KB, KB), KB), :]
        return jnp.dot(keys, qt[t], preferred_element_type=jnp.float32)

    def clear(t):
        acc[t] = jnp.zeros((HD + 16, QB), jnp.float32)

    def after(item):
        t, b = item
        turn = b + 1 == key_steps
        return jnp.minimum(jnp.where(turn, t + 1, t), query_tiles), jnp.where(turn, 0, b + 1)

    def plain(i, carry):
        before, now = carry
        then = now[-1]
        later = []
        for u in range(UN):
            t, b = before[u]
            acc[t] += jnp.dot(vt[b], held[u][...], preferred_element_type=jnp.float32)
            t, b = now[u]
            held[u][...] = jnp.exp2(block_scores(b, t)).astype(jnp.bfloat16)
            then = after(then)
            later.append(then)
        return now, tuple(later)

    def plain_all():
        each(0, query_tiles, clear)
        first = [(jnp.int32(0), jnp.int32(0))]
        for _ in range(UN - 1):
            first.append(after(first[-1]))
        nowhere = ((query_tiles, jnp.int32(0)),) * UN
        steps = (query_tiles * key_steps + UN - 1) // UN + 1
        lax.fori_loop(0, steps, plain, (nowhere, tuple(first)))

        each(0, query_tiles, lambda t: put(t, acc[t], 0.0))

    def shifted_tile(t):
        def step(b, carry):
            best, total = carry
            scores = block_scores(b, t)
            best_next = jnp.maximum(best, jnp.max(scores, axis=0, keepdims=True))
            weights = jnp.exp2(scores - best_next).astype(jnp.bfloat16)
            total = total * jnp.exp2(best - best_next) + jnp.dot(
                vt[b], weights, preferred_element_type=jnp.float32)
            return best_next, total

        best, total = lax.fori_loop(
            0, key_steps, step,
            (jnp.full((1, QB), DEAD, jnp.float32), jnp.zeros((HD + 16, QB), jnp.float32)))
        put(t, total, best)

    @pl.when(safe)
    def _():
        plain_all()

    @pl.when(jnp.logical_not(safe))
    def _():
        each(0, query_tiles, shifted_tile)

    lane = lax.broadcasted_iota(jnp.int32, (SLOT, 128), 1)
    in_low = lane < HD

    def give_back(i, sizes):
        f, l = i % 8, ((i // 8) % 2) * 2 + i // 16
        sizes_next = []
        for j in range(2):
            first = of[pl.ds(pl.multiple_of((at_q[j * 4 + l] + f) * SLOT, 8), SLOT), :]
            second = of[pl.ds(pl.multiple_of((at_q[j * 4 + 8 + l] + f) * SLOT, 8), SLOT), :]
            o_ref[i, j * SLOT:j * SLOT + SLOT, :] = jnp.where(in_low, first, second).astype(jnp.bfloat16)
            sizes_next.append(jnp.where(lane % HD == i, jnp.where(in_low, second, first), sizes[j]))
        return tuple(sizes_next)

    sizes = lax.fori_loop(0, 32, give_back, (jnp.zeros((SLOT, 128), jnp.float32),) * 2)
    turned = jnp.transpose(jnp.concatenate([*sizes, jnp.zeros((128 - 2 * SLOT, 128), jnp.float32)], axis=0))
    lse_ref[0] = turned[HD:HD + 32]
    lse_ref[1] = turned[0:32]


def attention(counts, q_all, kv_all, times):
    sources, half_rows, _ = q_all.shape
    q_units, k_units = 4 * sources, 4 * sources
    q_rows = (q_units * SLOT + QB - 1) // QB * QB
    step = KB
    k_rows = (k_units * SLOT + step - 1) // step * step
    fill = -(-step // SLOT)
    return pl.pallas_call(
        functools.partial(attention_kernel, times=times),
        out_shape=(VMEM((sources, half_rows, 128), jnp.bfloat16),
                   VMEM((2, sources, 128), jnp.float32)),
        in_specs=[spec(SMEM), spec(VMEM), spec(VMEM)],
        out_specs=(spec(VMEM), spec(VMEM)),
        scratch_shapes=[
            VMEM((k_units + max(fill, 8), SLOT, 128), jnp.bfloat16),
            VMEM((q_units + 8, SLOT, 128), jnp.bfloat16),
            VMEM((k_rows // KB, HD + 16, KB), jnp.bfloat16),
            VMEM((q_rows // QB + 1, 128, QB), jnp.bfloat16),
            VMEM((q_rows // QB + 1, HD + 16, QB), jnp.float32),
            VMEM((q_rows, 128), jnp.float32),
            SMEM((16,), jnp.int32),
            *[VMEM((KB, QB), jnp.bfloat16) for _ in range(UN)],
        ],
        compiler_params=pltpu.CompilerParams(vmem_limit_bytes=32 << 20),
        name="attention",
    )(counts, near(q_all.reshape(8, 4, half_rows, 128)),
      near(kv_all.reshape(4, 2, 4, 2 * half_rows, 128)))


def return_kernel(o_ref, lse_ref, back_ref, back_lse, mine, theirs, size_mine, size_theirs, both, size_both,
                  in_sem, t_send, t_recv, o_send, o_recv, l_send, l_recv):
    f, _, x, loc = place()
    hi, core = div(loc, 2), rem(loc, 2)
    half_rows = o_ref.shape[1]
    barrier = pltpu.get_barrier_semaphore()

    def greet(frame, there):
        pl.semaphore_signal(barrier, inc=1, device_id={"frame": frame, "space": x * 4 + there},
                            device_id_type=pl.DeviceIdType.MESH)

    greet(f, hi * 2 + 1 - core)
    each(1, 16, lambda n: greet(rem(f + div(n, 2), 8), rem(hi + n, 2) * 2 + core))

    keep = core * 16
    give = 16 - keep
    loads = [
        pltpu.make_async_copy(o_ref.at[pl.ds(keep, 16)], mine, in_sem.at[0]),
        pltpu.make_async_copy(lse_ref.at[:, pl.ds(keep, 16), :], size_mine, in_sem.at[1]),
    ]
    for copy in loads:
        copy.start()

    def twin(src, dst, n):
        return remote(src, dst, t_send.at[n], t_recv.at[n], f, x * 4 + hi * 2 + 1 - core)

    pl.semaphore_wait(barrier, 16)
    shares = [twin(lse_ref.at[:, pl.ds(give, 16), :], size_theirs, 0)]
    for n in range(2):
        shares.append(twin(o_ref.at[pl.ds(give + 8 * n, 8)], theirs.at[pl.ds(8 * n, 8)], 1 + n))
    for copy in shares:
        copy.start()
    for copy in loads:
        copy.wait()
    shares[0].wait_recv()

    turned = []
    for n in range(2):
        one, two = size_mine[n], size_theirs[n]
        top = jnp.maximum(one, two)
        one, two = jnp.exp2(one - top), jnp.exp2(two - top)
        total = one + two
        whole = top + jnp.log2(total)
        for r in range(16):
            size_both[r, n:n + 1, :] = whole[r:r + 1]
        turned.append(jnp.transpose(
            jnp.concatenate([one / total, two / total, jnp.zeros((96, 128), jnp.float32)], axis=0)))
    low = lax.broadcasted_iota(jnp.int32, (half_rows, 128), 1) < HD

    me = hi * 8 + f

    def copies(n):
        frame, there = rem(f + div(n, 2), 8), rem(hi + n, 2)
        r = there * 8 + frame
        space = x * 4 + there * 2 + core
        return (remote(both.at[r], back_ref.at[me], o_send.at[0], o_recv.at[0], frame, space),
                remote(size_both.at[r], back_lse.at[me], l_send.at[0], l_recv.at[0], frame, space))

    def start(n):
        for copy in copies(n):
            copy.start()

    for n in range(2):
        shares[1 + n].wait_recv()
        for r in range(8 * n, 8 * n + 8):
            one = jnp.where(low, turned[0][0:half_rows, r:r + 1], turned[1][0:half_rows, r:r + 1])
            two = jnp.where(low, turned[0][0:half_rows, 16 + r:17 + r], turned[1][0:half_rows, 16 + r:17 + r])
            both[r] = (mine[r].astype(jnp.float32) * one + theirs[r].astype(jnp.float32) * two).astype(jnp.bfloat16)

    each(1, 16, start)
    own = hi * 8 + f
    pltpu.make_async_copy(both.at[own], back_ref.at[me], o_recv.at[0]).start()
    pltpu.make_async_copy(size_both.at[own], back_lse.at[me], l_recv.at[0]).start()
    for copy in shares:
        copy.wait_send()
    for sem, ref in ((o_send, back_ref.at[pl.ds(0, 15)]), (l_send, back_lse.at[pl.ds(0, 15)]),
                     (o_recv, back_ref), (l_recv, back_lse)):
        pltpu.make_async_copy(ref, ref, sem.at[0]).wait()


def give_results(partial, sizes):
    dma = pltpu.SemaphoreType.DMA
    half_rows = partial.shape[1]
    held = VMEM((16, half_rows, 128), partial.dtype)
    return pl.pallas_call(
        return_kernel,
        out_shape=(VMEM((16, half_rows, 128), partial.dtype),
                   VMEM((16, 2, 128), sizes.dtype)),
        in_specs=[spec(ANY), spec(ANY)],
        out_specs=(spec(ANY), spec(ANY)),
        scratch_shapes=[
            held, held, VMEM((2, 16, 128), sizes.dtype), VMEM((2, 16, 128), sizes.dtype),
            held, VMEM((16, 2, 128), sizes.dtype),
            dma((2,)), dma((3,)), dma((3,)), dma((1,)), dma((1,)), dma((1,)), dma((1,))],
        compiler_params=pltpu.CompilerParams(
            collective_id=1, has_side_effects=True, vmem_limit_bytes=16 << 20),
        name="give_results",
    )(near(partial), near(sizes))


def finish_kernel(tok_ref, cnt_ref, back_ref, lse_ref, w_ref, o_ref, att, ys):
    times, slots, width = tok_ref.shape
    half = slots * SLOT // 2
    rows = slots * SLOT

    def shares(n):
        sizes = [lse_ref[p * 8:p * 8 + 8, n, :] for p in range(2)]
        top = jnp.maximum(sizes[0], sizes[1])
        powers = [jnp.exp2(v - top) for v in sizes]
        total = powers[0] + powers[1]
        return jnp.transpose(
            jnp.concatenate([v / total for v in powers] + [jnp.zeros((112, 128), jnp.float32)], axis=0))

    first, second = shares(0), shares(1)
    low = lax.broadcasted_iota(jnp.int32, (half, 128), 1) < HD

    def merged(h):
        out = jnp.zeros((half, 128), jnp.float32)
        for p in range(2):
            n = p * 8 + h
            share = jnp.where(low, first[0:half, n:n + 1], second[0:half, n:n + 1])
            out = out + back_ref[n].astype(jnp.float32) * share
        return out

    for j in range(HEADS // 2):
        a, b = merged(2 * j), merged(2 * j + 1)
        cols = slice(128 * j, 128 * j + 128)
        att[0:half, cols] = jnp.where(low, a, pltpu.roll(b, HD, 1)).astype(jnp.bfloat16)
        att[half:rows, cols] = jnp.where(low, pltpu.roll(a, HD, 1), b).astype(jnp.bfloat16)
    for c in range(width // 256):
        cols = slice(256 * c, 256 * c + 256)
        mixed = jnp.dot(att[...], w_ref[:, cols], preferred_element_type=jnp.float32)
        for i in range(slots):
            for e in range(2):
                ys[2 * c + e, pl.ds(i, SLOT, stride=slots), :] = (
                    mixed[i * SLOT:i * SLOT + SLOT, 128 * e:128 * e + 128])
    live = lax.broadcasted_iota(jnp.int32, (slots, width), 0) < cnt_ref[0]
    for t in range(times):
        mixed = jnp.concatenate([ys[c, t * slots:t * slots + slots, :] for c in range(width // 128)], axis=1)
        value = tok_ref[t].astype(jnp.float32) + mixed
        o_ref[t] = jnp.where(live, value, 0.0).astype(jnp.bfloat16)


def finish(tokens, count, back, sizes, w_out):
    times, slots, width = tokens.shape
    rows = slots * SLOT
    return pl.pallas_call(
        finish_kernel,
        out_shape=jax.ShapeDtypeStruct(tokens.shape, tokens.dtype),
        in_specs=[spec(VMEM), spec(SMEM), spec(VMEM), spec(VMEM), spec(VMEM)],
        out_specs=spec(VMEM),
        scratch_shapes=[VMEM((rows, w_out.shape[0]), jnp.bfloat16), VMEM((width // 128, rows, 128), jnp.float32)],
        compiler_params=pltpu.CompilerParams(vmem_limit_bytes=16 << 20),
        name="finish",
    )(near(tokens), count, near(back), near(sizes), near(w_out))


def on_device(tokens, tube_count, ln_gain, ln_bias, w_qkv, w_out):
    tokens = jnp.transpose(tokens, (1, 0, 2))
    q_all, kv_all, counts, tokens, w_out = project(
        tokens, tube_count, ln_gain.reshape(1, -1), ln_bias.reshape(1, -1), w_qkv, w_out)
    partial, sizes = attention(counts, q_all, kv_all, tokens.shape[0])
    mixed = finish(tokens, tube_count, *give_results(partial, sizes), w_out)
    return jnp.transpose(mixed, (1, 0, 2))


def solution(mesh):
    in_specs = (P("space", "frame", None), P("space"), P(), P(), P(), P())
    return jax.shard_map(
        on_device, mesh=mesh, in_specs=in_specs, out_specs=P("space", "frame", None), check_vma=False)
```

```python
import functools

import jax
import jax.numpy as jnp
from jax import lax
from jax.experimental import pallas as pl
from jax.experimental.pallas import tpu as pltpu
from jax.sharding import PartitionSpec as P

HEADS = 8
HD = 64
SLOT = 40
KB = 256
UN = 8
QB = 512
DEAD = -1e30
Q_AFTER = 2
SAFE = 100.0
EPSILON = 1e-06
SCALE = 1.4426950408889634 / 8.0
ANY = pl.ANY
VMEM = pltpu.VMEM
SMEM = pltpu.SMEM


def spec(space):
    return pl.BlockSpec(memory_space=space)


def near(array):
    return pltpu.with_memory_space_constraint(array, VMEM)


def place():
    f, s = lax.axis_index("frame"), lax.axis_index("space")
    return f, s, div(s, 4), rem(s, 4)


def remote(src, dst, send, recv, frame, space):
    return pltpu.make_async_remote_copy(
        src_ref=src, dst_ref=dst, send_sem=send, recv_sem=recv,
        device_id={"frame": frame, "space": space}, device_id_type=pl.DeviceIdType.MESH)


def rem(a, n):
    return lax.rem(a, jnp.int32(n))


def div(a, n):
    return lax.div(a, jnp.int32(n))


def each(lo, hi, body):
    def step(i, c):
        body(i)
        return c
    lax.fori_loop(lo, hi, step, 0)


def project_kernel(tok_in, cnt_ref, gain_ref, bias_ref, w_ref, w_last, q_out, kv_out, cnt_out, tok_ref, w_next,
                   w_v, xs, nb, kvs, qs, cnts,
                   w_sem, kv_send, kv_recv, q_send, q_recv, c_send, c_recv, x_send, r_send, pass_recv, rest_recv):
    f, s, x, loc = place()
    times, slots, width = tok_ref.shape
    inner = HEADS * HD

    tok_copy = pltpu.make_async_copy(tok_in, tok_ref, w_sem.at[3])
    tok_copy.start()
    last_copy = pltpu.make_async_copy(w_last, w_next, w_sem.at[4])
    copies = []
    for n, at in enumerate((inner, 2 * inner, 0)):
        cols = pl.ds(at, inner)
        copy = pltpu.make_async_copy(w_ref.at[:, cols], w_v.at[:, cols], w_sem.at[n])
        copy.start()
        copies.append(copy)

    barrier = pltpu.get_barrier_semaphore()

    def greet(frame, space):
        pl.semaphore_signal(barrier, inc=1, device_id={"frame": frame, "space": space},
                            device_id_type=pl.DeviceIdType.MESH)

    each(1, 32, lambda n: greet(rem(f + div(n, 4), 8), x * 4 + rem(loc + n, 4)))
    each(4, 16, lambda n: greet(f, rem(x * 4 + n, 16)))

    cnts[...] = jnp.full(cnts.shape, cnt_ref[0], jnp.int32)

    tok_copy.wait()
    for t in range(SLOT):
        values = tok_ref[t % times].astype(jnp.float32)
        for c in range(width // 128):
            xs[c, t * slots:t * slots + slots, :] = values[:, 128 * c:128 * c + 128]
    for i in range(slots):
        values = jnp.concatenate(
            [xs[c, pl.ds(i, SLOT, stride=slots), :] for c in range(width // 128)], axis=1)
        center = values - jnp.mean(values, axis=-1, keepdims=True)
        spread = jnp.mean(center * center, axis=-1, keepdims=True)
        normed = center * lax.rsqrt(spread + EPSILON) * gain_ref[...] + bias_ref[...]
        nb[i * SLOT:i * SLOT + SLOT, :] = normed.astype(jnp.bfloat16)

    rows_all = slots * SLOT
    half = rows_all // 2
    low = lax.broadcasted_iota(jnp.int32, (rows_all, 128), 1) < HD
    low_half = lax.broadcasted_iota(jnp.int32, (half, 128), 1) < HD

    copies[0].wait()
    copies[1].wait()
    for g in range(2):
        k4 = jnp.dot(nb[...], w_v[:, inner + 256 * g:inner + 256 * g + 256], preferred_element_type=jnp.float32)
        v4 = jnp.dot(nb[...], w_v[:, 2 * inner + 256 * g:2 * inner + 256 * g + 256],
                     preferred_element_type=jnp.float32)
        for j in range(2):
            k2, v2 = k4[:, 128 * j:128 * j + 128], v4[:, 128 * j:128 * j + 128]
            h = 4 * g + 2 * j
            kvs[h] = jnp.where(low, k2, pltpu.roll(v2, HD, 1)).astype(jnp.bfloat16)
            kvs[h + 1] = jnp.where(low, pltpu.roll(k2, HD, 1), v2).astype(jnp.bfloat16)

    part = div(f, 2)
    mine = rem(f, 2) * 4 + loc
    source = x * 8 + mine
    pl.semaphore_wait(barrier, 43)

    def kv_copy(d):
        h = rem(f + d + 2 * loc, 8)
        stays = (h == f) & (part == loc)
        return stays, h, remote(
            kvs.at[h], kv_out.at[source], kv_send.at[0], kv_recv.at[mine], h, x * 4 + part)

    def kv_start(d):
        stays, h, copy = kv_copy(d)

        @pl.when(stays)
        def _():
            pltpu.make_async_copy(kvs.at[h], kv_out.at[source], kv_recv.at[mine]).start()

        @pl.when(jnp.logical_not(stays))
        def _():
            copy.start()

    each(0, 8, kv_start)

    def count_copy(e):
        return remote(cnts, cnt_out.at[s], c_send.at[0], c_recv.at[0], f, rem(s + e, 16))

    each(1, 16, lambda e: count_copy(e).start())
    pltpu.make_async_copy(cnts, cnt_out.at[s], c_recv.at[0]).start()

    copies[2].wait()
    last_copy.start()
    for g in range(2):
        q4 = jnp.dot(nb[...], w_v[:, 256 * g:256 * g + 256], preferred_element_type=jnp.float32) * SCALE
        for j in range(2):
            q2 = q4[:, 128 * j:128 * j + 128]
            h = 4 * g + 2 * j
            qs[h] = jnp.where(low_half, q2[:half], pltpu.roll(q2[half:], HD, 1)).astype(jnp.bfloat16)
            qs[h + 1] = jnp.where(low_half, pltpu.roll(q2[:half], HD, 1), q2[half:]).astype(jnp.bfloat16)

    me = f * 4 + loc

    def q_copy(n):
        h = rem(f + div(n, 4), 8)
        return remote(qs.at[h], q_out.at[me], q_send.at[0], q_recv.at[0], h, x * 4 + rem(loc + n, 4))

    def ring(piece, send, recv, step):
        return remote(kv_out.at[piece], kv_out.at[piece], send.at[0], recv, f, rem(x + step, 4) * 4 + loc)

    def nth(t):
        u = rem(f - 2 * loc - t + 16, 8)
        return rem(u, 2) * 4 + div(u, 2)

    right, left = rem(x + 1, 4) * 8, rem(x + 3, 4) * 8

    def landed(sem, ref):
        pltpu.make_async_copy(ref, ref, sem).wait()

    def to_right(t, piece):
        even = rem(t, 2) == 0

        @pl.when(even)
        def _():
            ring(piece, x_send, pass_recv.at[t], 1).start()

        @pl.when(jnp.logical_not(even))
        def _():
            ring(piece, x_send, rest_recv.at[0], 1).start()

    def to_left(t, piece):
        odd = rem(t, 2) == 1

        @pl.when(odd)
        def _():
            ring(piece, x_send, pass_recv.at[t], 3).start()

        @pl.when(jnp.logical_not(odd))
        def _():
            ring(piece, x_send, rest_recv.at[0], 3).start()

    def arrived(t):
        i = nth(t)
        piece = x * 8 + i
        landed(kv_recv.at[i], kv_out.at[piece])
        to_right(t, piece)
        to_left(t, piece)

    each(0, Q_AFTER, arrived)
    each(1, 32, lambda n: q_copy(n).start())
    pltpu.make_async_copy(qs.at[f], q_out.at[me], q_recv.at[0]).start()
    each(Q_AFTER, 8, arrived)

    def relay(t):
        piece = left + nth(2 * t)
        landed(pass_recv.at[2 * t], kv_out.at[piece])
        ring(piece, r_send, rest_recv.at[0], 1).start()
        piece = right + nth(2 * t + 1)
        landed(pass_recv.at[2 * t + 1], kv_out.at[piece])
        ring(piece, r_send, rest_recv.at[0], 3).start()

    each(0, 4, relay)

    last_copy.wait()
    landed(kv_send.at[0], kv_out.at[pl.ds(0, 7)])

    @pl.when(part != loc)
    def _():
        landed(kv_send.at[0], kv_out.at[0])

    landed(c_send.at[0], cnt_out.at[pl.ds(0, 15)])
    landed(q_send.at[0], q_out.at[pl.ds(0, 31)])
    landed(x_send.at[0], kv_out.at[pl.ds(0, 16)])
    landed(r_send.at[0], kv_out.at[pl.ds(0, 8)])
    landed(c_recv.at[0], cnt_out)
    landed(q_recv.at[0], q_out)
    landed(rest_recv.at[0], kv_out.at[pl.ds(0, 16)])


def project(tokens, count, gain, bias, w_qkv, w_out):
    times, slots, width = tokens.shape
    rows = slots * SLOT
    bf16, i32 = jnp.bfloat16, jnp.int32
    dma = pltpu.SemaphoreType.DMA
    return pl.pallas_call(
        project_kernel,
        out_shape=(VMEM((32, rows // 2, 128), bf16),
                   VMEM((32, rows, 128), bf16),
                   VMEM((16, 1, 128), i32),
                   VMEM(tokens.shape, bf16), VMEM(w_out.shape, bf16)),
        in_specs=[spec(pltpu.HBM), spec(SMEM), spec(VMEM), spec(VMEM), spec(pltpu.HBM), spec(pltpu.HBM)],
        out_specs=(spec(ANY), spec(ANY), spec(ANY), spec(VMEM), spec(ANY)),
        scratch_shapes=[
            VMEM(w_qkv.shape, bf16), VMEM((width // 128, rows, 128), jnp.float32), VMEM((rows, width), bf16),
            VMEM((HEADS, rows, 128), bf16), VMEM((HEADS, rows // 2, 128), bf16), VMEM((1, 128), i32),
            dma((5,)), dma((1,)), dma((8,)), dma((1,)), dma((1,)), dma((1,)), dma((1,)),
            dma((1,)), dma((1,)), dma((8,)), dma((1,)),
        ],
        compiler_params=pltpu.CompilerParams(collective_id=0, has_side_effects=True),
        name="project",
    )(tokens, count, gain, bias, w_qkv, w_out)


def attention_kernel(cnt_ref, q_ref, kv_ref, of, kvc, qc, vt, qt, acc, *held, times):
    base = (lax.axis_index("space") // 4) * 4
    kv_flat = kvc.reshape(kvc.shape[0] * SLOT, 128)
    q_flat = qc.reshape(qc.shape[0] * SLOT, 128)
    of_flat = of.reshape(of.shape[0] * SLOT, 128)
    step_keys = KB

    def take_keys(n, unit):
        for j in range(4):
            for sub in range(2):
                kvc[unit + 2 * j + sub] = kv_ref[n // 4, sub, n % 4, j * SLOT:j * SLOT + SLOT, :]
        return unit + 2 * cnt_ref[n, 0, 0]

    unit = jnp.int32(0)
    for n in range(16):
        unit = take_keys(n, unit)
    key_units = unit
    for n in range(-(-step_keys // SLOT)):
        kvc[key_units + n] = kv_ref[0, 0, 0, 0:SLOT, :]

    unit = jnp.int32(0)
    for j in range(4):
        if j == 2:
            low_units = unit
        for l in range(4):
            live = j < cnt_ref[base + l, 0, 0]
            for f in range(8):
                qc[unit + f] = q_ref[f, l, (j % 2) * SLOT:(j % 2) * SLOT + SLOT, :]
            unit = unit + jnp.where(live, 8, 0)
    query_rows = unit * SLOT
    query_tiles = (query_rows + QB - 1) // QB
    key_rows = key_units * SLOT
    key_steps = (key_rows + step_keys - 1) // step_keys

    key_at = lax.broadcasted_iota(jnp.int32, (HD, KB), 1)
    row16 = lax.broadcasted_iota(jnp.int32, (16, KB), 0)

    def shape_keys(b, longest):
        turned = jnp.transpose(kv_flat[pl.ds(pl.multiple_of(b * KB, KB), KB), :].astype(jnp.float32))
        index = key_at + b * KB
        live = (index % SLOT < times) & (index < key_rows)
        vt[b, 0:HD, :] = jnp.where(live, turned[HD:], 0.0).astype(jnp.bfloat16)
        vt[b, HD:HD + 16, :] = jnp.where(live[:16] & (row16 == 0), 1.0, 0.0).astype(jnp.bfloat16)
        keys = turned[:HD]
        return jnp.maximum(longest, jnp.sum(keys * keys, axis=0, keepdims=True))

    longest_key = lax.fori_loop(0, key_steps, shape_keys, jnp.zeros((1, KB), jnp.float32))

    col = lax.broadcasted_iota(jnp.int32, (HD, QB), 1)
    low_rows = low_units * SLOT

    def shape_queries(t, longest):
        turned = jnp.transpose(q_flat[pl.ds(pl.multiple_of(t * QB, QB), QB), :].astype(jnp.float32))
        index = col + t * QB
        query = jnp.where(index < low_rows, turned[:HD], turned[HD:])
        query = jnp.where(index < query_rows, query, 0.0)
        qt[t, 0:HD, :] = query.astype(jnp.bfloat16)
        qt[t, HD:, :] = jnp.zeros((HD, QB), jnp.bfloat16)
        return jnp.maximum(longest, jnp.sum(query * query, axis=0, keepdims=True))

    longest_query = lax.fori_loop(0, query_tiles, shape_queries, jnp.zeros((1, QB), jnp.float32))
    safe = jnp.max(longest_key) * jnp.max(longest_query) < SAFE * SAFE

    def put(t, total, best):
        weight_sum = total[HD:HD + 1, :]
        out = total[0:HD, :] / weight_sum
        lse = jnp.broadcast_to(best + jnp.log2(weight_sum), (HD, QB))
        low = col + t * QB < low_rows
        both = jnp.concatenate([jnp.where(low, out, lse), jnp.where(low, lse, out)], axis=0)
        of_flat[pl.ds(pl.multiple_of(t * QB, QB), QB), :] = jnp.transpose(both)

    def block_scores(b, t):
        keys = kv_flat[pl.ds(pl.multiple_of(b * KB, KB), KB), :]
        return jnp.dot(keys, qt[t], preferred_element_type=jnp.float32)

    def clear(t):
        acc[t] = jnp.zeros((HD + 16, QB), jnp.float32)

    def after(item):
        t, b = item
        turn = b + 1 == key_steps
        return jnp.minimum(jnp.where(turn, t + 1, t), query_tiles), jnp.where(turn, 0, b + 1)

    def add(u, item):
        t, b = item
        acc[t] += jnp.dot(vt[b], held[u][...], preferred_element_type=jnp.float32)

    def weigh(u, item):
        t, b = item
        held[u][...] = jnp.exp2(block_scores(b, t)).astype(jnp.bfloat16)

    def plain(i, carry):
        before, now = carry
        then = now[-1]
        later = []
        for u in range(UN):
            add(u, before[u])
            weigh(u, now[u])
            then = after(then)
            later.append(then)
        return now, tuple(later)

    def plain_all():
        each(0, query_tiles, clear)
        first = [(jnp.int32(0), jnp.int32(0))]
        for _ in range(UN - 1):
            first.append(after(first[-1]))
        for u in range(UN):
            weigh(u, first[u])
        second = [after(first[-1])]
        for _ in range(UN - 1):
            second.append(after(second[-1]))
        steps = (query_tiles * key_steps + UN - 1) // UN
        last, _ = lax.fori_loop(1, steps, plain, (tuple(first), tuple(second)))
        for u in range(UN):
            add(u, last[u])

        each(0, query_tiles, lambda t: put(t, acc[t], 0.0))

    def shifted_tile(t):
        def step(b, carry):
            best, total = carry
            scores = block_scores(b, t)
            best_next = jnp.maximum(best, jnp.max(scores, axis=0, keepdims=True))
            weights = jnp.exp2(scores - best_next).astype(jnp.bfloat16)
            total = total * jnp.exp2(best - best_next) + jnp.dot(
                vt[b], weights, preferred_element_type=jnp.float32)
            return best_next, total

        best, total = lax.fori_loop(
            0, key_steps, step,
            (jnp.full((1, QB), DEAD, jnp.float32), jnp.zeros((HD + 16, QB), jnp.float32)))
        put(t, total, best)

    @pl.when(safe)
    def _():
        plain_all()

    @pl.when(jnp.logical_not(safe))
    def _():
        each(0, query_tiles, shifted_tile)


def attention(counts, q_all, kv_all, times):
    sources, half_rows, _ = q_all.shape
    q_units, k_units = 4 * sources, 4 * sources
    q_rows = (q_units * SLOT + QB - 1) // QB * QB
    step = KB
    k_rows = (k_units * SLOT + step - 1) // step * step
    fill = -(-step // SLOT)
    return pl.pallas_call(
        functools.partial(attention_kernel, times=times),
        out_shape=VMEM((q_rows // SLOT, SLOT, 128), jnp.float32),
        in_specs=[spec(SMEM), spec(VMEM), spec(VMEM)],
        out_specs=spec(VMEM),
        scratch_shapes=[
            VMEM((k_units + max(fill, 8), SLOT, 128), jnp.bfloat16),
            VMEM((q_units + 8, SLOT, 128), jnp.bfloat16),
            VMEM((k_rows // KB, HD + 16, KB), jnp.bfloat16),
            VMEM((q_rows // QB + 1, 128, QB), jnp.bfloat16),
            VMEM((q_rows // QB + 1, HD + 16, QB), jnp.float32),
            *[VMEM((KB, QB), jnp.bfloat16) for _ in range(UN)],
        ],
        compiler_params=pltpu.CompilerParams(vmem_limit_bytes=32 << 20),
        name="attention",
    )(counts, near(q_all.reshape(8, 4, half_rows, 128)),
      near(kv_all.reshape(4, 2, 4, 2 * half_rows, 128)))


def return_kernel(cnt_ref, of, back_ref, back_lse, packed, sizes, theirs, size_theirs, both, size_both,
                  t_send, t_recv, o_send, o_recv, l_send, l_recv):
    f, _, x, loc = place()
    hi, core = div(loc, 2), rem(loc, 2)
    half_rows = packed.shape[1]
    barrier = pltpu.get_barrier_semaphore()

    def greet(frame, there):
        pl.semaphore_signal(barrier, inc=1, device_id={"frame": frame, "space": x * 4 + there},
                            device_id_type=pl.DeviceIdType.MESH)

    greet(f, hi * 2 + 1 - core)
    for n in range(1, 16):
        greet(rem(f + n // 2, 8), rem(hi + n, 2) * 2 + core)

    starts, unit = [], jnp.int32(0)
    for j in range(4):
        for l in range(4):
            live = j < cnt_ref[x * 4 + l, 0, 0]
            starts.append(jnp.where(live, unit, 0))
            unit = unit + jnp.where(live, 8, 0)
    lane = lax.broadcasted_iota(jnp.int32, (SLOT, 128), 1)
    in_low = lane < HD

    def gather(frame, kept):
        for l in range(4):
            i = (l % 2) * 16 + (l // 2) * 8
            for j in range(2):
                first = of[starts[j * 4 + l] + frame]
                second = of[starts[j * 4 + 8 + l] + frame]
                packed[i + frame, j * SLOT:j * SLOT + SLOT, :] = jnp.where(in_low, first, second).astype(jnp.bfloat16)
                kept[j] = jnp.where(rem(lane, HD) == i + frame, jnp.where(in_low, second, first), kept[j])
        return kept

    kept = lax.fori_loop(0, 8, gather, [jnp.zeros((SLOT, 128), jnp.float32)] * 2)
    rows = jnp.transpose(jnp.concatenate([*kept, jnp.zeros((128 - 2 * SLOT, 128), jnp.float32)], axis=0))
    sizes[0] = rows[HD:HD + 32]
    sizes[1] = rows[0:32]

    keep = core * 16
    give = 16 - keep

    def twin(src, dst, n):
        return remote(src, dst, t_send.at[n], t_recv.at[n], f, x * 4 + hi * 2 + 1 - core)

    pl.semaphore_wait(barrier, 16)
    shares = [twin(sizes.at[:, pl.ds(give, 16), :], size_theirs, 0)]
    for n in range(2):
        shares.append(twin(packed.at[pl.ds(give + 8 * n, 8)], theirs.at[pl.ds(8 * n, 8)], 1 + n))
    for copy in shares:
        copy.start()
    shares[0].wait_recv()

    turned = []
    for n in range(2):
        one, two = sizes[n, pl.ds(pl.multiple_of(keep, 16), 16), :], size_theirs[n]
        top = jnp.maximum(one, two)
        one, two = jnp.exp2(one - top), jnp.exp2(two - top)
        total = one + two
        whole = top + jnp.log2(total)
        for r in range(16):
            size_both[r, n:n + 1, :] = whole[r:r + 1]
        turned.append(jnp.transpose(
            jnp.concatenate([one / total, two / total, jnp.zeros((96, 128), jnp.float32)], axis=0)))
    low = lax.broadcasted_iota(jnp.int32, (half_rows, 128), 1) < HD
    me = hi * 8 + f

    def send(there, frame):
        r = there * 8 + frame
        stays = (frame == f) & (hi == there)

        @pl.when(stays)
        def _():
            pltpu.make_async_copy(both.at[r], back_ref.at[me], o_recv.at[0]).start()
            pltpu.make_async_copy(size_both.at[r], back_lse.at[me], l_recv.at[0]).start()

        @pl.when(jnp.logical_not(stays))
        def _():
            space = x * 4 + there * 2 + core
            remote(both.at[r], back_ref.at[me], o_send.at[0], o_recv.at[0], frame, space).start()
            remote(size_both.at[r], back_lse.at[me], l_send.at[0], l_recv.at[0], frame, space).start()

    for n in range(2):
        shares[1 + n].wait_recv()
        for r in range(8 * n, 8 * n + 8):
            one = jnp.where(low, turned[0][0:half_rows, r:r + 1], turned[1][0:half_rows, r:r + 1])
            two = jnp.where(low, turned[0][0:half_rows, 16 + r:17 + r], turned[1][0:half_rows, 16 + r:17 + r])
            own = packed[keep + r].astype(jnp.float32)
            both[r] = (own * one + theirs[r].astype(jnp.float32) * two).astype(jnp.bfloat16)
        each(0, 8, lambda d, n=n: send(n, rem(f + 1 + d, 8)))

    for copy in shares:
        copy.wait_send()
    for sem, ref in ((o_send, back_ref.at[pl.ds(0, 15)]), (l_send, back_lse.at[pl.ds(0, 15)]),
                     (o_recv, back_ref), (l_recv, back_lse)):
        pltpu.make_async_copy(ref, ref, sem.at[0]).wait()


def give_results(counts, partial):
    dma = pltpu.SemaphoreType.DMA
    bf16, f32 = jnp.bfloat16, jnp.float32
    half_rows = 2 * SLOT
    return pl.pallas_call(
        return_kernel,
        out_shape=(VMEM((16, half_rows, 128), bf16), VMEM((16, 2, 128), f32)),
        in_specs=[spec(SMEM), spec(VMEM)],
        out_specs=(spec(ANY), spec(ANY)),
        scratch_shapes=[
            VMEM((32, half_rows, 128), bf16), VMEM((2, 32, 128), f32),
            VMEM((16, half_rows, 128), bf16), VMEM((2, 16, 128), f32),
            VMEM((16, half_rows, 128), bf16), VMEM((16, 2, 128), f32),
            dma((3,)), dma((3,)), dma((1,)), dma((1,)), dma((1,)), dma((1,))],
        compiler_params=pltpu.CompilerParams(
            collective_id=1, has_side_effects=True, vmem_limit_bytes=16 << 20),
        name="give_results",
    )(counts, near(partial))


def finish_kernel(tok_ref, cnt_ref, back_ref, lse_ref, w_ref, o_ref, att, ys):
    times, slots, width = tok_ref.shape
    half = slots * SLOT // 2
    rows = slots * SLOT

    def shares(n):
        sizes = [lse_ref[p * 8:p * 8 + 8, n, :] for p in range(2)]
        top = jnp.maximum(sizes[0], sizes[1])
        powers = [jnp.exp2(v - top) for v in sizes]
        total = powers[0] + powers[1]
        return jnp.transpose(
            jnp.concatenate([v / total for v in powers] + [jnp.zeros((112, 128), jnp.float32)], axis=0))

    first, second = shares(0), shares(1)
    low = lax.broadcasted_iota(jnp.int32, (half, 128), 1) < HD

    def merged(h):
        out = jnp.zeros((half, 128), jnp.float32)
        for p in range(2):
            n = p * 8 + h
            share = jnp.where(low, first[0:half, n:n + 1], second[0:half, n:n + 1])
            out = out + back_ref[n].astype(jnp.float32) * share
        return out

    for j in range(HEADS // 2):
        a, b = merged(2 * j), merged(2 * j + 1)
        cols = slice(128 * j, 128 * j + 128)
        att[0:half, cols] = jnp.where(low, a, pltpu.roll(b, HD, 1)).astype(jnp.bfloat16)
        att[half:rows, cols] = jnp.where(low, pltpu.roll(a, HD, 1), b).astype(jnp.bfloat16)
    for c in range(width // 256):
        cols = slice(256 * c, 256 * c + 256)
        mixed = jnp.dot(att[...], w_ref[:, cols], preferred_element_type=jnp.float32)
        for i in range(slots):
            for e in range(2):
                ys[2 * c + e, pl.ds(i, SLOT, stride=slots), :] = (
                    mixed[i * SLOT:i * SLOT + SLOT, 128 * e:128 * e + 128])
    live = lax.broadcasted_iota(jnp.int32, (slots, width), 0) < cnt_ref[0]
    for t in range(times):
        mixed = jnp.concatenate([ys[c, t * slots:t * slots + slots, :] for c in range(width // 128)], axis=1)
        value = tok_ref[t].astype(jnp.float32) + mixed
        o_ref[t] = jnp.where(live, value, 0.0).astype(jnp.bfloat16)


def finish(tokens, count, back, sizes, w_out):
    times, slots, width = tokens.shape
    rows = slots * SLOT
    return pl.pallas_call(
        finish_kernel,
        out_shape=jax.ShapeDtypeStruct(tokens.shape, tokens.dtype),
        in_specs=[spec(VMEM), spec(SMEM), spec(VMEM), spec(VMEM), spec(VMEM)],
        out_specs=spec(VMEM),
        scratch_shapes=[VMEM((rows, w_out.shape[0]), jnp.bfloat16), VMEM((width // 128, rows, 128), jnp.float32)],
        compiler_params=pltpu.CompilerParams(vmem_limit_bytes=16 << 20),
        name="finish",
    )(near(tokens), count, near(back), near(sizes), near(w_out))


def on_device(tokens, tube_count, ln_gain, ln_bias, w_qkv, w_out):
    tokens = jnp.transpose(tokens, (1, 0, 2))
    q_all, kv_all, counts, tokens, w_out = project(
        tokens, tube_count, ln_gain.reshape(1, -1), ln_bias.reshape(1, -1), w_qkv, w_out)
    partial = attention(counts, q_all, kv_all, tokens.shape[0])
    mixed = finish(tokens, tube_count, *give_results(counts, partial), w_out)
    return jnp.transpose(mixed, (1, 0, 2))


def solution(mesh):
    in_specs = (P("space", "frame", None), P("space"), P(), P(), P(), P())
    return jax.shard_map(
        on_device, mesh=mesh, in_specs=in_specs, out_specs=P("space", "frame", None), check_vma=False)
```

```python
import functools

import jax
import jax.numpy as jnp
from jax import lax
from jax.experimental import pallas as pl
from jax.experimental.pallas import tpu as pltpu
from jax.sharding import PartitionSpec as P

HEADS = 8
HD = 64
SLOT = 40
KB = 256
UN = 8
QB = 512
DEAD = -1e30
Q_AFTER = 2
SAFE = 100.0
EPSILON = 1e-06
SCALE = 1.4426950408889634 / 8.0
ANY = pl.ANY
VMEM = pltpu.VMEM
SMEM = pltpu.SMEM


def spec(space):
    return pl.BlockSpec(memory_space=space)


def near(array):
    return pltpu.with_memory_space_constraint(array, VMEM)


def place():
    f, s = lax.axis_index("frame"), lax.axis_index("space")
    return f, s, div(s, 4), rem(s, 4)


def remote(src, dst, send, recv, frame, space):
    return pltpu.make_async_remote_copy(
        src_ref=src, dst_ref=dst, send_sem=send, recv_sem=recv,
        device_id={"frame": frame, "space": space}, device_id_type=pl.DeviceIdType.MESH)


def rem(a, n):
    return lax.rem(a, jnp.int32(n))


def div(a, n):
    return lax.div(a, jnp.int32(n))


def each(lo, hi, body):
    def step(i, c):
        body(i)
        return c
    lax.fori_loop(lo, hi, step, 0)


def project_kernel(tok_in, cnt_ref, gain_ref, bias_ref, w_ref, w_last, q_out, kv_out, cnt_out, tok_ref, w_next,
                   w_v, xs, nb, kvs, qs, cnts,
                   w_sem, kv_send, kv_recv, q_send, q_recv, c_send, c_recv, x_send, r_send, pass_recv, rest_recv):
    f, s, x, loc = place()
    times, slots, width = tok_ref.shape
    inner = HEADS * HD

    tok_copy = pltpu.make_async_copy(tok_in, tok_ref, w_sem.at[3])
    tok_copy.start()
    last_copy = pltpu.make_async_copy(w_last, w_next, w_sem.at[4])
    copies = []
    for n, at in enumerate((inner, 2 * inner, 0)):
        cols = pl.ds(at, inner)
        copy = pltpu.make_async_copy(w_ref.at[:, cols], w_v.at[:, cols], w_sem.at[n])
        copy.start()
        copies.append(copy)

    barrier = pltpu.get_barrier_semaphore()

    def greet(frame, space):
        pl.semaphore_signal(barrier, inc=1, device_id={"frame": frame, "space": space},
                            device_id_type=pl.DeviceIdType.MESH)

    each(1, 32, lambda n: greet(rem(f + div(n, 4), 8), x * 4 + rem(loc + n, 4)))
    each(4, 16, lambda n: greet(f, rem(x * 4 + n, 16)))

    cnts[...] = jnp.full(cnts.shape, cnt_ref[0], jnp.int32)

    tok_copy.wait()
    for t in range(SLOT):
        values = tok_ref[t % times].astype(jnp.float32)
        for c in range(width // 128):
            xs[c, t * slots:t * slots + slots, :] = values[:, 128 * c:128 * c + 128]
    for i in range(slots):
        values = jnp.concatenate(
            [xs[c, pl.ds(i, SLOT, stride=slots), :] for c in range(width // 128)], axis=1)
        center = values - jnp.mean(values, axis=-1, keepdims=True)
        spread = jnp.mean(center * center, axis=-1, keepdims=True)
        normed = center * lax.rsqrt(spread + EPSILON) * gain_ref[...] + bias_ref[...]
        nb[i * SLOT:i * SLOT + SLOT, :] = normed.astype(jnp.bfloat16)

    rows_all = slots * SLOT
    half = rows_all // 2
    low = lax.broadcasted_iota(jnp.int32, (rows_all, 128), 1) < HD
    low_half = lax.broadcasted_iota(jnp.int32, (half, 128), 1) < HD

    copies[0].wait()
    copies[1].wait()
    for g in range(2):
        k4 = jnp.dot(nb[...], w_v[:, inner + 256 * g:inner + 256 * g + 256], preferred_element_type=jnp.float32)
        v4 = jnp.dot(nb[...], w_v[:, 2 * inner + 256 * g:2 * inner + 256 * g + 256],
                     preferred_element_type=jnp.float32)
        for j in range(2):
            k2, v2 = k4[:, 128 * j:128 * j + 128], v4[:, 128 * j:128 * j + 128]
            h = 4 * g + 2 * j
            kvs[h] = jnp.where(low, k2, pltpu.roll(v2, HD, 1)).astype(jnp.bfloat16)
            kvs[h + 1] = jnp.where(low, pltpu.roll(k2, HD, 1), v2).astype(jnp.bfloat16)

    part = div(f, 2)
    mine = rem(f, 2) * 4 + loc
    source = x * 8 + mine
    pl.semaphore_wait(barrier, 43)

    def kv_copy(d):
        h = rem(f + d + 2 * loc, 8)
        stays = (h == f) & (part == loc)
        return stays, h, remote(
            kvs.at[h], kv_out.at[source], kv_send.at[0], kv_recv.at[mine], h, x * 4 + part)

    def kv_start(d):
        stays, h, copy = kv_copy(d)

        @pl.when(stays)
        def _():
            pltpu.make_async_copy(kvs.at[h], kv_out.at[source], kv_recv.at[mine]).start()

        @pl.when(jnp.logical_not(stays))
        def _():
            copy.start()

    each(0, 8, kv_start)

    def count_copy(e):
        return remote(cnts, cnt_out.at[s], c_send.at[0], c_recv.at[0], f, rem(s + e, 16))

    each(1, 16, lambda e: count_copy(e).start())
    pltpu.make_async_copy(cnts, cnt_out.at[s], c_recv.at[0]).start()

    copies[2].wait()
    last_copy.start()
    for g in range(2):
        q4 = jnp.dot(nb[...], w_v[:, 256 * g:256 * g + 256], preferred_element_type=jnp.float32) * SCALE
        for j in range(2):
            q2 = q4[:, 128 * j:128 * j + 128]
            h = 4 * g + 2 * j
            qs[h] = jnp.where(low_half, q2[:half], pltpu.roll(q2[half:], HD, 1)).astype(jnp.bfloat16)
            qs[h + 1] = jnp.where(low_half, pltpu.roll(q2[:half], HD, 1), q2[half:]).astype(jnp.bfloat16)

    me = f * 4 + loc

    def q_copy(n):
        h = rem(f + div(n, 4), 8)
        return remote(qs.at[h], q_out.at[me], q_send.at[0], q_recv.at[0], h, x * 4 + rem(loc + n, 4))

    def ring(piece, send, recv, step):
        return remote(kv_out.at[piece], kv_out.at[piece], send.at[0], recv, f, rem(x + step, 4) * 4 + loc)

    def nth(t):
        u = rem(f - 2 * loc - t + 16, 8)
        return rem(u, 2) * 4 + div(u, 2)

    right, left = rem(x + 1, 4) * 8, rem(x + 3, 4) * 8

    def landed(sem, ref):
        pltpu.make_async_copy(ref, ref, sem).wait()

    def to_right(t, piece):
        even = rem(t, 2) == 0

        @pl.when(even)
        def _():
            ring(piece, x_send, pass_recv.at[t], 1).start()

        @pl.when(jnp.logical_not(even))
        def _():
            ring(piece, x_send, rest_recv.at[0], 1).start()

    def to_left(t, piece):
        odd = rem(t, 2) == 1

        @pl.when(odd)
        def _():
            ring(piece, x_send, pass_recv.at[t], 3).start()

        @pl.when(jnp.logical_not(odd))
        def _():
            ring(piece, x_send, rest_recv.at[0], 3).start()

    def arrived(t):
        i = nth(t)
        piece = x * 8 + i
        landed(kv_recv.at[i], kv_out.at[piece])
        to_right(t, piece)
        to_left(t, piece)

    each(0, Q_AFTER, arrived)
    each(1, 32, lambda n: q_copy(n).start())
    pltpu.make_async_copy(qs.at[f], q_out.at[me], q_recv.at[0]).start()
    each(Q_AFTER, 8, arrived)

    def relay(t):
        piece = left + nth(2 * t)
        landed(pass_recv.at[2 * t], kv_out.at[piece])
        ring(piece, r_send, rest_recv.at[0], 1).start()
        piece = right + nth(2 * t + 1)
        landed(pass_recv.at[2 * t + 1], kv_out.at[piece])
        ring(piece, r_send, rest_recv.at[0], 3).start()

    each(0, 4, relay)

    last_copy.wait()
    landed(kv_send.at[0], kv_out.at[pl.ds(0, 7)])

    @pl.when(part != loc)
    def _():
        landed(kv_send.at[0], kv_out.at[0])

    landed(c_send.at[0], cnt_out.at[pl.ds(0, 15)])
    landed(q_send.at[0], q_out.at[pl.ds(0, 31)])
    landed(x_send.at[0], kv_out.at[pl.ds(0, 16)])
    landed(r_send.at[0], kv_out.at[pl.ds(0, 8)])
    landed(c_recv.at[0], cnt_out)
    landed(q_recv.at[0], q_out)
    landed(rest_recv.at[0], kv_out.at[pl.ds(0, 16)])


def project(tokens, count, gain, bias, w_qkv, w_out):
    times, slots, width = tokens.shape
    rows = slots * SLOT
    bf16, i32 = jnp.bfloat16, jnp.int32
    dma = pltpu.SemaphoreType.DMA
    return pl.pallas_call(
        project_kernel,
        out_shape=(VMEM((32, rows // 2, 128), bf16),
                   VMEM((32, rows, 128), bf16),
                   VMEM((16, 1, 128), i32),
                   VMEM(tokens.shape, bf16), VMEM(w_out.shape, bf16)),
        in_specs=[spec(pltpu.HBM), spec(SMEM), spec(VMEM), spec(VMEM), spec(pltpu.HBM), spec(pltpu.HBM)],
        out_specs=(spec(ANY), spec(ANY), spec(ANY), spec(VMEM), spec(ANY)),
        scratch_shapes=[
            VMEM(w_qkv.shape, bf16), VMEM((width // 128, rows, 128), jnp.float32), VMEM((rows, width), bf16),
            VMEM((HEADS, rows, 128), bf16), VMEM((HEADS, rows // 2, 128), bf16), VMEM((1, 128), i32),
            dma((5,)), dma((1,)), dma((8,)), dma((1,)), dma((1,)), dma((1,)), dma((1,)),
            dma((1,)), dma((1,)), dma((8,)), dma((1,)),
        ],
        compiler_params=pltpu.CompilerParams(collective_id=0, has_side_effects=True),
        name="project",
    )(tokens, count, gain, bias, w_qkv, w_out)


def attention_kernel(cnt_ref, q_ref, kv_ref, acc, kvc, qc, vt, qt, *held, times):
    base = (lax.axis_index("space") // 4) * 4
    kv_flat = kvc.reshape(kvc.shape[0] * SLOT, 128)
    q_flat = qc.reshape(qc.shape[0] * SLOT, 128)
    step_keys = KB

    def take_keys(n, unit):
        for j in range(4):
            for sub in range(2):
                kvc[unit + 2 * j + sub] = kv_ref[n // 4, sub, n % 4, j * SLOT:j * SLOT + SLOT, :]
        return unit + 2 * cnt_ref[n, 0, 0]

    unit = jnp.int32(0)
    for n in range(16):
        unit = take_keys(n, unit)
    key_units = unit
    for n in range(-(-step_keys // SLOT)):
        kvc[key_units + n] = kv_ref[0, 0, 0, 0:SLOT, :]

    unit = jnp.int32(0)
    for j in range(4):
        if j == 2:
            low_units = unit
        for l in range(4):
            live = j < cnt_ref[base + l, 0, 0]
            for f in range(8):
                qc[unit + f] = q_ref[f, l, (j % 2) * SLOT:(j % 2) * SLOT + SLOT, :]
            unit = unit + jnp.where(live, 8, 0)
    query_rows = unit * SLOT
    query_tiles = (query_rows + QB - 1) // QB
    key_rows = key_units * SLOT
    key_steps = (key_rows + step_keys - 1) // step_keys

    key_at = lax.broadcasted_iota(jnp.int32, (HD, KB), 1)
    row16 = lax.broadcasted_iota(jnp.int32, (16, KB), 0)

    def shape_keys(b, longest):
        turned = jnp.transpose(kv_flat[pl.ds(pl.multiple_of(b * KB, KB), KB), :].astype(jnp.float32))
        index = key_at + b * KB
        live = (index % SLOT < times) & (index < key_rows)
        vt[b, 0:HD, :] = jnp.where(live, turned[HD:], 0.0).astype(jnp.bfloat16)
        vt[b, HD:HD + 16, :] = jnp.where(live[:16] & (row16 == 0), 1.0, 0.0).astype(jnp.bfloat16)
        keys = turned[:HD]
        return jnp.maximum(longest, jnp.sum(keys * keys, axis=0, keepdims=True))

    longest_key = lax.fori_loop(0, key_steps, shape_keys, jnp.zeros((1, KB), jnp.float32))

    col = lax.broadcasted_iota(jnp.int32, (HD, QB), 1)
    low_rows = low_units * SLOT

    def shape_queries(t, longest):
        turned = jnp.transpose(q_flat[pl.ds(pl.multiple_of(t * QB, QB), QB), :].astype(jnp.float32))
        index = col + t * QB
        query = jnp.where(index < low_rows, turned[:HD], turned[HD:])
        query = jnp.where(index < query_rows, query, 0.0)
        qt[t, 0:HD, :] = query.astype(jnp.bfloat16)
        qt[t, HD:, :] = jnp.zeros((HD, QB), jnp.bfloat16)
        return jnp.maximum(longest, jnp.sum(query * query, axis=0, keepdims=True))

    longest_query = lax.fori_loop(0, query_tiles, shape_queries, jnp.zeros((1, QB), jnp.float32))
    safe = jnp.max(longest_key) * jnp.max(longest_query) < SAFE * SAFE

    def block_scores(b, t):
        keys = kv_flat[pl.ds(pl.multiple_of(b * KB, KB), KB), :]
        return jnp.dot(keys, qt[t], preferred_element_type=jnp.float32)

    def clear(t):
        acc[t] = jnp.zeros((HD + 16, QB), jnp.float32)

    def after(item):
        t, b = item
        turn = b + 1 == key_steps
        return jnp.minimum(jnp.where(turn, t + 1, t), query_tiles), jnp.where(turn, 0, b + 1)

    def add(u, item):
        t, b = item
        acc[t] += jnp.dot(vt[b], held[u][...], preferred_element_type=jnp.float32)

    def weigh(u, item):
        t, b = item
        held[u][...] = jnp.exp2(block_scores(b, t)).astype(jnp.bfloat16)

    def plain(i, carry):
        before, now = carry
        then = now[-1]
        later = []
        for u in range(UN):
            add(u, before[u])
            weigh(u, now[u])
            then = after(then)
            later.append(then)
        return now, tuple(later)

    def plain_all():
        each(0, query_tiles, clear)
        first = [(jnp.int32(0), jnp.int32(0))]
        for _ in range(UN - 1):
            first.append(after(first[-1]))
        for u in range(UN):
            weigh(u, first[u])
        second = [after(first[-1])]
        for _ in range(UN - 1):
            second.append(after(second[-1]))
        steps = (query_tiles * key_steps + UN - 1) // UN
        last, _ = lax.fori_loop(1, steps, plain, (tuple(first), tuple(second)))
        for u in range(UN):
            add(u, last[u])

    def shifted_tile(t):
        def step(b, carry):
            best, total = carry
            scores = block_scores(b, t)
            best_next = jnp.maximum(best, jnp.max(scores, axis=0, keepdims=True))
            weights = jnp.exp2(scores - best_next).astype(jnp.bfloat16)
            total = total * jnp.exp2(best - best_next) + jnp.dot(
                vt[b], weights, preferred_element_type=jnp.float32)
            return best_next, total

        best, total = lax.fori_loop(
            0, key_steps, step,
            (jnp.full((1, QB), DEAD, jnp.float32), jnp.zeros((HD + 16, QB), jnp.float32)))
        acc[t] = total
        acc[t, HD + 8:HD + 9, :] = best

    @pl.when(safe)
    def _():
        plain_all()

    @pl.when(jnp.logical_not(safe))
    def _():
        each(0, query_tiles, shifted_tile)


def attention(counts, q_all, kv_all, times):
    sources, half_rows, _ = q_all.shape
    q_units, k_units = 4 * sources, 4 * sources
    q_rows = (q_units * SLOT + QB - 1) // QB * QB
    step = KB
    k_rows = (k_units * SLOT + step - 1) // step * step
    fill = -(-step // SLOT)
    return pl.pallas_call(
        functools.partial(attention_kernel, times=times),
        out_shape=VMEM((q_rows // QB + 1, HD + 16, QB), jnp.float32),
        in_specs=[spec(SMEM), spec(VMEM), spec(VMEM)],
        out_specs=spec(VMEM),
        scratch_shapes=[
            VMEM((k_units + max(fill, 8), SLOT, 128), jnp.bfloat16),
            VMEM((q_units + 8, SLOT, 128), jnp.bfloat16),
            VMEM((k_rows // KB, HD + 16, KB), jnp.bfloat16),
            VMEM((q_rows // QB + 1, 128, QB), jnp.bfloat16),
            *[VMEM((KB, QB), jnp.bfloat16) for _ in range(UN)],
        ],
        compiler_params=pltpu.CompilerParams(vmem_limit_bytes=32 << 20),
        name="attention",
    )(counts, near(q_all.reshape(8, 4, half_rows, 128)),
      near(kv_all.reshape(4, 2, 4, 2 * half_rows, 128)))


def return_kernel(cnt_ref, acc, back_ref, back_lse, of, packed, sizes, theirs, size_theirs, both, size_both,
                  t_send, t_recv, o_send, o_recv, l_send, l_recv):
    f, _, x, loc = place()
    hi, core = div(loc, 2), rem(loc, 2)
    half_rows = packed.shape[1]
    barrier = pltpu.get_barrier_semaphore()

    def greet(frame, there):
        pl.semaphore_signal(barrier, inc=1, device_id={"frame": frame, "space": x * 4 + there},
                            device_id_type=pl.DeviceIdType.MESH)

    greet(f, hi * 2 + 1 - core)
    for n in range(1, 16):
        greet(rem(f + n // 2, 8), rem(hi + n, 2) * 2 + core)

    starts, unit = [], jnp.int32(0)
    for j in range(4):
        for l in range(4):
            live = j < cnt_ref[x * 4 + l, 0, 0]
            starts.append(jnp.where(live, unit, 0))
            unit = unit + jnp.where(live, 8, 0)
        if j == 1:
            low_rows = unit * SLOT
    lane = lax.broadcasted_iota(jnp.int32, (SLOT, 128), 1)
    in_low = lane < HD
    of_flat = of.reshape(of.shape[0] * SLOT, 128)
    col = lax.broadcasted_iota(jnp.int32, (HD, QB), 1)

    def put(t):
        weight_sum = acc[t, HD:HD + 1, :]
        out = acc[t, 0:HD, :] / weight_sum
        lse = jnp.broadcast_to(acc[t, HD + 8:HD + 9, :] + jnp.log2(weight_sum), (HD, QB))
        low = col + t * QB < low_rows
        both = jnp.concatenate([jnp.where(low, out, lse), jnp.where(low, lse, out)], axis=0)
        of_flat[pl.ds(pl.multiple_of(t * QB, QB), QB), :] = jnp.transpose(both)

    each(0, acc.shape[0] - 1, put)

    def gather(frame, kept):
        for l in range(4):
            i = (l % 2) * 16 + (l // 2) * 8
            for j in range(2):
                first = of[starts[j * 4 + l] + frame]
                second = of[starts[j * 4 + 8 + l] + frame]
                packed[i + frame, j * SLOT:j * SLOT + SLOT, :] = jnp.where(in_low, first, second).astype(jnp.bfloat16)
                kept[j] = jnp.where(rem(lane, HD) == i + frame, jnp.where(in_low, second, first), kept[j])
        return kept

    kept = lax.fori_loop(0, 8, gather, [jnp.zeros((SLOT, 128), jnp.float32)] * 2)
    rows = jnp.transpose(jnp.concatenate([*kept, jnp.zeros((128 - 2 * SLOT, 128), jnp.float32)], axis=0))
    sizes[0] = rows[HD:HD + 32]
    sizes[1] = rows[0:32]

    keep = core * 16
    give = 16 - keep

    def twin(src, dst, n):
        return remote(src, dst, t_send.at[n], t_recv.at[n], f, x * 4 + hi * 2 + 1 - core)

    pl.semaphore_wait(barrier, 16)
    shares = [twin(sizes.at[:, pl.ds(give, 16), :], size_theirs, 0)]
    for n in range(2):
        shares.append(twin(packed.at[pl.ds(give + 8 * n, 8)], theirs.at[pl.ds(8 * n, 8)], 1 + n))
    for copy in shares:
        copy.start()
    shares[0].wait_recv()

    turned = []
    for n in range(2):
        one, two = sizes[n, pl.ds(pl.multiple_of(keep, 16), 16), :], size_theirs[n]
        top = jnp.maximum(one, two)
        one, two = jnp.exp2(one - top), jnp.exp2(two - top)
        total = one + two
        whole = top + jnp.log2(total)
        for r in range(16):
            size_both[r, n:n + 1, :] = whole[r:r + 1]
        turned.append(jnp.transpose(
            jnp.concatenate([one / total, two / total, jnp.zeros((96, 128), jnp.float32)], axis=0)))
    low = lax.broadcasted_iota(jnp.int32, (half_rows, 128), 1) < HD
    me = hi * 8 + f

    def send(there, frame):
        r = there * 8 + frame
        stays = (frame == f) & (hi == there)

        @pl.when(stays)
        def _():
            pltpu.make_async_copy(both.at[r], back_ref.at[me], o_recv.at[0]).start()
            pltpu.make_async_copy(size_both.at[r], back_lse.at[me], l_recv.at[0]).start()

        @pl.when(jnp.logical_not(stays))
        def _():
            space = x * 4 + there * 2 + core
            remote(both.at[r], back_ref.at[me], o_send.at[0], o_recv.at[0], frame, space).start()
            remote(size_both.at[r], back_lse.at[me], l_send.at[0], l_recv.at[0], frame, space).start()

    for n in range(2):
        shares[1 + n].wait_recv()
        for r in range(8 * n, 8 * n + 8):
            one = jnp.where(low, turned[0][0:half_rows, r:r + 1], turned[1][0:half_rows, r:r + 1])
            two = jnp.where(low, turned[0][0:half_rows, 16 + r:17 + r], turned[1][0:half_rows, 16 + r:17 + r])
            own = packed[keep + r].astype(jnp.float32)
            both[r] = (own * one + theirs[r].astype(jnp.float32) * two).astype(jnp.bfloat16)
        each(0, 8, lambda d, n=n: send(n, rem(f + 1 + d, 8)))

    for copy in shares:
        copy.wait_send()
    for sem, ref in ((o_send, back_ref.at[pl.ds(0, 15)]), (l_send, back_lse.at[pl.ds(0, 15)]),
                     (o_recv, back_ref), (l_recv, back_lse)):
        pltpu.make_async_copy(ref, ref, sem.at[0]).wait()


def give_results(counts, partial):
    dma = pltpu.SemaphoreType.DMA
    bf16, f32 = jnp.bfloat16, jnp.float32
    half_rows = 2 * SLOT
    return pl.pallas_call(
        return_kernel,
        out_shape=(VMEM((16, half_rows, 128), bf16), VMEM((16, 2, 128), f32)),
        in_specs=[spec(SMEM), spec(VMEM)],
        out_specs=(spec(ANY), spec(ANY)),
        scratch_shapes=[
            VMEM(((partial.shape[0] - 1) * QB // SLOT, SLOT, 128), f32),
            VMEM((32, half_rows, 128), bf16), VMEM((2, 32, 128), f32),
            VMEM((16, half_rows, 128), bf16), VMEM((2, 16, 128), f32),
            VMEM((16, half_rows, 128), bf16), VMEM((16, 2, 128), f32),
            dma((3,)), dma((3,)), dma((1,)), dma((1,)), dma((1,)), dma((1,))],
        compiler_params=pltpu.CompilerParams(
            collective_id=1, has_side_effects=True, vmem_limit_bytes=16 << 20),
        name="give_results",
    )(counts, near(partial))


def finish_kernel(tok_ref, cnt_ref, back_ref, lse_ref, w_ref, o_ref, att, ys):
    times, slots, width = tok_ref.shape
    half = slots * SLOT // 2
    rows = slots * SLOT

    def shares(n):
        sizes = [lse_ref[p * 8:p * 8 + 8, n, :] for p in range(2)]
        top = jnp.maximum(sizes[0], sizes[1])
        powers = [jnp.exp2(v - top) for v in sizes]
        total = powers[0] + powers[1]
        return jnp.transpose(
            jnp.concatenate([v / total for v in powers] + [jnp.zeros((112, 128), jnp.float32)], axis=0))

    first, second = shares(0), shares(1)
    low = lax.broadcasted_iota(jnp.int32, (half, 128), 1) < HD

    def merged(h):
        out = jnp.zeros((half, 128), jnp.float32)
        for p in range(2):
            n = p * 8 + h
            share = jnp.where(low, first[0:half, n:n + 1], second[0:half, n:n + 1])
            out = out + back_ref[n].astype(jnp.float32) * share
        return out

    for j in range(HEADS // 2):
        a, b = merged(2 * j), merged(2 * j + 1)
        cols = slice(128 * j, 128 * j + 128)
        att[0:half, cols] = jnp.where(low, a, pltpu.roll(b, HD, 1)).astype(jnp.bfloat16)
        att[half:rows, cols] = jnp.where(low, pltpu.roll(a, HD, 1), b).astype(jnp.bfloat16)
    for c in range(width // 256):
        cols = slice(256 * c, 256 * c + 256)
        mixed = jnp.dot(att[...], w_ref[:, cols], preferred_element_type=jnp.float32)
        for i in range(slots):
            for e in range(2):
                ys[2 * c + e, pl.ds(i, SLOT, stride=slots), :] = (
                    mixed[i * SLOT:i * SLOT + SLOT, 128 * e:128 * e + 128])
    live = lax.broadcasted_iota(jnp.int32, (slots, width), 0) < cnt_ref[0]
    for t in range(times):
        mixed = jnp.concatenate([ys[c, t * slots:t * slots + slots, :] for c in range(width // 128)], axis=1)
        value = tok_ref[t].astype(jnp.float32) + mixed
        o_ref[t] = jnp.where(live, value, 0.0).astype(jnp.bfloat16)


def finish(tokens, count, back, sizes, w_out):
    times, slots, width = tokens.shape
    rows = slots * SLOT
    return pl.pallas_call(
        finish_kernel,
        out_shape=jax.ShapeDtypeStruct(tokens.shape, tokens.dtype),
        in_specs=[spec(VMEM), spec(SMEM), spec(VMEM), spec(VMEM), spec(VMEM)],
        out_specs=spec(VMEM),
        scratch_shapes=[VMEM((rows, w_out.shape[0]), jnp.bfloat16), VMEM((width // 128, rows, 128), jnp.float32)],
        compiler_params=pltpu.CompilerParams(vmem_limit_bytes=16 << 20),
        name="finish",
    )(near(tokens), count, near(back), near(sizes), near(w_out))


def on_device(tokens, tube_count, ln_gain, ln_bias, w_qkv, w_out):
    tokens = jnp.transpose(tokens, (1, 0, 2))
    q_all, kv_all, counts, tokens, w_out = project(
        tokens, tube_count, ln_gain.reshape(1, -1), ln_bias.reshape(1, -1), w_qkv, w_out)
    partial = attention(counts, q_all, kv_all, tokens.shape[0])
    mixed = finish(tokens, tube_count, *give_results(counts, partial), w_out)
    return jnp.transpose(mixed, (1, 0, 2))


def solution(mesh):
    in_specs = (P("space", "frame", None), P("space"), P(), P(), P(), P())
    return jax.shard_map(
        on_device, mesh=mesh, in_specs=in_specs, out_specs=P("space", "frame", None), check_vma=False)
```

```python
import functools

import jax
import jax.numpy as jnp
from jax import lax
from jax.experimental import pallas as pl
from jax.experimental.pallas import tpu as pltpu
from jax.sharding import PartitionSpec as P

HEADS = 8
HD = 64
SLOT = 40
KB = 256
UN = 8
QB = 512
DEAD = -1e30
Q_AFTER = 2
SAFE = 100.0
EPSILON = 1e-06
SCALE = 1.4426950408889634 / 8.0
ANY = pl.ANY
VMEM = pltpu.VMEM
SMEM = pltpu.SMEM


def spec(space):
    return pl.BlockSpec(memory_space=space)


def near(array):
    return pltpu.with_memory_space_constraint(array, VMEM)


def place():
    f, s = lax.axis_index("frame"), lax.axis_index("space")
    return f, s, div(s, 4), rem(s, 4)


def remote(src, dst, send, recv, frame, space):
    return pltpu.make_async_remote_copy(
        src_ref=src, dst_ref=dst, send_sem=send, recv_sem=recv,
        device_id={"frame": frame, "space": space}, device_id_type=pl.DeviceIdType.MESH)


def rem(a, n):
    return lax.rem(a, jnp.int32(n))


def div(a, n):
    return lax.div(a, jnp.int32(n))


def each(lo, hi, body):
    def step(i, c):
        body(i)
        return c
    lax.fori_loop(lo, hi, step, 0)


def project_kernel(tok_in, cnt_ref, gain_ref, bias_ref, w_ref, w_last, q_out, kv_out, cnt_out, tok_ref, w_next,
                   w_v, xs, nb, kvs, qs, cnts,
                   w_sem, kv_send, kv_recv, q_send, q_recv, c_send, c_recv, x_send, r_send, pass_recv, rest_recv):
    f, s, x, loc = place()
    times, slots, width = tok_ref.shape
    inner = HEADS * HD

    tok_copy = pltpu.make_async_copy(tok_in, tok_ref, w_sem.at[3])
    tok_copy.start()
    last_copy = pltpu.make_async_copy(w_last, w_next, w_sem.at[4])
    copies = []
    for n, at in enumerate((inner, 2 * inner, 0)):
        cols = pl.ds(at, inner)
        copies.append(pltpu.make_async_copy(w_ref.at[:, cols], w_v.at[:, cols], w_sem.at[n]))
    copies[0].start()
    copies[1].start()

    barrier = pltpu.get_barrier_semaphore()

    def greet(frame, space):
        pl.semaphore_signal(barrier, inc=1, device_id={"frame": frame, "space": space},
                            device_id_type=pl.DeviceIdType.MESH)

    each(1, 32, lambda n: greet(rem(f + div(n, 4), 8), x * 4 + rem(loc + n, 4)))
    each(4, 16, lambda n: greet(f, rem(x * 4 + n, 16)))

    cnts[...] = jnp.full(cnts.shape, cnt_ref[0], jnp.int32)

    tok_copy.wait()
    for t in range(SLOT):
        values = tok_ref[t % times].astype(jnp.float32)
        for c in range(width // 128):
            xs[c, t * slots:t * slots + slots, :] = values[:, 128 * c:128 * c + 128]
    for i in range(slots):
        values = jnp.concatenate(
            [xs[c, pl.ds(i, SLOT, stride=slots), :] for c in range(width // 128)], axis=1)
        center = values - jnp.mean(values, axis=-1, keepdims=True)
        spread = jnp.mean(center * center, axis=-1, keepdims=True)
        normed = center * lax.rsqrt(spread + EPSILON) * gain_ref[...] + bias_ref[...]
        nb[i * SLOT:i * SLOT + SLOT, :] = normed.astype(jnp.bfloat16)

    rows_all = slots * SLOT
    half = rows_all // 2
    low = lax.broadcasted_iota(jnp.int32, (rows_all, 128), 1) < HD
    low_half = lax.broadcasted_iota(jnp.int32, (half, 128), 1) < HD

    copies[0].wait()
    copies[1].wait()
    copies[2].start()
    for g in range(2):
        k4 = jnp.dot(nb[...], w_v[:, inner + 256 * g:inner + 256 * g + 256], preferred_element_type=jnp.float32)
        v4 = jnp.dot(nb[...], w_v[:, 2 * inner + 256 * g:2 * inner + 256 * g + 256],
                     preferred_element_type=jnp.float32)
        for j in range(2):
            k2, v2 = k4[:, 128 * j:128 * j + 128], v4[:, 128 * j:128 * j + 128]
            h = 4 * g + 2 * j
            kvs[h] = jnp.where(low, k2, pltpu.roll(v2, HD, 1)).astype(jnp.bfloat16)
            kvs[h + 1] = jnp.where(low, pltpu.roll(k2, HD, 1), v2).astype(jnp.bfloat16)

    part = div(f, 2)
    mine = rem(f, 2) * 4 + loc
    source = x * 8 + mine
    pl.semaphore_wait(barrier, 43)

    def kv_copy(d):
        h = rem(f + d + 2 * loc, 8)
        stays = (h == f) & (part == loc)
        return stays, h, remote(
            kvs.at[h], kv_out.at[source], kv_send.at[0], kv_recv.at[mine], h, x * 4 + part)

    def kv_start(d):
        stays, h, copy = kv_copy(d)

        @pl.when(stays)
        def _():
            pltpu.make_async_copy(kvs.at[h], kv_out.at[source], kv_recv.at[mine]).start()

        @pl.when(jnp.logical_not(stays))
        def _():
            copy.start()

    each(0, 8, kv_start)

    def count_copy(e):
        return remote(cnts, cnt_out.at[s], c_send.at[0], c_recv.at[0], f, rem(s + e, 16))

    each(1, 16, lambda e: count_copy(e).start())
    pltpu.make_async_copy(cnts, cnt_out.at[s], c_recv.at[0]).start()

    copies[2].wait()
    last_copy.start()
    for g in range(2):
        q4 = jnp.dot(nb[...], w_v[:, 256 * g:256 * g + 256], preferred_element_type=jnp.float32) * SCALE
        for j in range(2):
            q2 = q4[:, 128 * j:128 * j + 128]
            h = 4 * g + 2 * j
            qs[h] = jnp.where(low_half, q2[:half], pltpu.roll(q2[half:], HD, 1)).astype(jnp.bfloat16)
            qs[h + 1] = jnp.where(low_half, pltpu.roll(q2[:half], HD, 1), q2[half:]).astype(jnp.bfloat16)

    me = f * 4 + loc

    def q_copy(n):
        h = rem(f + div(n, 4), 8)
        return remote(qs.at[h], q_out.at[me], q_send.at[0], q_recv.at[0], h, x * 4 + rem(loc + n, 4))

    def ring(piece, send, recv, step):
        return remote(kv_out.at[piece], kv_out.at[piece], send.at[0], recv, f, rem(x + step, 4) * 4 + loc)

    def nth(t):
        u = rem(f - 2 * loc - t + 16, 8)
        return rem(u, 2) * 4 + div(u, 2)

    right, left = rem(x + 1, 4) * 8, rem(x + 3, 4) * 8

    def landed(sem, ref):
        pltpu.make_async_copy(ref, ref, sem).wait()

    def to_right(t, piece):
        even = rem(t, 2) == 0

        @pl.when(even)
        def _():
            ring(piece, x_send, pass_recv.at[t], 1).start()

        @pl.when(jnp.logical_not(even))
        def _():
            ring(piece, x_send, rest_recv.at[0], 1).start()

    def to_left(t, piece):
        odd = rem(t, 2) == 1

        @pl.when(odd)
        def _():
            ring(piece, x_send, pass_recv.at[t], 3).start()

        @pl.when(jnp.logical_not(odd))
        def _():
            ring(piece, x_send, rest_recv.at[0], 3).start()

    def arrived(t):
        i = nth(t)
        piece = x * 8 + i
        landed(kv_recv.at[i], kv_out.at[piece])
        to_right(t, piece)
        to_left(t, piece)

    each(0, Q_AFTER, arrived)
    each(1, 32, lambda n: q_copy(n).start())
    pltpu.make_async_copy(qs.at[f], q_out.at[me], q_recv.at[0]).start()
    each(Q_AFTER, 8, arrived)

    def relay(t):
        piece = left + nth(2 * t)
        landed(pass_recv.at[2 * t], kv_out.at[piece])
        ring(piece, r_send, rest_recv.at[0], 1).start()
        piece = right + nth(2 * t + 1)
        landed(pass_recv.at[2 * t + 1], kv_out.at[piece])
        ring(piece, r_send, rest_recv.at[0], 3).start()

    each(0, 4, relay)

    last_copy.wait()
    landed(kv_send.at[0], kv_out.at[pl.ds(0, 7)])

    @pl.when(part != loc)
    def _():
        landed(kv_send.at[0], kv_out.at[0])

    landed(c_send.at[0], cnt_out.at[pl.ds(0, 15)])
    landed(q_send.at[0], q_out.at[pl.ds(0, 31)])
    landed(x_send.at[0], kv_out.at[pl.ds(0, 16)])
    landed(r_send.at[0], kv_out.at[pl.ds(0, 8)])
    landed(c_recv.at[0], cnt_out)
    landed(q_recv.at[0], q_out)
    landed(rest_recv.at[0], kv_out.at[pl.ds(0, 16)])


def project(tokens, count, gain, bias, w_qkv, w_out):
    times, slots, width = tokens.shape
    rows = slots * SLOT
    bf16, i32 = jnp.bfloat16, jnp.int32
    dma = pltpu.SemaphoreType.DMA
    return pl.pallas_call(
        project_kernel,
        out_shape=(VMEM((32, rows // 2, 128), bf16),
                   VMEM((32, rows, 128), bf16),
                   VMEM((16, 1, 128), i32),
                   VMEM(tokens.shape, bf16), VMEM(w_out.shape, bf16)),
        in_specs=[spec(pltpu.HBM), spec(SMEM), spec(VMEM), spec(VMEM), spec(pltpu.HBM), spec(pltpu.HBM)],
        out_specs=(spec(ANY), spec(ANY), spec(ANY), spec(VMEM), spec(ANY)),
        scratch_shapes=[
            VMEM(w_qkv.shape, bf16), VMEM((width // 128, rows, 128), jnp.float32), VMEM((rows, width), bf16),
            VMEM((HEADS, rows, 128), bf16), VMEM((HEADS, rows // 2, 128), bf16), VMEM((1, 128), i32),
            dma((5,)), dma((1,)), dma((8,)), dma((1,)), dma((1,)), dma((1,)), dma((1,)),
            dma((1,)), dma((1,)), dma((8,)), dma((1,)),
        ],
        compiler_params=pltpu.CompilerParams(collective_id=0, has_side_effects=True),
        name="project",
    )(tokens, count, gain, bias, w_qkv, w_out)


def attention_kernel(cnt_ref, q_ref, kv_ref, acc, kvc, qc, vt, qt, *held, times):
    base = (lax.axis_index("space") // 4) * 4
    kv_flat = kvc.reshape(kvc.shape[0] * SLOT, 128)
    q_flat = qc.reshape(qc.shape[0] * SLOT, 128)
    step_keys = KB

    def take_keys(n, unit):
        for j in range(4):
            for sub in range(2):
                kvc[unit + 2 * j + sub] = kv_ref[n // 4, sub, n % 4, j * SLOT:j * SLOT + SLOT, :]
        return unit + 2 * cnt_ref[n, 0, 0]

    unit = jnp.int32(0)
    for n in range(16):
        unit = take_keys(n, unit)
    key_units = unit
    for n in range(-(-step_keys // SLOT)):
        kvc[key_units + n] = kv_ref[0, 0, 0, 0:SLOT, :]

    unit = jnp.int32(0)
    for j in range(4):
        if j == 2:
            low_units = unit
        for l in range(4):
            live = j < cnt_ref[base + l, 0, 0]
            for f in range(8):
                qc[unit + f] = q_ref[f, l, (j % 2) * SLOT:(j % 2) * SLOT + SLOT, :]
            unit = unit + jnp.where(live, 8, 0)
    query_rows = unit * SLOT
    query_tiles = (query_rows + QB - 1) // QB
    key_rows = key_units * SLOT
    key_steps = (key_rows + step_keys - 1) // step_keys

    key_at = lax.broadcasted_iota(jnp.int32, (HD, KB), 1)
    row16 = lax.broadcasted_iota(jnp.int32, (16, KB), 0)

    def shape_keys(b, longest):
        turned = jnp.transpose(kv_flat[pl.ds(pl.multiple_of(b * KB, KB), KB), :].astype(jnp.float32))
        index = key_at + b * KB
        live = (index % SLOT < times) & (index < key_rows)
        vt[b, 0:HD, :] = jnp.where(live, turned[HD:], 0.0).astype(jnp.bfloat16)
        vt[b, HD:HD + 16, :] = jnp.where(live[:16] & (row16 == 0), 1.0, 0.0).astype(jnp.bfloat16)
        keys = turned[:HD]
        return jnp.maximum(longest, jnp.sum(keys * keys, axis=0, keepdims=True))

    longest_key = lax.fori_loop(0, key_steps, shape_keys, jnp.zeros((1, KB), jnp.float32))

    col = lax.broadcasted_iota(jnp.int32, (HD, QB), 1)
    low_rows = low_units * SLOT

    def shape_queries(t, longest):
        turned = jnp.transpose(q_flat[pl.ds(pl.multiple_of(t * QB, QB), QB), :].astype(jnp.float32))
        index = col + t * QB
        query = jnp.where(index < low_rows, turned[:HD], turned[HD:])
        query = jnp.where(index < query_rows, query, 0.0)
        qt[t, 0:HD, :] = query.astype(jnp.bfloat16)
        qt[t, HD:, :] = jnp.zeros((HD, QB), jnp.bfloat16)
        return jnp.maximum(longest, jnp.sum(query * query, axis=0, keepdims=True))

    longest_query = lax.fori_loop(0, query_tiles, shape_queries, jnp.zeros((1, QB), jnp.float32))
    safe = jnp.max(longest_key) * jnp.max(longest_query) < SAFE * SAFE

    def block_scores(b, t):
        keys = kv_flat[pl.ds(pl.multiple_of(b * KB, KB), KB), :]
        return jnp.dot(keys, qt[t], preferred_element_type=jnp.float32)

    def clear(t):
        acc[t] = jnp.zeros((HD + 16, QB), jnp.float32)

    def after(item):
        t, b = item
        turn = b + 1 == key_steps
        return jnp.minimum(jnp.where(turn, t + 1, t), query_tiles), jnp.where(turn, 0, b + 1)

    def add(u, item):
        t, b = item
        acc[t] += jnp.dot(vt[b], held[u][...], preferred_element_type=jnp.float32)

    def weigh(u, item):
        t, b = item
        held[u][...] = jnp.exp2(block_scores(b, t)).astype(jnp.bfloat16)

    def plain(i, carry):
        before, now = carry
        then = now[-1]
        later = []
        for u in range(UN):
            add(u, before[u])
            weigh(u, now[u])
            then = after(then)
            later.append(then)
        return now, tuple(later)

    def plain_all():
        each(0, query_tiles, clear)
        first = [(jnp.int32(0), jnp.int32(0))]
        for _ in range(UN - 1):
            first.append(after(first[-1]))
        for u in range(UN):
            weigh(u, first[u])
        second = [after(first[-1])]
        for _ in range(UN - 1):
            second.append(after(second[-1]))
        steps = (query_tiles * key_steps + UN - 1) // UN
        last, _ = lax.fori_loop(1, steps, plain, (tuple(first), tuple(second)))
        for u in range(UN):
            add(u, last[u])

    def shifted_tile(t):
        def step(b, carry):
            best, total = carry
            scores = block_scores(b, t)
            best_next = jnp.maximum(best, jnp.max(scores, axis=0, keepdims=True))
            weights = jnp.exp2(scores - best_next).astype(jnp.bfloat16)
            total = total * jnp.exp2(best - best_next) + jnp.dot(
                vt[b], weights, preferred_element_type=jnp.float32)
            return best_next, total

        best, total = lax.fori_loop(
            0, key_steps, step,
            (jnp.full((1, QB), DEAD, jnp.float32), jnp.zeros((HD + 16, QB), jnp.float32)))
        acc[t] = total
        acc[t, HD + 8:HD + 9, :] = best

    @pl.when(safe)
    def _():
        plain_all()

    @pl.when(jnp.logical_not(safe))
    def _():
        each(0, query_tiles, shifted_tile)


def attention(counts, q_all, kv_all, times):
    sources, half_rows, _ = q_all.shape
    q_units, k_units = 4 * sources, 4 * sources
    q_rows = (q_units * SLOT + QB - 1) // QB * QB
    step = KB
    k_rows = (k_units * SLOT + step - 1) // step * step
    fill = -(-step // SLOT)
    return pl.pallas_call(
        functools.partial(attention_kernel, times=times),
        out_shape=VMEM((q_rows // QB + 1, HD + 16, QB), jnp.float32),
        in_specs=[spec(SMEM), spec(VMEM), spec(VMEM)],
        out_specs=spec(VMEM),
        scratch_shapes=[
            VMEM((k_units + max(fill, 8), SLOT, 128), jnp.bfloat16),
            VMEM((q_units + 8, SLOT, 128), jnp.bfloat16),
            VMEM((k_rows // KB, HD + 16, KB), jnp.bfloat16),
            VMEM((q_rows // QB + 1, 128, QB), jnp.bfloat16),
            *[VMEM((KB, QB), jnp.bfloat16) for _ in range(UN)],
        ],
        compiler_params=pltpu.CompilerParams(vmem_limit_bytes=32 << 20),
        name="attention",
    )(counts, near(q_all.reshape(8, 4, half_rows, 128)),
      near(kv_all.reshape(4, 2, 4, 2 * half_rows, 128)))


def return_kernel(cnt_ref, acc, back_ref, back_lse, of, packed, sizes, theirs, size_theirs, both, size_both,
                  t_send, t_recv, o_send, o_recv, l_send, l_recv):
    f, _, x, loc = place()
    hi, core = div(loc, 2), rem(loc, 2)
    half_rows = packed.shape[1]
    barrier = pltpu.get_barrier_semaphore()

    def greet(frame, there):
        pl.semaphore_signal(barrier, inc=1, device_id={"frame": frame, "space": x * 4 + there},
                            device_id_type=pl.DeviceIdType.MESH)

    greet(f, hi * 2 + 1 - core)
    for n in range(1, 16):
        greet(rem(f + n // 2, 8), rem(hi + n, 2) * 2 + core)

    starts, unit = [], jnp.int32(0)
    for j in range(4):
        for l in range(4):
            live = j < cnt_ref[x * 4 + l, 0, 0]
            starts.append(jnp.where(live, unit, 0))
            unit = unit + jnp.where(live, 8, 0)
        if j == 1:
            low_rows = unit * SLOT
    lane = lax.broadcasted_iota(jnp.int32, (SLOT, 128), 1)
    in_low = lane < HD
    of_flat = of.reshape(of.shape[0] * SLOT, 128)
    col = lax.broadcasted_iota(jnp.int32, (HD, QB), 1)

    def put(t):
        weight_sum = acc[t, HD:HD + 1, :]
        out = acc[t, 0:HD, :] / weight_sum
        lse = jnp.broadcast_to(acc[t, HD + 8:HD + 9, :] + jnp.log2(weight_sum), (HD, QB))
        low = col + t * QB < low_rows
        both = jnp.concatenate([jnp.where(low, out, lse), jnp.where(low, lse, out)], axis=0)
        of_flat[pl.ds(pl.multiple_of(t * QB, QB), QB), :] = jnp.transpose(both)

    each(0, acc.shape[0] - 1, put)

    def gather(frame, kept):
        for l in range(4):
            i = (l % 2) * 16 + (l // 2) * 8
            for j in range(2):
                first = of[starts[j * 4 + l] + frame]
                second = of[starts[j * 4 + 8 + l] + frame]
                packed[i + frame, j * SLOT:j * SLOT + SLOT, :] = jnp.where(in_low, first, second).astype(jnp.bfloat16)
                kept[j] = jnp.where(rem(lane, HD) == i + frame, jnp.where(in_low, second, first), kept[j])
        return kept

    kept = lax.fori_loop(0, 8, gather, [jnp.zeros((SLOT, 128), jnp.float32)] * 2)
    rows = jnp.transpose(jnp.concatenate([*kept, jnp.zeros((128 - 2 * SLOT, 128), jnp.float32)], axis=0))
    sizes[0] = rows[HD:HD + 32]
    sizes[1] = rows[0:32]

    keep = core * 16
    give = 16 - keep

    def twin(src, dst, n):
        return remote(src, dst, t_send.at[n], t_recv.at[n], f, x * 4 + hi * 2 + 1 - core)

    pl.semaphore_wait(barrier, 16)
    shares = [twin(sizes.at[:, pl.ds(give, 16), :], size_theirs, 0)]
    for n in range(2):
        shares.append(twin(packed.at[pl.ds(give + 8 * n, 8)], theirs.at[pl.ds(8 * n, 8)], 1 + n))
    for copy in shares:
        copy.start()
    shares[0].wait_recv()

    turned = []
    for n in range(2):
        one, two = sizes[n, pl.ds(pl.multiple_of(keep, 16), 16), :], size_theirs[n]
        top = jnp.maximum(one, two)
        one, two = jnp.exp2(one - top), jnp.exp2(two - top)
        total = one + two
        whole = top + jnp.log2(total)
        for r in range(16):
            size_both[r, n:n + 1, :] = whole[r:r + 1]
        turned.append(jnp.transpose(
            jnp.concatenate([one / total, two / total, jnp.zeros((96, 128), jnp.float32)], axis=0)))
    low = lax.broadcasted_iota(jnp.int32, (half_rows, 128), 1) < HD
    me = hi * 8 + f

    def send(there, frame):
        r = there * 8 + frame
        stays = (frame == f) & (hi == there)

        @pl.when(stays)
        def _():
            pltpu.make_async_copy(both.at[r], back_ref.at[me], o_recv.at[0]).start()
            pltpu.make_async_copy(size_both.at[r], back_lse.at[me], l_recv.at[0]).start()

        @pl.when(jnp.logical_not(stays))
        def _():
            space = x * 4 + there * 2 + core
            remote(both.at[r], back_ref.at[me], o_send.at[0], o_recv.at[0], frame, space).start()
            remote(size_both.at[r], back_lse.at[me], l_send.at[0], l_recv.at[0], frame, space).start()

    for n in range(2):
        shares[1 + n].wait_recv()
        for r in range(8 * n, 8 * n + 8):
            one = jnp.where(low, turned[0][0:half_rows, r:r + 1], turned[1][0:half_rows, r:r + 1])
            two = jnp.where(low, turned[0][0:half_rows, 16 + r:17 + r], turned[1][0:half_rows, 16 + r:17 + r])
            own = packed[keep + r].astype(jnp.float32)
            both[r] = (own * one + theirs[r].astype(jnp.float32) * two).astype(jnp.bfloat16)
        each(0, 8, lambda d, n=n: send(n, rem(f + 1 + d, 8)))

    for copy in shares:
        copy.wait_send()
    for sem, ref in ((o_send, back_ref.at[pl.ds(0, 15)]), (l_send, back_lse.at[pl.ds(0, 15)]),
                     (o_recv, back_ref), (l_recv, back_lse)):
        pltpu.make_async_copy(ref, ref, sem.at[0]).wait()


def give_results(counts, partial):
    dma = pltpu.SemaphoreType.DMA
    bf16, f32 = jnp.bfloat16, jnp.float32
    half_rows = 2 * SLOT
    return pl.pallas_call(
        return_kernel,
        out_shape=(VMEM((16, half_rows, 128), bf16), VMEM((16, 2, 128), f32)),
        in_specs=[spec(SMEM), spec(VMEM)],
        out_specs=(spec(ANY), spec(ANY)),
        scratch_shapes=[
            VMEM(((partial.shape[0] - 1) * QB // SLOT, SLOT, 128), f32),
            VMEM((32, half_rows, 128), bf16), VMEM((2, 32, 128), f32),
            VMEM((16, half_rows, 128), bf16), VMEM((2, 16, 128), f32),
            VMEM((16, half_rows, 128), bf16), VMEM((16, 2, 128), f32),
            dma((3,)), dma((3,)), dma((1,)), dma((1,)), dma((1,)), dma((1,))],
        compiler_params=pltpu.CompilerParams(
            collective_id=1, has_side_effects=True, vmem_limit_bytes=16 << 20),
        name="give_results",
    )(counts, near(partial))


def finish_kernel(tok_ref, cnt_ref, back_ref, lse_ref, w_ref, o_ref, att, ys, done, o_sem):
    times, slots, width = tok_ref.shape
    half = slots * SLOT // 2
    rows = slots * SLOT

    def shares(n):
        sizes = [lse_ref[p * 8:p * 8 + 8, n, :] for p in range(2)]
        top = jnp.maximum(sizes[0], sizes[1])
        powers = [jnp.exp2(v - top) for v in sizes]
        total = powers[0] + powers[1]
        return jnp.transpose(
            jnp.concatenate([v / total for v in powers] + [jnp.zeros((112, 128), jnp.float32)], axis=0))

    first, second = shares(0), shares(1)
    low = lax.broadcasted_iota(jnp.int32, (half, 128), 1) < HD

    def merged(h):
        out = jnp.zeros((half, 128), jnp.float32)
        for p in range(2):
            n = p * 8 + h
            share = jnp.where(low, first[0:half, n:n + 1], second[0:half, n:n + 1])
            out = out + back_ref[n].astype(jnp.float32) * share
        return out

    for j in range(HEADS // 2):
        a, b = merged(2 * j), merged(2 * j + 1)
        cols = slice(128 * j, 128 * j + 128)
        att[0:half, cols] = jnp.where(low, a, pltpu.roll(b, HD, 1)).astype(jnp.bfloat16)
        att[half:rows, cols] = jnp.where(low, pltpu.roll(a, HD, 1), b).astype(jnp.bfloat16)
    for c in range(width // 256):
        cols = slice(256 * c, 256 * c + 256)
        mixed = jnp.dot(att[...], w_ref[:, cols], preferred_element_type=jnp.float32)
        for i in range(slots):
            for e in range(2):
                ys[2 * c + e, pl.ds(i, SLOT, stride=slots), :] = (
                    mixed[i * SLOT:i * SLOT + SLOT, 128 * e:128 * e + 128])
    live = lax.broadcasted_iota(jnp.int32, (slots, width), 0) < cnt_ref[0]
    ends, copies = [times // 4, times // 2, times * 3 // 4, times], []
    for t in range(times):
        mixed = jnp.concatenate([ys[c, t * slots:t * slots + slots, :] for c in range(width // 128)], axis=1)
        value = tok_ref[t].astype(jnp.float32) + mixed
        done[t] = jnp.where(live, value, 0.0).astype(jnp.bfloat16)
        if t + 1 in ends:
            n = ends.index(t + 1)
            rows = pl.ds(ends[n - 1] if n else 0, ends[n] - (ends[n - 1] if n else 0))
            copies.append(pltpu.make_async_copy(done.at[rows], o_ref.at[rows], o_sem.at[n]))
            copies[n].start()
    for copy in copies:
        copy.wait()


def finish(tokens, count, back, sizes, w_out):
    times, slots, width = tokens.shape
    rows = slots * SLOT
    return pl.pallas_call(
        finish_kernel,
        out_shape=jax.ShapeDtypeStruct(tokens.shape, tokens.dtype),
        in_specs=[spec(VMEM), spec(SMEM), spec(VMEM), spec(VMEM), spec(VMEM)],
        out_specs=spec(ANY),
        scratch_shapes=[VMEM((rows, w_out.shape[0]), jnp.bfloat16), VMEM((width // 128, rows, 128), jnp.float32),
                        VMEM(tokens.shape, tokens.dtype), pltpu.SemaphoreType.DMA((4,))],
        compiler_params=pltpu.CompilerParams(vmem_limit_bytes=16 << 20),
        name="finish",
    )(near(tokens), count, near(back), near(sizes), near(w_out))


def on_device(tokens, tube_count, ln_gain, ln_bias, w_qkv, w_out):
    tokens = jnp.transpose(tokens, (1, 0, 2))
    q_all, kv_all, counts, tokens, w_out = project(
        tokens, tube_count, ln_gain.reshape(1, -1), ln_bias.reshape(1, -1), w_qkv, w_out)
    partial = attention(counts, q_all, kv_all, tokens.shape[0])
    mixed = finish(tokens, tube_count, *give_results(counts, partial), w_out)
    return jnp.transpose(mixed, (1, 0, 2))


def solution(mesh):
    in_specs = (P("space", "frame", None), P("space"), P(), P(), P(), P())
    return jax.shard_map(
        on_device, mesh=mesh, in_specs=in_specs, out_specs=P("space", "frame", None), check_vma=False)
```

```python
import functools

import jax
import jax.numpy as jnp
from jax import lax
from jax.experimental import pallas as pl
from jax.experimental.pallas import tpu as pltpu
from jax.sharding import PartitionSpec as P

HEADS = 8
HD = 64
SLOT = 40
KB = 256
UN = 8
QB = 512
DEAD = -1e30
Q_AFTER = 2
SAFE = 100.0
EPSILON = 1e-06
SCALE = 1.4426950408889634 / 8.0
ANY = pl.ANY
VMEM = pltpu.VMEM
SMEM = pltpu.SMEM


def spec(space):
    return pl.BlockSpec(memory_space=space)


def near(array):
    return pltpu.with_memory_space_constraint(array, VMEM)


def place():
    f, s = lax.axis_index("frame"), lax.axis_index("space")
    return f, s, div(s, 4), rem(s, 4)


def remote(src, dst, send, recv, frame, space):
    return pltpu.make_async_remote_copy(
        src_ref=src, dst_ref=dst, send_sem=send, recv_sem=recv,
        device_id={"frame": frame, "space": space}, device_id_type=pl.DeviceIdType.MESH)


def rem(a, n):
    return lax.rem(a, jnp.int32(n))


def div(a, n):
    return lax.div(a, jnp.int32(n))


def each(lo, hi, body):
    def step(i, c):
        body(i)
        return c
    lax.fori_loop(lo, hi, step, 0)


def project_kernel(tok_in, cnt_ref, gain_ref, bias_ref, w_ref, w_last, q_out, kv_out, cnt_out, tok_ref, w_next,
                   w_v, xs, nb, kvs, qs, cnts,
                   w_sem, kv_send, kv_recv, q_send, q_recv, c_send, c_recv, x_send, r_send, pass_recv, rest_recv):
    f, s, x, loc = place()
    times, slots, width = tok_ref.shape
    inner = HEADS * HD

    tok_copy = pltpu.make_async_copy(tok_in, tok_ref, w_sem.at[3])
    tok_copy.start()
    last_copy = pltpu.make_async_copy(w_last, w_next, w_sem.at[4])
    copies = []
    for n, at in enumerate((inner, 2 * inner, 0)):
        cols = pl.ds(at, inner)
        copies.append(pltpu.make_async_copy(w_ref.at[:, cols], w_v.at[:, cols], w_sem.at[n]))
    copies[0].start()
    copies[1].start()

    barrier = pltpu.get_barrier_semaphore()

    def greet(frame, space):
        pl.semaphore_signal(barrier, inc=1, device_id={"frame": frame, "space": space},
                            device_id_type=pl.DeviceIdType.MESH)

    each(1, 32, lambda n: greet(rem(f + div(n, 4), 8), x * 4 + rem(loc + n, 4)))
    each(4, 16, lambda n: greet(f, rem(x * 4 + n, 16)))

    cnts[...] = jnp.full(cnts.shape, cnt_ref[0], jnp.int32)

    tok_copy.wait()
    for t in range(SLOT):
        values = tok_ref[t % times].astype(jnp.float32)
        for c in range(width // 128):
            xs[c, t * slots:t * slots + slots, :] = values[:, 128 * c:128 * c + 128]
    for i in range(slots):
        values = jnp.concatenate(
            [xs[c, pl.ds(i, SLOT, stride=slots), :] for c in range(width // 128)], axis=1)
        center = values - jnp.mean(values, axis=-1, keepdims=True)
        spread = jnp.mean(center * center, axis=-1, keepdims=True)
        normed = center * lax.rsqrt(spread + EPSILON) * gain_ref[...] + bias_ref[...]
        nb[i * SLOT:i * SLOT + SLOT, :] = normed.astype(jnp.bfloat16)

    rows_all = slots * SLOT
    half = rows_all // 2
    low = lax.broadcasted_iota(jnp.int32, (rows_all, 128), 1) < HD
    low_half = lax.broadcasted_iota(jnp.int32, (half, 128), 1) < HD

    copies[0].wait()
    copies[1].wait()
    copies[2].start()
    for g in range(2):
        k4 = jnp.dot(nb[...], w_v[:, inner + 256 * g:inner + 256 * g + 256], preferred_element_type=jnp.float32)
        v4 = jnp.dot(nb[...], w_v[:, 2 * inner + 256 * g:2 * inner + 256 * g + 256],
                     preferred_element_type=jnp.float32)
        for j in range(2):
            k2, v2 = k4[:, 128 * j:128 * j + 128], v4[:, 128 * j:128 * j + 128]
            h = 4 * g + 2 * j
            kvs[h] = jnp.where(low, k2, pltpu.roll(v2, HD, 1)).astype(jnp.bfloat16)
            kvs[h + 1] = jnp.where(low, pltpu.roll(k2, HD, 1), v2).astype(jnp.bfloat16)

    part = div(f, 2)
    mine = rem(f, 2) * 4 + loc
    source = x * 8 + mine
    pl.semaphore_wait(barrier, 43)

    def kv_copy(d):
        h = rem(f + d + 2 * loc, 8)
        stays = (h == f) & (part == loc)
        return stays, h, remote(
            kvs.at[h], kv_out.at[source], kv_send.at[0], kv_recv.at[mine], h, x * 4 + part)

    def kv_start(d):
        stays, h, copy = kv_copy(d)

        @pl.when(stays)
        def _():
            pltpu.make_async_copy(kvs.at[h], kv_out.at[source], kv_recv.at[mine]).start()

        @pl.when(jnp.logical_not(stays))
        def _():
            copy.start()

    each(0, 8, kv_start)

    def count_copy(e):
        return remote(cnts, cnt_out.at[s], c_send.at[0], c_recv.at[0], f, rem(s + e, 16))

    each(1, 16, lambda e: count_copy(e).start())
    pltpu.make_async_copy(cnts, cnt_out.at[s], c_recv.at[0]).start()

    copies[2].wait()
    last_copy.start()
    for g in range(2):
        q4 = jnp.dot(nb[...], w_v[:, 256 * g:256 * g + 256], preferred_element_type=jnp.float32) * SCALE
        for j in range(2):
            q2 = q4[:, 128 * j:128 * j + 128]
            h = 4 * g + 2 * j
            qs[h] = jnp.where(low_half, q2[:half], pltpu.roll(q2[half:], HD, 1)).astype(jnp.bfloat16)
            qs[h + 1] = jnp.where(low_half, pltpu.roll(q2[:half], HD, 1), q2[half:]).astype(jnp.bfloat16)

    me = f * 4 + loc

    def q_copy(n):
        h = rem(f + div(n, 4), 8)
        return remote(qs.at[h], q_out.at[me], q_send.at[0], q_recv.at[0], h, x * 4 + rem(loc + n, 4))

    def ring(piece, send, recv, step):
        return remote(kv_out.at[piece], kv_out.at[piece], send.at[0], recv, f, rem(x + step, 4) * 4 + loc)

    def nth(t):
        u = rem(f - 2 * loc - t + 16, 8)
        return rem(u, 2) * 4 + div(u, 2)

    right, left = rem(x + 1, 4) * 8, rem(x + 3, 4) * 8

    def landed(sem, ref):
        pltpu.make_async_copy(ref, ref, sem).wait()

    def to_right(t, piece):
        even = rem(t, 2) == 0

        @pl.when(even)
        def _():
            ring(piece, x_send, pass_recv.at[t], 1).start()

        @pl.when(jnp.logical_not(even))
        def _():
            ring(piece, x_send, rest_recv.at[0], 1).start()

    def to_left(t, piece):
        odd = rem(t, 2) == 1

        @pl.when(odd)
        def _():
            ring(piece, x_send, pass_recv.at[t], 3).start()

        @pl.when(jnp.logical_not(odd))
        def _():
            ring(piece, x_send, rest_recv.at[0], 3).start()

    def arrived(t):
        i = nth(t)
        piece = x * 8 + i
        landed(kv_recv.at[i], kv_out.at[piece])
        to_right(t, piece)
        to_left(t, piece)

    each(0, Q_AFTER, arrived)
    each(1, 32, lambda n: q_copy(n).start())
    pltpu.make_async_copy(qs.at[f], q_out.at[me], q_recv.at[0]).start()
    each(Q_AFTER, 8, arrived)

    def relay(t):
        piece = left + nth(2 * t)
        landed(pass_recv.at[2 * t], kv_out.at[piece])
        ring(piece, r_send, rest_recv.at[0], 1).start()
        piece = right + nth(2 * t + 1)
        landed(pass_recv.at[2 * t + 1], kv_out.at[piece])
        ring(piece, r_send, rest_recv.at[0], 3).start()

    each(0, 4, relay)

    last_copy.wait()
    landed(kv_send.at[0], kv_out.at[pl.ds(0, 7)])

    @pl.when(part != loc)
    def _():
        landed(kv_send.at[0], kv_out.at[0])

    landed(c_send.at[0], cnt_out.at[pl.ds(0, 15)])
    landed(q_send.at[0], q_out.at[pl.ds(0, 31)])
    landed(x_send.at[0], kv_out.at[pl.ds(0, 16)])
    landed(r_send.at[0], kv_out.at[pl.ds(0, 8)])
    landed(c_recv.at[0], cnt_out)
    landed(q_recv.at[0], q_out)
    landed(rest_recv.at[0], kv_out.at[pl.ds(0, 16)])


def project(tokens, count, gain, bias, w_qkv, w_out):
    times, slots, width = tokens.shape
    rows = slots * SLOT
    bf16, i32 = jnp.bfloat16, jnp.int32
    dma = pltpu.SemaphoreType.DMA
    return pl.pallas_call(
        project_kernel,
        out_shape=(VMEM((32, rows // 2, 128), bf16),
                   VMEM((32, rows, 128), bf16),
                   VMEM((16, 1, 128), i32),
                   VMEM(tokens.shape, bf16), VMEM(w_out.shape, bf16)),
        in_specs=[spec(pltpu.HBM), spec(SMEM), spec(VMEM), spec(VMEM), spec(pltpu.HBM), spec(pltpu.HBM)],
        out_specs=(spec(ANY), spec(ANY), spec(ANY), spec(VMEM), spec(ANY)),
        scratch_shapes=[
            VMEM(w_qkv.shape, bf16), VMEM((width // 128, rows, 128), jnp.float32), VMEM((rows, width), bf16),
            VMEM((HEADS, rows, 128), bf16), VMEM((HEADS, rows // 2, 128), bf16), VMEM((1, 128), i32),
            dma((5,)), dma((1,)), dma((8,)), dma((1,)), dma((1,)), dma((1,)), dma((1,)),
            dma((1,)), dma((1,)), dma((8,)), dma((1,)),
        ],
        compiler_params=pltpu.CompilerParams(collective_id=0, has_side_effects=True),
        name="project",
    )(tokens, count, gain, bias, w_qkv, w_out)


def attention_kernel(cnt_ref, q_ref, kv_ref, acc, kvc, qc, vt, qt, *held, times):
    base = (lax.axis_index("space") // 4) * 4
    kv_flat = kvc.reshape(kvc.shape[0] * SLOT, 128)
    q_flat = qc.reshape(qc.shape[0] * SLOT, 128)
    step_keys = KB

    def take_keys(n, unit):
        for j in range(4):
            for sub in range(2):
                kvc[unit + 2 * j + sub] = kv_ref[n // 4, sub, n % 4, j * SLOT:j * SLOT + SLOT, :]
        return unit + 2 * cnt_ref[n, 0, 0]

    unit = jnp.int32(0)
    for n in range(16):
        unit = take_keys(n, unit)
    key_units = unit
    for n in range(-(-step_keys // SLOT)):
        kvc[key_units + n] = kv_ref[0, 0, 0, 0:SLOT, :]

    unit = jnp.int32(0)
    for j in range(4):
        if j == 2:
            low_units = unit
        for l in range(4):
            live = j < cnt_ref[base + l, 0, 0]
            for f in range(8):
                qc[unit + f] = q_ref[f, l, (j % 2) * SLOT:(j % 2) * SLOT + SLOT, :]
            unit = unit + jnp.where(live, 8, 0)
    query_rows = unit * SLOT
    query_tiles = (query_rows + QB - 1) // QB
    key_rows = key_units * SLOT
    key_steps = (key_rows + step_keys - 1) // step_keys

    key_at = lax.broadcasted_iota(jnp.int32, (HD, KB), 1)
    row16 = lax.broadcasted_iota(jnp.int32, (16, KB), 0)

    def shape_keys(b, longest):
        turned = jnp.transpose(kv_flat[pl.ds(pl.multiple_of(b * KB, KB), KB), :])
        index = key_at + b * KB
        live = (index % SLOT < times) & (index < key_rows)
        vt[b, 0:HD, :] = jnp.where(live, turned[HD:], jnp.bfloat16(0.0))
        vt[b, HD:HD + 16, :] = jnp.where(live[:16] & (row16 == 0), 1.0, 0.0).astype(jnp.bfloat16)
        keys = turned[:HD].astype(jnp.float32)
        return jnp.maximum(longest, jnp.sum(keys * keys, axis=0, keepdims=True))

    longest_key = lax.fori_loop(0, key_steps, shape_keys, jnp.zeros((1, KB), jnp.float32))

    col = lax.broadcasted_iota(jnp.int32, (HD, QB), 1)
    low_rows = low_units * SLOT

    def shape_queries(t, longest):
        turned = jnp.transpose(q_flat[pl.ds(pl.multiple_of(t * QB, QB), QB), :])
        index = col + t * QB
        query = jnp.where(index < low_rows, turned[:HD], turned[HD:])
        query = jnp.where(index < query_rows, query, jnp.bfloat16(0.0))
        qt[t, 0:HD, :] = query
        qt[t, HD:, :] = jnp.zeros((HD, QB), jnp.bfloat16)
        query = query.astype(jnp.float32)
        return jnp.maximum(longest, jnp.sum(query * query, axis=0, keepdims=True))

    longest_query = lax.fori_loop(0, query_tiles, shape_queries, jnp.zeros((1, QB), jnp.float32))
    safe = jnp.max(longest_key) * jnp.max(longest_query) < SAFE * SAFE

    def block_scores(b, t):
        keys = kv_flat[pl.ds(pl.multiple_of(b * KB, KB), KB), :]
        return jnp.dot(keys, qt[t], preferred_element_type=jnp.float32)

    def clear(t):
        acc[t] = jnp.zeros((HD + 16, QB), jnp.float32)

    def after(item):
        t, b = item
        turn = b + 1 == key_steps
        return jnp.minimum(jnp.where(turn, t + 1, t), query_tiles), jnp.where(turn, 0, b + 1)

    def add(u, item):
        t, b = item
        acc[t] += jnp.dot(vt[b], held[u][...], preferred_element_type=jnp.float32)

    def weigh(u, item):
        t, b = item
        held[u][...] = jnp.exp2(block_scores(b, t)).astype(jnp.bfloat16)

    def plain(i, carry):
        before, now = carry
        then = now[-1]
        later = []
        for u in range(UN):
            add(u, before[u])
            weigh(u, now[u])
            then = after(then)
            later.append(then)
        return now, tuple(later)

    def plain_all():
        each(0, query_tiles, clear)
        first = [(jnp.int32(0), jnp.int32(0))]
        for _ in range(UN - 1):
            first.append(after(first[-1]))
        for u in range(UN):
            weigh(u, first[u])
        second = [after(first[-1])]
        for _ in range(UN - 1):
            second.append(after(second[-1]))
        steps = (query_tiles * key_steps + UN - 1) // UN
        last, _ = lax.fori_loop(1, steps, plain, (tuple(first), tuple(second)))
        for u in range(UN):
            add(u, last[u])

    def shifted_tile(t):
        def step(b, carry):
            best, total = carry
            scores = block_scores(b, t)
            best_next = jnp.maximum(best, jnp.max(scores, axis=0, keepdims=True))
            weights = jnp.exp2(scores - best_next).astype(jnp.bfloat16)
            total = total * jnp.exp2(best - best_next) + jnp.dot(
                vt[b], weights, preferred_element_type=jnp.float32)
            return best_next, total

        best, total = lax.fori_loop(
            0, key_steps, step,
            (jnp.full((1, QB), DEAD, jnp.float32), jnp.zeros((HD + 16, QB), jnp.float32)))
        acc[t] = total
        acc[t, HD + 8:HD + 9, :] = best

    @pl.when(safe)
    def _():
        plain_all()

    @pl.when(jnp.logical_not(safe))
    def _():
        each(0, query_tiles, shifted_tile)


def attention(counts, q_all, kv_all, times):
    sources, half_rows, _ = q_all.shape
    q_units, k_units = 4 * sources, 4 * sources
    q_rows = (q_units * SLOT + QB - 1) // QB * QB
    step = KB
    k_rows = (k_units * SLOT + step - 1) // step * step
    fill = -(-step // SLOT)
    return pl.pallas_call(
        functools.partial(attention_kernel, times=times),
        out_shape=VMEM((q_rows // QB + 1, HD + 16, QB), jnp.float32),
        in_specs=[spec(SMEM), spec(VMEM), spec(VMEM)],
        out_specs=spec(VMEM),
        scratch_shapes=[
            VMEM((k_units + max(fill, 8), SLOT, 128), jnp.bfloat16),
            VMEM((q_units + 8, SLOT, 128), jnp.bfloat16),
            VMEM((k_rows // KB, HD + 16, KB), jnp.bfloat16),
            VMEM((q_rows // QB + 1, 128, QB), jnp.bfloat16),
            *[VMEM((KB, QB), jnp.bfloat16) for _ in range(UN)],
        ],
        compiler_params=pltpu.CompilerParams(vmem_limit_bytes=32 << 20),
        name="attention",
    )(counts, near(q_all.reshape(8, 4, half_rows, 128)),
      near(kv_all.reshape(4, 2, 4, 2 * half_rows, 128)))


def return_kernel(cnt_ref, acc, back_ref, back_lse, of, packed, sizes, theirs, size_theirs, both, size_both,
                  t_send, t_recv, o_send, o_recv, l_send, l_recv):
    f, _, x, loc = place()
    hi, core = div(loc, 2), rem(loc, 2)
    half_rows = packed.shape[1]
    barrier = pltpu.get_barrier_semaphore()

    def greet(frame, there):
        pl.semaphore_signal(barrier, inc=1, device_id={"frame": frame, "space": x * 4 + there},
                            device_id_type=pl.DeviceIdType.MESH)

    greet(f, hi * 2 + 1 - core)
    for n in range(1, 16):
        greet(rem(f + n // 2, 8), rem(hi + n, 2) * 2 + core)

    starts, unit = [], jnp.int32(0)
    for j in range(4):
        for l in range(4):
            live = j < cnt_ref[x * 4 + l, 0, 0]
            starts.append(jnp.where(live, unit, 0))
            unit = unit + jnp.where(live, 8, 0)
        if j == 1:
            low_rows = unit * SLOT
    lane = lax.broadcasted_iota(jnp.int32, (SLOT, 128), 1)
    in_low = lane < HD
    of_flat = of.reshape(of.shape[0] * SLOT, 128)
    col = lax.broadcasted_iota(jnp.int32, (HD, QB), 1)

    def put(t):
        weight_sum = acc[t, HD:HD + 1, :]
        out = acc[t, 0:HD, :] / weight_sum
        lse = jnp.broadcast_to(acc[t, HD + 8:HD + 9, :] + jnp.log2(weight_sum), (HD, QB))
        low = col + t * QB < low_rows
        both = jnp.concatenate([jnp.where(low, out, lse), jnp.where(low, lse, out)], axis=0)
        of_flat[pl.ds(pl.multiple_of(t * QB, QB), QB), :] = jnp.transpose(both)

    each(0, acc.shape[0] - 1, put)

    def gather(frame, kept):
        for l in range(4):
            i = (l % 2) * 16 + (l // 2) * 8
            for j in range(2):
                first = of[starts[j * 4 + l] + frame]
                second = of[starts[j * 4 + 8 + l] + frame]
                packed[i + frame, j * SLOT:j * SLOT + SLOT, :] = jnp.where(in_low, first, second).astype(jnp.bfloat16)
                kept[j] = jnp.where(rem(lane, HD) == i + frame, jnp.where(in_low, second, first), kept[j])
        return kept

    kept = lax.fori_loop(0, 8, gather, [jnp.zeros((SLOT, 128), jnp.float32)] * 2)
    rows = jnp.transpose(jnp.concatenate([*kept, jnp.zeros((128 - 2 * SLOT, 128), jnp.float32)], axis=0))
    sizes[0] = rows[HD:HD + 32]
    sizes[1] = rows[0:32]

    keep = core * 16
    give = 16 - keep

    def twin(src, dst, n):
        return remote(src, dst, t_send.at[n], t_recv.at[n], f, x * 4 + hi * 2 + 1 - core)

    pl.semaphore_wait(barrier, 16)
    order = (1 - hi, hi)
    shares = [twin(sizes.at[:, pl.ds(give, 16), :], size_theirs, 0)]
    for n in range(2):
        shares.append(twin(packed.at[pl.ds(give + 8 * order[n], 8)], theirs.at[pl.ds(8 * n, 8)], 1 + n))
    for copy in shares:
        copy.start()
    shares[0].wait_recv()

    turned = []
    for n in range(2):
        one = jnp.concatenate([sizes[n, pl.ds(pl.multiple_of(keep + 8 * o, 8), 8), :] for o in order], axis=0)
        two = jnp.concatenate([size_theirs[n, pl.ds(pl.multiple_of(8 * o, 8), 8), :] for o in order], axis=0)
        top = jnp.maximum(one, two)
        one, two = jnp.exp2(one - top), jnp.exp2(two - top)
        total = one + two
        whole = top + jnp.log2(total)
        for r in range(16):
            size_both[r, n:n + 1, :] = whole[r:r + 1]
        turned.append(jnp.transpose(
            jnp.concatenate([one / total, two / total, jnp.zeros((96, 128), jnp.float32)], axis=0)))
    low = lax.broadcasted_iota(jnp.int32, (half_rows, 128), 1) < HD
    me = hi * 8 + f

    def send(n, frame):
        r = n * 8 + frame
        space = x * 4 + order[n] * 2 + core
        remote(both.at[r], back_ref.at[me], o_send.at[0], o_recv.at[0], frame, space).start()
        remote(size_both.at[r], back_lse.at[me], l_send.at[0], l_recv.at[0], frame, space).start()

    for n in range(2):
        shares[1 + n].wait_recv()
        for r in range(8 * n, 8 * n + 8):
            one = jnp.where(low, turned[0][0:half_rows, r:r + 1], turned[1][0:half_rows, r:r + 1])
            two = jnp.where(low, turned[0][0:half_rows, 16 + r:17 + r], turned[1][0:half_rows, 16 + r:17 + r])
            own = packed[keep + 8 * order[n] + r % 8].astype(jnp.float32)
            both[r] = (own * one + theirs[r].astype(jnp.float32) * two).astype(jnp.bfloat16)
        each(0, 8 - n, lambda d, n=n: send(n, rem(f + 1 + d, 8)))
    pltpu.make_async_copy(both.at[8 + f], back_ref.at[me], o_recv.at[0]).start()
    pltpu.make_async_copy(size_both.at[8 + f], back_lse.at[me], l_recv.at[0]).start()

    for copy in shares:
        copy.wait_send()
    for sem, ref in ((o_send, back_ref.at[pl.ds(0, 15)]), (l_send, back_lse.at[pl.ds(0, 15)]),
                     (o_recv, back_ref), (l_recv, back_lse)):
        pltpu.make_async_copy(ref, ref, sem.at[0]).wait()


def give_results(counts, partial):
    dma = pltpu.SemaphoreType.DMA
    bf16, f32 = jnp.bfloat16, jnp.float32
    half_rows = 2 * SLOT
    return pl.pallas_call(
        return_kernel,
        out_shape=(VMEM((16, half_rows, 128), bf16), VMEM((16, 2, 128), f32)),
        in_specs=[spec(SMEM), spec(VMEM)],
        out_specs=(spec(ANY), spec(ANY)),
        scratch_shapes=[
            VMEM(((partial.shape[0] - 1) * QB // SLOT, SLOT, 128), f32),
            VMEM((32, half_rows, 128), bf16), VMEM((2, 32, 128), f32),
            VMEM((16, half_rows, 128), bf16), VMEM((2, 16, 128), f32),
            VMEM((16, half_rows, 128), bf16), VMEM((16, 2, 128), f32),
            dma((3,)), dma((3,)), dma((1,)), dma((1,)), dma((1,)), dma((1,))],
        compiler_params=pltpu.CompilerParams(
            collective_id=1, has_side_effects=True, vmem_limit_bytes=16 << 20),
        name="give_results",
    )(counts, near(partial))


def finish_kernel(tok_ref, cnt_ref, back_ref, lse_ref, w_ref, o_ref, att, ys, done, o_sem):
    times, slots, width = tok_ref.shape
    half = slots * SLOT // 2
    rows = slots * SLOT

    def shares(n):
        sizes = [lse_ref[p * 8:p * 8 + 8, n, :] for p in range(2)]
        top = jnp.maximum(sizes[0], sizes[1])
        powers = [jnp.exp2(v - top) for v in sizes]
        total = powers[0] + powers[1]
        return jnp.transpose(
            jnp.concatenate([v / total for v in powers] + [jnp.zeros((112, 128), jnp.float32)], axis=0))

    first, second = shares(0), shares(1)
    low = lax.broadcasted_iota(jnp.int32, (half, 128), 1) < HD

    def merged(h):
        out = jnp.zeros((half, 128), jnp.float32)
        for p in range(2):
            n = p * 8 + h
            share = jnp.where(low, first[0:half, n:n + 1], second[0:half, n:n + 1])
            out = out + back_ref[n].astype(jnp.float32) * share
        return out

    for j in range(HEADS // 2):
        a, b = merged(2 * j), merged(2 * j + 1)
        cols = slice(128 * j, 128 * j + 128)
        att[0:half, cols] = jnp.where(low, a, pltpu.roll(b, HD, 1)).astype(jnp.bfloat16)
        att[half:rows, cols] = jnp.where(low, pltpu.roll(a, HD, 1), b).astype(jnp.bfloat16)
    for c in range(width // 256):
        cols = slice(256 * c, 256 * c + 256)
        mixed = jnp.dot(att[...], w_ref[:, cols], preferred_element_type=jnp.float32)
        for i in range(slots):
            for e in range(2):
                ys[2 * c + e, pl.ds(i, SLOT, stride=slots), :] = (
                    mixed[i * SLOT:i * SLOT + SLOT, 128 * e:128 * e + 128])
    live = lax.broadcasted_iota(jnp.int32, (slots, width), 0) < cnt_ref[0]
    ends, copies = [times // 4, times // 2, times * 3 // 4, times], []
    for t in range(times):
        mixed = jnp.concatenate([ys[c, t * slots:t * slots + slots, :] for c in range(width // 128)], axis=1)
        value = tok_ref[t].astype(jnp.float32) + mixed
        done[t] = jnp.where(live, value, 0.0).astype(jnp.bfloat16)
        if t + 1 in ends:
            n = ends.index(t + 1)
            rows = pl.ds(ends[n - 1] if n else 0, ends[n] - (ends[n - 1] if n else 0))
            copies.append(pltpu.make_async_copy(done.at[rows], o_ref.at[rows], o_sem.at[n]))
            copies[n].start()
    for copy in copies:
        copy.wait()


def finish(tokens, count, back, sizes, w_out):
    times, slots, width = tokens.shape
    rows = slots * SLOT
    return pl.pallas_call(
        finish_kernel,
        out_shape=jax.ShapeDtypeStruct(tokens.shape, tokens.dtype),
        in_specs=[spec(VMEM), spec(SMEM), spec(VMEM), spec(VMEM), spec(VMEM)],
        out_specs=spec(ANY),
        scratch_shapes=[VMEM((rows, w_out.shape[0]), jnp.bfloat16), VMEM((width // 128, rows, 128), jnp.float32),
                        VMEM(tokens.shape, tokens.dtype), pltpu.SemaphoreType.DMA((4,))],
        compiler_params=pltpu.CompilerParams(vmem_limit_bytes=16 << 20),
        name="finish",
    )(near(tokens), count, near(back), near(sizes), near(w_out))


def on_device(tokens, tube_count, ln_gain, ln_bias, w_qkv, w_out):
    tokens = jnp.transpose(tokens, (1, 0, 2))
    q_all, kv_all, counts, tokens, w_out = project(
        tokens, tube_count, ln_gain.reshape(1, -1), ln_bias.reshape(1, -1), w_qkv, w_out)
    partial = attention(counts, q_all, kv_all, tokens.shape[0])
    mixed = finish(tokens, tube_count, *give_results(counts, partial), w_out)
    return jnp.transpose(mixed, (1, 0, 2))


def solution(mesh):
    in_specs = (P("space", "frame", None), P("space"), P(), P(), P(), P())
    return jax.shard_map(
        on_device, mesh=mesh, in_specs=in_specs, out_specs=P("space", "frame", None), check_vma=False)
```

```python
import functools

import jax
import jax.numpy as jnp
from jax import lax
from jax.experimental import pallas as pl
from jax.experimental.pallas import tpu as pltpu
from jax.sharding import PartitionSpec as P

HEADS = 8
HD = 64
SLOT = 40
KB = 256
UN = 8
QB = 512
DEAD = -1e30
Q_AFTER = 2
SAFE = 80.0
EPSILON = 1e-06
SCALE = 1.4426950408889634 / 8.0
ANY = pl.ANY
VMEM = pltpu.VMEM
SMEM = pltpu.SMEM


def spec(space):
    return pl.BlockSpec(memory_space=space)


def near(array):
    return pltpu.with_memory_space_constraint(array, VMEM)


def place():
    f, s = lax.axis_index("frame"), lax.axis_index("space")
    return f, s, div(s, 4), rem(s, 4)


def remote(src, dst, send, recv, frame, space):
    return pltpu.make_async_remote_copy(
        src_ref=src, dst_ref=dst, send_sem=send, recv_sem=recv,
        device_id={"frame": frame, "space": space}, device_id_type=pl.DeviceIdType.MESH)


def rem(a, n):
    return lax.rem(a, jnp.int32(n))


def div(a, n):
    return lax.div(a, jnp.int32(n))


def each(lo, hi, body):
    def step(i, c):
        body(i)
        return c
    lax.fori_loop(lo, hi, step, 0)


def project_kernel(tok_in, cnt_ref, gain_ref, bias_ref, w_ref, w_last, q_out, kv_out, cnt_out, tok_ref, w_next,
                   w_v, xs, nb, kvs, qs, cnts,
                   w_sem, kv_send, kv_recv, q_send, q_recv, c_send, c_recv, x_send, r_send, pass_recv, rest_recv):
    f, s, x, loc = place()
    times, slots, width = tok_ref.shape
    inner = HEADS * HD

    tok_copy = pltpu.make_async_copy(tok_in, tok_ref, w_sem.at[3])
    tok_copy.start()
    last_copy = pltpu.make_async_copy(w_last, w_next, w_sem.at[4])
    copies = []
    for n, at in enumerate((inner, 2 * inner, 0)):
        cols = pl.ds(at, inner)
        copies.append(pltpu.make_async_copy(w_ref.at[:, cols], w_v.at[:, cols], w_sem.at[n]))
    copies[0].start()
    copies[1].start()

    barrier = pltpu.get_barrier_semaphore()

    def greet(frame, space):
        pl.semaphore_signal(barrier, inc=1, device_id={"frame": frame, "space": space},
                            device_id_type=pl.DeviceIdType.MESH)

    each(1, 32, lambda n: greet(rem(f + div(n, 4), 8), x * 4 + rem(loc + n, 4)))
    each(4, 16, lambda n: greet(f, rem(x * 4 + n, 16)))

    cnts[...] = jnp.full(cnts.shape, cnt_ref[0], jnp.int32)

    tok_copy.wait()
    for t in range(SLOT):
        values = tok_ref[t % times].astype(jnp.float32)
        for c in range(width // 128):
            xs[c, t * slots:t * slots + slots, :] = values[:, 128 * c:128 * c + 128]
    for i in range(slots):
        values = jnp.concatenate(
            [xs[c, pl.ds(i, SLOT, stride=slots), :] for c in range(width // 128)], axis=1)
        center = values - jnp.mean(values, axis=-1, keepdims=True)
        spread = jnp.mean(center * center, axis=-1, keepdims=True)
        normed = center * lax.rsqrt(spread + EPSILON) * gain_ref[...] + bias_ref[...]
        nb[i * SLOT:i * SLOT + SLOT, :] = normed.astype(jnp.bfloat16)

    rows_all = slots * SLOT
    half = rows_all // 2
    low = lax.broadcasted_iota(jnp.int32, (rows_all, 128), 1) < HD
    low_half = lax.broadcasted_iota(jnp.int32, (half, 128), 1) < HD

    copies[0].wait()
    copies[1].wait()
    copies[2].start()
    for g in range(2):
        k4 = jnp.dot(nb[...], w_v[:, inner + 256 * g:inner + 256 * g + 256], preferred_element_type=jnp.float32)
        v4 = jnp.dot(nb[...], w_v[:, 2 * inner + 256 * g:2 * inner + 256 * g + 256],
                     preferred_element_type=jnp.float32)
        for j in range(2):
            k2, v2 = k4[:, 128 * j:128 * j + 128], v4[:, 128 * j:128 * j + 128]
            h = 4 * g + 2 * j
            kvs[h] = jnp.where(low, k2, pltpu.roll(v2, HD, 1)).astype(jnp.bfloat16)
            kvs[h + 1] = jnp.where(low, pltpu.roll(k2, HD, 1), v2).astype(jnp.bfloat16)

    part = div(f, 2)
    mine = rem(f, 2) * 4 + loc
    source = x * 8 + mine
    pl.semaphore_wait(barrier, 43)

    def kv_copy(d):
        h = rem(f + d + 2 * loc, 8)
        stays = (h == f) & (part == loc)
        return stays, h, remote(
            kvs.at[h], kv_out.at[source], kv_send.at[0], kv_recv.at[mine], h, x * 4 + part)

    def kv_start(d):
        stays, h, copy = kv_copy(d)

        @pl.when(stays)
        def _():
            pltpu.make_async_copy(kvs.at[h], kv_out.at[source], kv_recv.at[mine]).start()

        @pl.when(jnp.logical_not(stays))
        def _():
            copy.start()

    each(0, 8, kv_start)

    def count_copy(e):
        return remote(cnts, cnt_out.at[s], c_send.at[0], c_recv.at[0], f, rem(s + e, 16))

    each(1, 16, lambda e: count_copy(e).start())
    pltpu.make_async_copy(cnts, cnt_out.at[s], c_recv.at[0]).start()

    copies[2].wait()
    last_copy.start()
    for g in range(2):
        q4 = jnp.dot(nb[...], w_v[:, 256 * g:256 * g + 256], preferred_element_type=jnp.float32) * SCALE
        for j in range(2):
            q2 = q4[:, 128 * j:128 * j + 128]
            h = 4 * g + 2 * j
            qs[h] = jnp.where(low_half, q2[:half], pltpu.roll(q2[half:], HD, 1)).astype(jnp.bfloat16)
            qs[h + 1] = jnp.where(low_half, pltpu.roll(q2[:half], HD, 1), q2[half:]).astype(jnp.bfloat16)

    me = f * 4 + loc

    def q_copy(n):
        h = rem(f + div(n, 4), 8)
        return remote(qs.at[h], q_out.at[me], q_send.at[0], q_recv.at[0], h, x * 4 + rem(loc + n, 4))

    def ring(piece, send, recv, step):
        return remote(kv_out.at[piece], kv_out.at[piece], send.at[0], recv, f, rem(x + step, 4) * 4 + loc)

    def nth(t):
        u = rem(f - 2 * loc - t + 16, 8)
        return rem(u, 2) * 4 + div(u, 2)

    right, left = rem(x + 1, 4) * 8, rem(x + 3, 4) * 8

    def landed(sem, ref):
        pltpu.make_async_copy(ref, ref, sem).wait()

    def to_right(t, piece):
        even = rem(t, 2) == 0

        @pl.when(even)
        def _():
            ring(piece, x_send, pass_recv.at[t], 1).start()

        @pl.when(jnp.logical_not(even))
        def _():
            ring(piece, x_send, rest_recv.at[0], 1).start()

    def to_left(t, piece):
        odd = rem(t, 2) == 1

        @pl.when(odd)
        def _():
            ring(piece, x_send, pass_recv.at[t], 3).start()

        @pl.when(jnp.logical_not(odd))
        def _():
            ring(piece, x_send, rest_recv.at[0], 3).start()

    def arrived(t):
        i = nth(t)
        piece = x * 8 + i
        landed(kv_recv.at[i], kv_out.at[piece])
        to_right(t, piece)
        to_left(t, piece)

    each(0, Q_AFTER, arrived)
    each(1, 32, lambda n: q_copy(n).start())
    pltpu.make_async_copy(qs.at[f], q_out.at[me], q_recv.at[0]).start()
    each(Q_AFTER, 8, arrived)

    def relay(t):
        piece = left + nth(2 * t)
        landed(pass_recv.at[2 * t], kv_out.at[piece])
        ring(piece, r_send, rest_recv.at[0], 1).start()
        piece = right + nth(2 * t + 1)
        landed(pass_recv.at[2 * t + 1], kv_out.at[piece])
        ring(piece, r_send, rest_recv.at[0], 3).start()

    each(0, 4, relay)

    last_copy.wait()
    landed(kv_send.at[0], kv_out.at[pl.ds(0, 7)])

    @pl.when(part != loc)
    def _():
        landed(kv_send.at[0], kv_out.at[0])

    landed(c_send.at[0], cnt_out.at[pl.ds(0, 15)])
    landed(q_send.at[0], q_out.at[pl.ds(0, 31)])
    landed(x_send.at[0], kv_out.at[pl.ds(0, 16)])
    landed(r_send.at[0], kv_out.at[pl.ds(0, 8)])
    landed(c_recv.at[0], cnt_out)
    landed(q_recv.at[0], q_out)
    landed(rest_recv.at[0], kv_out.at[pl.ds(0, 16)])


def project(tokens, count, gain, bias, w_qkv, w_out):
    times, slots, width = tokens.shape
    rows = slots * SLOT
    bf16, i32 = jnp.bfloat16, jnp.int32
    dma = pltpu.SemaphoreType.DMA
    return pl.pallas_call(
        project_kernel,
        out_shape=(VMEM((32, rows // 2, 128), bf16),
                   VMEM((32, rows, 128), bf16),
                   VMEM((16, 1, 128), i32),
                   VMEM(tokens.shape, bf16), VMEM(w_out.shape, bf16)),
        in_specs=[spec(pltpu.HBM), spec(SMEM), spec(VMEM), spec(VMEM), spec(pltpu.HBM), spec(pltpu.HBM)],
        out_specs=(spec(ANY), spec(ANY), spec(ANY), spec(VMEM), spec(ANY)),
        scratch_shapes=[
            VMEM(w_qkv.shape, bf16), VMEM((width // 128, rows, 128), jnp.float32), VMEM((rows, width), bf16),
            VMEM((HEADS, rows, 128), bf16), VMEM((HEADS, rows // 2, 128), bf16), VMEM((1, 128), i32),
            dma((5,)), dma((1,)), dma((8,)), dma((1,)), dma((1,)), dma((1,)), dma((1,)),
            dma((1,)), dma((1,)), dma((8,)), dma((1,)),
        ],
        compiler_params=pltpu.CompilerParams(collective_id=0, has_side_effects=True),
        name="project",
    )(tokens, count, gain, bias, w_qkv, w_out)


def attention_kernel(cnt_ref, q_ref, kv_ref, acc, kvc, qc, vt, qt, *held, times):
    base = (lax.axis_index("space") // 4) * 4
    kv_flat = kvc.reshape(kvc.shape[0] * SLOT, 128)
    q_flat = qc.reshape(qc.shape[0] * SLOT, 128)
    step_keys = KB

    def take_keys(n, unit):
        for j in range(4):
            for sub in range(2):
                kvc[unit + 2 * j + sub] = kv_ref[n // 4, sub, n % 4, j * SLOT:j * SLOT + SLOT, :]
        return unit + 2 * cnt_ref[n, 0, 0]

    unit = jnp.int32(0)
    for n in range(16):
        unit = take_keys(n, unit)
    key_units = unit
    for n in range(-(-step_keys // SLOT)):
        kvc[key_units + n] = kv_ref[0, 0, 0, 0:SLOT, :]

    unit = jnp.int32(0)
    for j in range(4):
        if j == 2:
            low_units = unit
        for l in range(4):
            live = j < cnt_ref[base + l, 0, 0]
            for f in range(8):
                qc[unit + f] = q_ref[f, l, (j % 2) * SLOT:(j % 2) * SLOT + SLOT, :]
            unit = unit + jnp.where(live, 8, 0)
    query_rows = unit * SLOT
    query_tiles = (query_rows + QB - 1) // QB
    key_rows = key_units * SLOT
    key_steps = (key_rows + step_keys - 1) // step_keys

    key_at = lax.broadcasted_iota(jnp.int32, (HD, KB), 1)
    row16 = lax.broadcasted_iota(jnp.int32, (16, KB), 0)

    def shape_keys(b, longest):
        turned = jnp.transpose(kv_flat[pl.ds(pl.multiple_of(b * KB, KB), KB), :])
        index = key_at + b * KB
        live = (index % SLOT < times) & (index < key_rows)
        vt[b, 0:HD, :] = jnp.where(live, turned[HD:], jnp.bfloat16(0.0))
        vt[b, HD:HD + 16, :] = jnp.where(live[:16] & (row16 == 0), 1.0, 0.0).astype(jnp.bfloat16)
        keys = turned[:HD].astype(jnp.float32)
        return jnp.maximum(longest, jnp.sum(keys * keys, axis=0, keepdims=True))

    longest_key = lax.fori_loop(0, key_steps, shape_keys, jnp.zeros((1, KB), jnp.float32))

    col = lax.broadcasted_iota(jnp.int32, (HD, QB), 1)
    low_rows = low_units * SLOT

    def shape_queries(t, longest):
        turned = jnp.transpose(q_flat[pl.ds(pl.multiple_of(t * QB, QB), QB), :])
        index = col + t * QB
        query = jnp.where(index < low_rows, turned[:HD], turned[HD:])
        query = jnp.where(index < query_rows, query, jnp.bfloat16(0.0))
        qt[t, 0:HD, :] = query
        qt[t, HD:, :] = jnp.zeros((HD, QB), jnp.bfloat16)
        query = query.astype(jnp.float32)
        return jnp.maximum(longest, jnp.sum(query * query, axis=0, keepdims=True))

    longest_query = lax.fori_loop(0, query_tiles, shape_queries, jnp.zeros((1, QB), jnp.float32))
    safe = jnp.max(longest_key) * jnp.max(longest_query) < SAFE * SAFE

    def block_scores(b, t):
        keys = kv_flat[pl.ds(pl.multiple_of(b * KB, KB), KB), :]
        return jnp.dot(keys, qt[t], preferred_element_type=jnp.float32)

    def clear(t):
        acc[t] = jnp.zeros((HD + 16, QB), jnp.float32)

    def after(item):
        t, b = item
        turn = b + 1 == key_steps
        return jnp.minimum(jnp.where(turn, t + 1, t), query_tiles), jnp.where(turn, 0, b + 1)

    def add(u, item):
        t, b = item
        acc[t] += jnp.dot(vt[b], held[u][...], preferred_element_type=jnp.float32)

    def weigh(u, item):
        t, b = item
        held[u][...] = jnp.exp2(block_scores(b, t)).astype(jnp.bfloat16)

    def plain(i, carry):
        before, now = carry
        then = now[-1]
        later = []
        for u in range(UN):
            add(u, before[u])
            weigh(u, now[u])
            then = after(then)
            later.append(then)
        return now, tuple(later)

    def plain_all():
        each(0, query_tiles, clear)
        first = [(jnp.int32(0), jnp.int32(0))]
        for _ in range(UN - 1):
            first.append(after(first[-1]))
        for u in range(UN):
            weigh(u, first[u])
        second = [after(first[-1])]
        for _ in range(UN - 1):
            second.append(after(second[-1]))
        steps = (query_tiles * key_steps + UN - 1) // UN
        last, _ = lax.fori_loop(1, steps, plain, (tuple(first), tuple(second)))
        for u in range(UN):
            add(u, last[u])

    def shifted_tile(t):
        def step(b, carry):
            best, total = carry
            scores = block_scores(b, t)
            best_next = jnp.maximum(best, jnp.max(scores, axis=0, keepdims=True))
            weights = jnp.exp2(scores - best_next).astype(jnp.bfloat16)
            total = total * jnp.exp2(best - best_next) + jnp.dot(
                vt[b], weights, preferred_element_type=jnp.float32)
            return best_next, total

        best, total = lax.fori_loop(
            0, key_steps, step,
            (jnp.full((1, QB), DEAD, jnp.float32), jnp.zeros((HD + 16, QB), jnp.float32)))
        acc[t] = total
        acc[t, HD + 8:HD + 9, :] = best

    @pl.when(safe)
    def _():
        plain_all()

    @pl.when(jnp.logical_not(safe))
    def _():
        each(0, query_tiles, shifted_tile)


def attention(counts, q_all, kv_all, times):
    sources, half_rows, _ = q_all.shape
    q_units, k_units = 4 * sources, 4 * sources
    q_rows = (q_units * SLOT + QB - 1) // QB * QB
    step = KB
    k_rows = (k_units * SLOT + step - 1) // step * step
    fill = -(-step // SLOT)
    return pl.pallas_call(
        functools.partial(attention_kernel, times=times),
        out_shape=VMEM((q_rows // QB + 1, HD + 16, QB), jnp.float32),
        in_specs=[spec(SMEM), spec(VMEM), spec(VMEM)],
        out_specs=spec(VMEM),
        scratch_shapes=[
            VMEM((k_units + max(fill, 8), SLOT, 128), jnp.bfloat16),
            VMEM((q_units + 8, SLOT, 128), jnp.bfloat16),
            VMEM((k_rows // KB, HD + 16, KB), jnp.bfloat16),
            VMEM((q_rows // QB + 1, 128, QB), jnp.bfloat16),
            *[VMEM((KB, QB), jnp.bfloat16) for _ in range(UN)],
        ],
        compiler_params=pltpu.CompilerParams(vmem_limit_bytes=32 << 20),
        name="attention",
    )(counts, near(q_all.reshape(8, 4, half_rows, 128)),
      near(kv_all.reshape(4, 2, 4, 2 * half_rows, 128)))


def return_kernel(cnt_ref, acc, back_ref, back_lse, of, packed, sizes, theirs, size_theirs, both, size_both,
                  t_send, t_recv, o_send, o_recv, l_send, l_recv):
    f, _, x, loc = place()
    hi, core = div(loc, 2), rem(loc, 2)
    half_rows = packed.shape[1]
    barrier = pltpu.get_barrier_semaphore()

    def greet(frame, there):
        pl.semaphore_signal(barrier, inc=1, device_id={"frame": frame, "space": x * 4 + there},
                            device_id_type=pl.DeviceIdType.MESH)

    greet(f, hi * 2 + 1 - core)
    for n in range(1, 16):
        greet(rem(f + n // 2, 8), rem(hi + n, 2) * 2 + core)

    starts, unit = [], jnp.int32(0)
    for j in range(4):
        for l in range(4):
            live = j < cnt_ref[x * 4 + l, 0, 0]
            starts.append(jnp.where(live, unit, 0))
            unit = unit + jnp.where(live, 8, 0)
        if j == 1:
            low_rows = unit * SLOT
    lane = lax.broadcasted_iota(jnp.int32, (SLOT, 128), 1)
    in_low = lane < HD
    of_flat = of.reshape(of.shape[0] * SLOT, 128)
    col = lax.broadcasted_iota(jnp.int32, (HD, QB), 1)

    def put(t):
        weight_sum = acc[t, HD:HD + 1, :]
        out = acc[t, 0:HD, :] / weight_sum
        lse = jnp.broadcast_to(acc[t, HD + 8:HD + 9, :] + jnp.log2(weight_sum), (HD, QB))
        low = col + t * QB < low_rows
        both = jnp.concatenate([jnp.where(low, out, lse), jnp.where(low, lse, out)], axis=0)
        of_flat[pl.ds(pl.multiple_of(t * QB, QB), QB), :] = jnp.transpose(both)

    each(0, acc.shape[0] - 1, put)

    def gather(frame, kept):
        for l in range(4):
            i = (l % 2) * 16 + (l // 2) * 8
            for j in range(2):
                first = of[starts[j * 4 + l] + frame]
                second = of[starts[j * 4 + 8 + l] + frame]
                packed[i + frame, j * SLOT:j * SLOT + SLOT, :] = jnp.where(in_low, first, second).astype(jnp.bfloat16)
                kept[j] = jnp.where(rem(lane, HD) == i + frame, jnp.where(in_low, second, first), kept[j])
        return kept

    kept = lax.fori_loop(0, 8, gather, [jnp.zeros((SLOT, 128), jnp.float32)] * 2)
    rows = jnp.transpose(jnp.concatenate([*kept, jnp.zeros((128 - 2 * SLOT, 128), jnp.float32)], axis=0))
    sizes[0] = rows[HD:HD + 32]
    sizes[1] = rows[0:32]

    keep = core * 16
    give = 16 - keep

    def twin(src, dst, n):
        return remote(src, dst, t_send.at[n], t_recv.at[n], f, x * 4 + hi * 2 + 1 - core)

    pl.semaphore_wait(barrier, 16)
    order = (1 - hi, hi)
    shares = [twin(sizes.at[:, pl.ds(give, 16), :], size_theirs, 0)]
    for n in range(2):
        shares.append(twin(packed.at[pl.ds(give + 8 * order[n], 8)], theirs.at[pl.ds(8 * n, 8)], 1 + n))
    for copy in shares:
        copy.start()
    shares[0].wait_recv()

    turned = []
    for n in range(2):
        one = jnp.concatenate([sizes[n, pl.ds(pl.multiple_of(keep + 8 * o, 8), 8), :] for o in order], axis=0)
        two = jnp.concatenate([size_theirs[n, pl.ds(pl.multiple_of(8 * o, 8), 8), :] for o in order], axis=0)
        top = jnp.maximum(one, two)
        one, two = jnp.exp2(one - top), jnp.exp2(two - top)
        total = one + two
        whole = top + jnp.log2(total)
        for r in range(16):
            size_both[r, n:n + 1, :] = whole[r:r + 1]
        turned.append(jnp.transpose(
            jnp.concatenate([one / total, two / total, jnp.zeros((96, 128), jnp.float32)], axis=0)))
    low = lax.broadcasted_iota(jnp.int32, (half_rows, 128), 1) < HD
    me = hi * 8 + f

    def send(n, frame):
        r = n * 8 + frame
        space = x * 4 + order[n] * 2 + core
        remote(both.at[r], back_ref.at[me], o_send.at[0], o_recv.at[0], frame, space).start()
        remote(size_both.at[r], back_lse.at[me], l_send.at[0], l_recv.at[0], frame, space).start()

    for n in range(2):
        shares[1 + n].wait_recv()
        for r in range(8 * n, 8 * n + 8):
            one = jnp.where(low, turned[0][0:half_rows, r:r + 1], turned[1][0:half_rows, r:r + 1])
            two = jnp.where(low, turned[0][0:half_rows, 16 + r:17 + r], turned[1][0:half_rows, 16 + r:17 + r])
            own = packed[keep + 8 * order[n] + r % 8].astype(jnp.float32)
            both[r] = (own * one + theirs[r].astype(jnp.float32) * two).astype(jnp.bfloat16)
        each(0, 8 - n, lambda d, n=n: send(n, rem(f + 1 + d, 8)))
    pltpu.make_async_copy(both.at[8 + f], back_ref.at[me], o_recv.at[0]).start()
    pltpu.make_async_copy(size_both.at[8 + f], back_lse.at[me], l_recv.at[0]).start()

    for copy in shares:
        copy.wait_send()
    for sem, ref in ((o_send, back_ref.at[pl.ds(0, 15)]), (l_send, back_lse.at[pl.ds(0, 15)]),
                     (o_recv, back_ref), (l_recv, back_lse)):
        pltpu.make_async_copy(ref, ref, sem.at[0]).wait()


def give_results(counts, partial):
    dma = pltpu.SemaphoreType.DMA
    bf16, f32 = jnp.bfloat16, jnp.float32
    half_rows = 2 * SLOT
    return pl.pallas_call(
        return_kernel,
        out_shape=(VMEM((16, half_rows, 128), bf16), VMEM((16, 2, 128), f32)),
        in_specs=[spec(SMEM), spec(VMEM)],
        out_specs=(spec(ANY), spec(ANY)),
        scratch_shapes=[
            VMEM(((partial.shape[0] - 1) * QB // SLOT, SLOT, 128), f32),
            VMEM((32, half_rows, 128), bf16), VMEM((2, 32, 128), f32),
            VMEM((16, half_rows, 128), bf16), VMEM((2, 16, 128), f32),
            VMEM((16, half_rows, 128), bf16), VMEM((16, 2, 128), f32),
            dma((3,)), dma((3,)), dma((1,)), dma((1,)), dma((1,)), dma((1,))],
        compiler_params=pltpu.CompilerParams(
            collective_id=1, has_side_effects=True, vmem_limit_bytes=16 << 20),
        name="give_results",
    )(counts, near(partial))


def finish_kernel(tok_ref, cnt_ref, back_ref, lse_ref, w_ref, o_ref, att, ys, done, o_sem):
    times, slots, width = tok_ref.shape
    half = slots * SLOT // 2
    rows = slots * SLOT

    def shares(n):
        sizes = [lse_ref[p * 8:p * 8 + 8, n, :] for p in range(2)]
        top = jnp.maximum(sizes[0], sizes[1])
        powers = [jnp.exp2(v - top) for v in sizes]
        total = powers[0] + powers[1]
        return jnp.transpose(
            jnp.concatenate([v / total for v in powers] + [jnp.zeros((112, 128), jnp.float32)], axis=0))

    first, second = shares(0), shares(1)
    low = lax.broadcasted_iota(jnp.int32, (half, 128), 1) < HD

    def merged(h):
        out = jnp.zeros((half, 128), jnp.float32)
        for p in range(2):
            n = p * 8 + h
            share = jnp.where(low, first[0:half, n:n + 1], second[0:half, n:n + 1])
            out = out + back_ref[n].astype(jnp.float32) * share
        return out

    for j in range(HEADS // 2):
        a, b = merged(2 * j), merged(2 * j + 1)
        cols = slice(128 * j, 128 * j + 128)
        att[0:half, cols] = jnp.where(low, a, pltpu.roll(b, HD, 1)).astype(jnp.bfloat16)
        att[half:rows, cols] = jnp.where(low, pltpu.roll(a, HD, 1), b).astype(jnp.bfloat16)
    for c in range(width // 256):
        cols = slice(256 * c, 256 * c + 256)
        mixed = jnp.dot(att[...], w_ref[:, cols], preferred_element_type=jnp.float32)
        for i in range(slots):
            for e in range(2):
                ys[2 * c + e, pl.ds(i, SLOT, stride=slots), :] = (
                    mixed[i * SLOT:i * SLOT + SLOT, 128 * e:128 * e + 128])
    live = lax.broadcasted_iota(jnp.int32, (slots, width), 0) < cnt_ref[0]
    ends, copies = [times // 4, times // 2, times * 3 // 4, times], []
    for t in range(times):
        mixed = jnp.concatenate([ys[c, t * slots:t * slots + slots, :] for c in range(width // 128)], axis=1)
        value = tok_ref[t].astype(jnp.float32) + mixed
        done[t] = jnp.where(live, value, 0.0).astype(jnp.bfloat16)
        if t + 1 in ends:
            n = ends.index(t + 1)
            rows = pl.ds(ends[n - 1] if n else 0, ends[n] - (ends[n - 1] if n else 0))
            copies.append(pltpu.make_async_copy(done.at[rows], o_ref.at[rows], o_sem.at[n]))
            copies[n].start()
    for copy in copies:
        copy.wait()


def finish(tokens, count, back, sizes, w_out):
    times, slots, width = tokens.shape
    rows = slots * SLOT
    return pl.pallas_call(
        finish_kernel,
        out_shape=jax.ShapeDtypeStruct(tokens.shape, tokens.dtype),
        in_specs=[spec(VMEM), spec(SMEM), spec(VMEM), spec(VMEM), spec(VMEM)],
        out_specs=spec(ANY),
        scratch_shapes=[VMEM((rows, w_out.shape[0]), jnp.bfloat16), VMEM((width // 128, rows, 128), jnp.float32),
                        VMEM(tokens.shape, tokens.dtype), pltpu.SemaphoreType.DMA((4,))],
        compiler_params=pltpu.CompilerParams(vmem_limit_bytes=16 << 20),
        name="finish",
    )(near(tokens), count, near(back), near(sizes), near(w_out))


def on_device(tokens, tube_count, ln_gain, ln_bias, w_qkv, w_out):
    tokens = jnp.transpose(tokens, (1, 0, 2))
    q_all, kv_all, counts, tokens, w_out = project(
        tokens, tube_count, ln_gain.reshape(1, -1), ln_bias.reshape(1, -1), w_qkv, w_out)
    partial = attention(counts, q_all, kv_all, tokens.shape[0])
    mixed = finish(tokens, tube_count, *give_results(counts, partial), w_out)
    return jnp.transpose(mixed, (1, 0, 2))


def solution(mesh):
    in_specs = (P("space", "frame", None), P("space"), P(), P(), P(), P())
    return jax.shard_map(
        on_device, mesh=mesh, in_specs=in_specs, out_specs=P("space", "frame", None), check_vma=False)
```

```python
import functools

import jax
import jax.numpy as jnp
from jax import lax
from jax.experimental import pallas as pl
from jax.experimental.pallas import tpu as pltpu
from jax.sharding import PartitionSpec as P

HEADS = 8
HD = 64
SLOT = 40
KB = 256
UN = 8
QB = 512
DEAD = -1e30
Q_AFTER = 2
SAFE = 100.0
EPSILON = 1e-06
SCALE = 1.4426950408889634 / 8.0
ANY = pl.ANY
VMEM = pltpu.VMEM
SMEM = pltpu.SMEM


def spec(space):
    return pl.BlockSpec(memory_space=space)


def near(array):
    return pltpu.with_memory_space_constraint(array, VMEM)


def place():
    f, s = lax.axis_index("frame"), lax.axis_index("space")
    return f, s, div(s, 4), rem(s, 4)


def remote(src, dst, send, recv, frame, space):
    return pltpu.make_async_remote_copy(
        src_ref=src, dst_ref=dst, send_sem=send, recv_sem=recv,
        device_id={"frame": frame, "space": space}, device_id_type=pl.DeviceIdType.MESH)


def rem(a, n):
    return lax.rem(a, jnp.int32(n))


def div(a, n):
    return lax.div(a, jnp.int32(n))


def each(lo, hi, body):
    def step(i, c):
        body(i)
        return c
    lax.fori_loop(lo, hi, step, 0)


def project_kernel(tok_in, cnt_ref, gain_ref, bias_ref, w_ref, w_last, q_out, kv_out, cnt_out, tok_ref, w_next,
                   w_v, xs, nb, kvs, qs, cnts,
                   w_sem, kv_send, kv_recv, q_send, q_recv, c_send, c_recv, x_send, r_send, pass_recv, rest_recv):
    f, s, x, loc = place()
    times, slots, width = tok_ref.shape
    inner = HEADS * HD

    tok_copy = pltpu.make_async_copy(tok_in, tok_ref, w_sem.at[3])
    tok_copy.start()
    last_copy = pltpu.make_async_copy(w_last, w_next, w_sem.at[4])
    copies = []
    for n, at in enumerate((inner, 2 * inner, 0)):
        cols = pl.ds(at, inner)
        copies.append(pltpu.make_async_copy(w_ref.at[:, cols], w_v.at[:, cols], w_sem.at[n]))
    copies[0].start()
    copies[1].start()

    barrier = pltpu.get_barrier_semaphore()

    def greet(frame, space):
        pl.semaphore_signal(barrier, inc=1, device_id={"frame": frame, "space": space},
                            device_id_type=pl.DeviceIdType.MESH)

    each(1, 32, lambda n: greet(rem(f + div(n, 4), 8), x * 4 + rem(loc + n, 4)))
    each(4, 16, lambda n: greet(f, rem(x * 4 + n, 16)))

    cnts[...] = jnp.full(cnts.shape, cnt_ref[0], jnp.int32)

    tok_copy.wait()
    for t in range(SLOT):
        values = tok_ref[t % times].astype(jnp.float32)
        for c in range(width // 128):
            xs[c, t * slots:t * slots + slots, :] = values[:, 128 * c:128 * c + 128]
    for i in range(slots):
        values = jnp.concatenate(
            [xs[c, pl.ds(i, SLOT, stride=slots), :] for c in range(width // 128)], axis=1)
        center = values - jnp.mean(values, axis=-1, keepdims=True)
        spread = jnp.mean(center * center, axis=-1, keepdims=True)
        normed = center * lax.rsqrt(spread + EPSILON) * gain_ref[...] + bias_ref[...]
        nb[i * SLOT:i * SLOT + SLOT, :] = normed.astype(jnp.bfloat16)

    rows_all = slots * SLOT
    half = rows_all // 2
    low = lax.broadcasted_iota(jnp.int32, (rows_all, 128), 1) < HD
    low_half = lax.broadcasted_iota(jnp.int32, (half, 128), 1) < HD

    copies[0].wait()
    copies[1].wait()
    copies[2].start()
    for g in range(2):
        k4 = jnp.dot(nb[...], w_v[:, inner + 256 * g:inner + 256 * g + 256], preferred_element_type=jnp.float32)
        v4 = jnp.dot(nb[...], w_v[:, 2 * inner + 256 * g:2 * inner + 256 * g + 256],
                     preferred_element_type=jnp.float32)
        for j in range(2):
            k2, v2 = k4[:, 128 * j:128 * j + 128], v4[:, 128 * j:128 * j + 128]
            h = 4 * g + 2 * j
            kvs[h] = jnp.where(low, k2, pltpu.roll(v2, HD, 1)).astype(jnp.bfloat16)
            kvs[h + 1] = jnp.where(low, pltpu.roll(k2, HD, 1), v2).astype(jnp.bfloat16)

    part = div(f, 2)
    mine = rem(f, 2) * 4 + loc
    source = x * 8 + mine
    pl.semaphore_wait(barrier, 43)

    def kv_copy(d):
        h = rem(f + d + 2 * loc, 8)
        stays = (h == f) & (part == loc)
        return stays, h, remote(
            kvs.at[h], kv_out.at[source], kv_send.at[0], kv_recv.at[mine], h, x * 4 + part)

    def kv_start(d):
        stays, h, copy = kv_copy(d)

        @pl.when(stays)
        def _():
            pltpu.make_async_copy(kvs.at[h], kv_out.at[source], kv_recv.at[mine]).start()

        @pl.when(jnp.logical_not(stays))
        def _():
            copy.start()

    each(0, 8, kv_start)

    def count_copy(e):
        return remote(cnts, cnt_out.at[s], c_send.at[0], c_recv.at[0], f, rem(s + e, 16))

    each(1, 16, lambda e: count_copy(e).start())
    pltpu.make_async_copy(cnts, cnt_out.at[s], c_recv.at[0]).start()

    copies[2].wait()
    last_copy.start()
    for g in range(2):
        q4 = jnp.dot(nb[...], w_v[:, 256 * g:256 * g + 256], preferred_element_type=jnp.float32) * SCALE
        for j in range(2):
            q2 = q4[:, 128 * j:128 * j + 128]
            h = 4 * g + 2 * j
            qs[h] = jnp.where(low_half, q2[:half], pltpu.roll(q2[half:], HD, 1)).astype(jnp.bfloat16)
            qs[h + 1] = jnp.where(low_half, pltpu.roll(q2[:half], HD, 1), q2[half:]).astype(jnp.bfloat16)

    me = f * 4 + loc

    def q_copy(n):
        h = rem(f + div(n, 4), 8)
        return remote(qs.at[h], q_out.at[me], q_send.at[0], q_recv.at[0], h, x * 4 + rem(loc + n, 4))

    def ring(piece, send, recv, step):
        return remote(kv_out.at[piece], kv_out.at[piece], send.at[0], recv, f, rem(x + step, 4) * 4 + loc)

    def nth(t):
        u = rem(f - 2 * loc - t + 16, 8)
        return rem(u, 2) * 4 + div(u, 2)

    right, left = rem(x + 1, 4) * 8, rem(x + 3, 4) * 8

    def landed(sem, ref):
        pltpu.make_async_copy(ref, ref, sem).wait()

    def to_right(t, piece):
        even = rem(t, 2) == 0

        @pl.when(even)
        def _():
            ring(piece, x_send, pass_recv.at[t], 1).start()

        @pl.when(jnp.logical_not(even))
        def _():
            ring(piece, x_send, rest_recv.at[0], 1).start()

    def to_left(t, piece):
        odd = rem(t, 2) == 1

        @pl.when(odd)
        def _():
            ring(piece, x_send, pass_recv.at[t], 3).start()

        @pl.when(jnp.logical_not(odd))
        def _():
            ring(piece, x_send, rest_recv.at[0], 3).start()

    def arrived(t):
        i = nth(t)
        piece = x * 8 + i
        landed(kv_recv.at[i], kv_out.at[piece])
        to_right(t, piece)
        to_left(t, piece)

    each(0, Q_AFTER, arrived)
    each(1, 32, lambda n: q_copy(n).start())
    pltpu.make_async_copy(qs.at[f], q_out.at[me], q_recv.at[0]).start()
    each(Q_AFTER, 8, arrived)

    def relay(t):
        piece = left + nth(2 * t)
        landed(pass_recv.at[2 * t], kv_out.at[piece])
        ring(piece, r_send, rest_recv.at[0], 1).start()
        piece = right + nth(2 * t + 1)
        landed(pass_recv.at[2 * t + 1], kv_out.at[piece])
        ring(piece, r_send, rest_recv.at[0], 3).start()

    each(0, 4, relay)

    last_copy.wait()
    landed(kv_send.at[0], kv_out.at[pl.ds(0, 7)])

    @pl.when(part != loc)
    def _():
        landed(kv_send.at[0], kv_out.at[0])

    landed(c_send.at[0], cnt_out.at[pl.ds(0, 15)])
    landed(q_send.at[0], q_out.at[pl.ds(0, 31)])
    landed(x_send.at[0], kv_out.at[pl.ds(0, 16)])
    landed(r_send.at[0], kv_out.at[pl.ds(0, 8)])
    landed(c_recv.at[0], cnt_out)
    landed(q_recv.at[0], q_out)
    landed(rest_recv.at[0], kv_out.at[pl.ds(0, 16)])


def project(tokens, count, gain, bias, w_qkv, w_out):
    times, slots, width = tokens.shape
    rows = slots * SLOT
    bf16, i32 = jnp.bfloat16, jnp.int32
    dma = pltpu.SemaphoreType.DMA
    return pl.pallas_call(
        project_kernel,
        out_shape=(VMEM((32, rows // 2, 128), bf16),
                   VMEM((32, rows, 128), bf16),
                   VMEM((16, 1, 128), i32),
                   VMEM(tokens.shape, bf16), VMEM(w_out.shape, bf16)),
        in_specs=[spec(pltpu.HBM), spec(SMEM), spec(VMEM), spec(VMEM), spec(pltpu.HBM), spec(pltpu.HBM)],
        out_specs=(spec(ANY), spec(ANY), spec(ANY), spec(VMEM), spec(ANY)),
        scratch_shapes=[
            VMEM(w_qkv.shape, bf16), VMEM((width // 128, rows, 128), jnp.float32), VMEM((rows, width), bf16),
            VMEM((HEADS, rows, 128), bf16), VMEM((HEADS, rows // 2, 128), bf16), VMEM((1, 128), i32),
            dma((5,)), dma((1,)), dma((8,)), dma((1,)), dma((1,)), dma((1,)), dma((1,)),
            dma((1,)), dma((1,)), dma((8,)), dma((1,)),
        ],
        compiler_params=pltpu.CompilerParams(collective_id=0, has_side_effects=True),
        name="project",
    )(tokens, count, gain, bias, w_qkv, w_out)


def attention_kernel(cnt_ref, q_ref, kv_ref, acc, kvc, qc, vt, qt, *held, times):
    base = (lax.axis_index("space") // 4) * 4
    kv_flat = kvc.reshape(kvc.shape[0] * SLOT, 128)
    q_flat = qc.reshape(qc.shape[0] * SLOT, 128)
    step_keys = KB

    def take_keys(n, unit):
        for j in range(4):
            for sub in range(2):
                kvc[unit + 2 * j + sub] = kv_ref[n // 4, sub, n % 4, j * SLOT:j * SLOT + SLOT, :]
        return unit + 2 * cnt_ref[n, 0, 0]

    unit = jnp.int32(0)
    for n in range(16):
        unit = take_keys(n, unit)
    key_units = unit
    for n in range(-(-step_keys // SLOT)):
        kvc[key_units + n] = kv_ref[0, 0, 0, 0:SLOT, :]

    unit = jnp.int32(0)
    for j in range(4):
        if j == 2:
            low_units = unit
        for l in range(4):
            live = j < cnt_ref[base + l, 0, 0]
            for f in range(8):
                qc[unit + f] = q_ref[f, l, (j % 2) * SLOT:(j % 2) * SLOT + SLOT, :]
            unit = unit + jnp.where(live, 8, 0)
    query_rows = unit * SLOT
    query_tiles = (query_rows + QB - 1) // QB
    key_rows = key_units * SLOT
    key_steps = (key_rows + step_keys - 1) // step_keys

    key_at = lax.broadcasted_iota(jnp.int32, (HD, KB), 1)
    row16 = lax.broadcasted_iota(jnp.int32, (16, KB), 0)

    def shape_keys(b, longest):
        turned = jnp.transpose(kv_flat[pl.ds(pl.multiple_of(b * KB, KB), KB), :])
        index = key_at + b * KB
        live = (index % SLOT < times) & (index < key_rows)
        vt[b, 0:HD, :] = jnp.where(live, turned[HD:], jnp.bfloat16(0.0))
        vt[b, HD:HD + 16, :] = jnp.where(live[:16] & (row16 == 0), 1.0, 0.0).astype(jnp.bfloat16)
        keys = jnp.where(live, turned[:HD], jnp.bfloat16(0.0)).astype(jnp.float32)
        return jnp.maximum(longest, jnp.sum(keys * keys, axis=0, keepdims=True))

    def in_pairs(body):
        return lambda i, longest: body(2 * i + 1, body(2 * i, longest))

    longest_key = lax.fori_loop(0, (key_steps + 1) // 2, in_pairs(shape_keys), jnp.zeros((1, KB), jnp.float32))

    col = lax.broadcasted_iota(jnp.int32, (HD, QB), 1)
    low_rows = low_units * SLOT

    def shape_queries(t, longest):
        turned = jnp.transpose(q_flat[pl.ds(pl.multiple_of(t * QB, QB), QB), :])
        index = col + t * QB
        query = jnp.where(index < low_rows, turned[:HD], turned[HD:])
        query = jnp.where(index < query_rows, query, jnp.bfloat16(0.0))
        qt[t, 0:HD, :] = query
        qt[t, HD:, :] = jnp.zeros((HD, QB), jnp.bfloat16)
        query = query.astype(jnp.float32)
        return jnp.maximum(longest, jnp.sum(query * query, axis=0, keepdims=True))

    longest_query = lax.fori_loop(0, (query_tiles + 1) // 2, in_pairs(shape_queries), jnp.zeros((1, QB), jnp.float32))
    safe = jnp.max(longest_key) * jnp.max(longest_query) < SAFE * SAFE

    def block_scores(b, t):
        keys = kv_flat[pl.ds(pl.multiple_of(b * KB, KB), KB), :]
        return jnp.dot(keys, qt[t], preferred_element_type=jnp.float32)

    def clear(t):
        acc[t] = jnp.zeros((HD + 16, QB), jnp.float32)

    def after(item):
        t, b = item
        turn = b + 1 == key_steps
        return jnp.minimum(jnp.where(turn, t + 1, t), query_tiles), jnp.where(turn, 0, b + 1)

    def add(u, item):
        t, b = item
        acc[t] += jnp.dot(vt[b], held[u][...], preferred_element_type=jnp.float32)

    def weigh(u, item):
        t, b = item
        held[u][...] = jnp.exp2(block_scores(b, t)).astype(jnp.bfloat16)

    def plain(i, carry):
        before, now = carry
        then = now[-1]
        later = []
        for u in range(UN):
            add(u, before[u])
            weigh(u, now[u])
            then = after(then)
            later.append(then)
        return now, tuple(later)

    def plain_all():
        each(0, query_tiles, clear)
        first = [(jnp.int32(0), jnp.int32(0))]
        for _ in range(UN - 1):
            first.append(after(first[-1]))
        for u in range(UN):
            weigh(u, first[u])
        second = [after(first[-1])]
        for _ in range(UN - 1):
            second.append(after(second[-1]))
        steps = (query_tiles * key_steps + UN - 1) // UN
        last, _ = lax.fori_loop(1, steps, plain, (tuple(first), tuple(second)))
        for u in range(UN):
            add(u, last[u])

    def shifted_tile(t):
        def step(b, carry):
            best, total = carry
            scores = block_scores(b, t)
            best_next = jnp.maximum(best, jnp.max(scores, axis=0, keepdims=True))
            weights = jnp.exp2(scores - best_next).astype(jnp.bfloat16)
            total = total * jnp.exp2(best - best_next) + jnp.dot(
                vt[b], weights, preferred_element_type=jnp.float32)
            return best_next, total

        best, total = lax.fori_loop(
            0, key_steps, step,
            (jnp.full((1, QB), DEAD, jnp.float32), jnp.zeros((HD + 16, QB), jnp.float32)))
        acc[t] = total
        acc[t, HD + 8:HD + 9, :] = best

    @pl.when(safe)
    def _():
        plain_all()

    @pl.when(jnp.logical_not(safe))
    def _():
        each(0, query_tiles, shifted_tile)


def attention(counts, q_all, kv_all, times):
    sources, half_rows, _ = q_all.shape
    q_units, k_units = 4 * sources, 4 * sources
    q_rows = (q_units * SLOT + QB - 1) // QB * QB
    step = KB
    k_rows = (k_units * SLOT + step - 1) // step * step
    fill = -(-step // SLOT)
    return pl.pallas_call(
        functools.partial(attention_kernel, times=times),
        out_shape=VMEM((q_rows // QB + 1, HD + 16, QB), jnp.float32),
        in_specs=[spec(SMEM), spec(VMEM), spec(VMEM)],
        out_specs=spec(VMEM),
        scratch_shapes=[
            VMEM((k_units + max(fill, 8), SLOT, 128), jnp.bfloat16),
            VMEM((q_units + 8, SLOT, 128), jnp.bfloat16),
            VMEM((k_rows // KB, HD + 16, KB), jnp.bfloat16),
            VMEM((q_rows // QB + 1, 128, QB), jnp.bfloat16),
            *[VMEM((KB, QB), jnp.bfloat16) for _ in range(UN)],
        ],
        compiler_params=pltpu.CompilerParams(vmem_limit_bytes=32 << 20),
        name="attention",
    )(counts, near(q_all.reshape(8, 4, half_rows, 128)),
      near(kv_all.reshape(4, 2, 4, 2 * half_rows, 128)))


def return_kernel(cnt_ref, acc, back_ref, back_lse, of, packed, sizes, theirs, size_theirs, both, size_both,
                  t_send, t_recv, o_send, o_recv, l_send, l_recv):
    f, _, x, loc = place()
    hi, core = div(loc, 2), rem(loc, 2)
    half_rows = packed.shape[1]
    barrier = pltpu.get_barrier_semaphore()

    def greet(frame, there):
        pl.semaphore_signal(barrier, inc=1, device_id={"frame": frame, "space": x * 4 + there},
                            device_id_type=pl.DeviceIdType.MESH)

    greet(f, hi * 2 + 1 - core)
    for n in range(1, 16):
        greet(rem(f + n // 2, 8), rem(hi + n, 2) * 2 + core)

    starts, unit = [], jnp.int32(0)
    for j in range(4):
        for l in range(4):
            live = j < cnt_ref[x * 4 + l, 0, 0]
            starts.append(jnp.where(live, unit, 0))
            unit = unit + jnp.where(live, 8, 0)
        if j == 1:
            low_rows = unit * SLOT
    lane = lax.broadcasted_iota(jnp.int32, (SLOT, 128), 1)
    in_low = lane < HD
    of_flat = of.reshape(of.shape[0] * SLOT, 128)
    col = lax.broadcasted_iota(jnp.int32, (HD, QB), 1)

    def put(t):
        weight_sum = acc[t, HD:HD + 1, :]
        out = acc[t, 0:HD, :] / weight_sum
        lse = jnp.broadcast_to(acc[t, HD + 8:HD + 9, :] + jnp.log2(weight_sum), (HD, QB))
        low = col + t * QB < low_rows
        both = jnp.concatenate([jnp.where(low, out, lse), jnp.where(low, lse, out)], axis=0)
        of_flat[pl.ds(pl.multiple_of(t * QB, QB), QB), :] = jnp.transpose(both)

    each(0, acc.shape[0] - 1, put)

    def gather(frame, kept):
        for l in range(4):
            i = (l % 2) * 16 + (l // 2) * 8
            for j in range(2):
                first = of[starts[j * 4 + l] + frame]
                second = of[starts[j * 4 + 8 + l] + frame]
                packed[i + frame, j * SLOT:j * SLOT + SLOT, :] = jnp.where(in_low, first, second).astype(jnp.bfloat16)
                kept[j] = jnp.where(rem(lane, HD) == i + frame, jnp.where(in_low, second, first), kept[j])
        return kept

    kept = lax.fori_loop(0, 8, gather, [jnp.zeros((SLOT, 128), jnp.float32)] * 2)
    rows = jnp.transpose(jnp.concatenate([*kept, jnp.zeros((128 - 2 * SLOT, 128), jnp.float32)], axis=0))
    sizes[0] = rows[HD:HD + 32]
    sizes[1] = rows[0:32]

    keep = core * 16
    give = 16 - keep

    def twin(src, dst, n):
        return remote(src, dst, t_send.at[n], t_recv.at[n], f, x * 4 + hi * 2 + 1 - core)

    pl.semaphore_wait(barrier, 16)
    order = (1 - hi, hi)
    shares = [twin(sizes.at[:, pl.ds(give, 16), :], size_theirs, 0)]
    for n in range(2):
        shares.append(twin(packed.at[pl.ds(give + 8 * order[n], 8)], theirs.at[pl.ds(8 * n, 8)], 1 + n))
    for copy in shares:
        copy.start()
    shares[0].wait_recv()

    turned = []
    for n in range(2):
        one = jnp.concatenate([sizes[n, pl.ds(pl.multiple_of(keep + 8 * o, 8), 8), :] for o in order], axis=0)
        two = jnp.concatenate([size_theirs[n, pl.ds(pl.multiple_of(8 * o, 8), 8), :] for o in order], axis=0)
        top = jnp.maximum(one, two)
        one, two = jnp.exp2(one - top), jnp.exp2(two - top)
        total = one + two
        whole = top + jnp.log2(total)
        for r in range(16):
            size_both[r, n:n + 1, :] = whole[r:r + 1]
        turned.append(jnp.transpose(
            jnp.concatenate([one / total, two / total, jnp.zeros((96, 128), jnp.float32)], axis=0)))
    low = lax.broadcasted_iota(jnp.int32, (half_rows, 128), 1) < HD
    me = hi * 8 + f

    def send(n, frame):
        r = n * 8 + frame
        space = x * 4 + order[n] * 2 + core
        remote(both.at[r], back_ref.at[me], o_send.at[0], o_recv.at[0], frame, space).start()
        remote(size_both.at[r], back_lse.at[me], l_send.at[0], l_recv.at[0], frame, space).start()

    for n in range(2):
        shares[1 + n].wait_recv()
        for r in range(8 * n, 8 * n + 8):
            one = jnp.where(low, turned[0][0:half_rows, r:r + 1], turned[1][0:half_rows, r:r + 1])
            two = jnp.where(low, turned[0][0:half_rows, 16 + r:17 + r], turned[1][0:half_rows, 16 + r:17 + r])
            own = packed[keep + 8 * order[n] + r % 8].astype(jnp.float32)
            both[r] = (own * one + theirs[r].astype(jnp.float32) * two).astype(jnp.bfloat16)
        each(0, 8 - n, lambda d, n=n: send(n, rem(f + 1 + d, 8)))
    pltpu.make_async_copy(both.at[8 + f], back_ref.at[me], o_recv.at[0]).start()
    pltpu.make_async_copy(size_both.at[8 + f], back_lse.at[me], l_recv.at[0]).start()

    for copy in shares:
        copy.wait_send()
    for sem, ref in ((o_send, back_ref.at[pl.ds(0, 15)]), (l_send, back_lse.at[pl.ds(0, 15)]),
                     (o_recv, back_ref), (l_recv, back_lse)):
        pltpu.make_async_copy(ref, ref, sem.at[0]).wait()


def give_results(counts, partial):
    dma = pltpu.SemaphoreType.DMA
    bf16, f32 = jnp.bfloat16, jnp.float32
    half_rows = 2 * SLOT
    return pl.pallas_call(
        return_kernel,
        out_shape=(VMEM((16, half_rows, 128), bf16), VMEM((16, 2, 128), f32)),
        in_specs=[spec(SMEM), spec(VMEM)],
        out_specs=(spec(ANY), spec(ANY)),
        scratch_shapes=[
            VMEM(((partial.shape[0] - 1) * QB // SLOT, SLOT, 128), f32),
            VMEM((32, half_rows, 128), bf16), VMEM((2, 32, 128), f32),
            VMEM((16, half_rows, 128), bf16), VMEM((2, 16, 128), f32),
            VMEM((16, half_rows, 128), bf16), VMEM((16, 2, 128), f32),
            dma((3,)), dma((3,)), dma((1,)), dma((1,)), dma((1,)), dma((1,))],
        compiler_params=pltpu.CompilerParams(
            collective_id=1, has_side_effects=True, vmem_limit_bytes=16 << 20),
        name="give_results",
    )(counts, near(partial))


def finish_kernel(tok_ref, cnt_ref, back_ref, lse_ref, w_ref, o_ref, att, ys, done, o_sem):
    times, slots, width = tok_ref.shape
    half = slots * SLOT // 2
    rows = slots * SLOT

    def shares(n):
        sizes = [lse_ref[p * 8:p * 8 + 8, n, :] for p in range(2)]
        top = jnp.maximum(sizes[0], sizes[1])
        powers = [jnp.exp2(v - top) for v in sizes]
        total = powers[0] + powers[1]
        return jnp.transpose(
            jnp.concatenate([v / total for v in powers] + [jnp.zeros((112, 128), jnp.float32)], axis=0))

    first, second = shares(0), shares(1)
    low = lax.broadcasted_iota(jnp.int32, (half, 128), 1) < HD

    def merged(h):
        out = jnp.zeros((half, 128), jnp.float32)
        for p in range(2):
            n = p * 8 + h
            share = jnp.where(low, first[0:half, n:n + 1], second[0:half, n:n + 1])
            out = out + back_ref[n].astype(jnp.float32) * share
        return out

    for j in range(HEADS // 2):
        a, b = merged(2 * j), merged(2 * j + 1)
        cols = slice(128 * j, 128 * j + 128)
        att[0:half, cols] = jnp.where(low, a, pltpu.roll(b, HD, 1)).astype(jnp.bfloat16)
        att[half:rows, cols] = jnp.where(low, pltpu.roll(a, HD, 1), b).astype(jnp.bfloat16)
    for c in range(width // 256):
        cols = slice(256 * c, 256 * c + 256)
        mixed = jnp.dot(att[...], w_ref[:, cols], preferred_element_type=jnp.float32)
        for i in range(slots):
            for e in range(2):
                ys[2 * c + e, pl.ds(i, SLOT, stride=slots), :] = (
                    mixed[i * SLOT:i * SLOT + SLOT, 128 * e:128 * e + 128])
    live = lax.broadcasted_iota(jnp.int32, (slots, width), 0) < cnt_ref[0]
    ends, copies = [times // 4, times // 2, times * 3 // 4, times], []
    for t in range(times):
        mixed = jnp.concatenate([ys[c, t * slots:t * slots + slots, :] for c in range(width // 128)], axis=1)
        value = tok_ref[t].astype(jnp.float32) + mixed
        done[t] = jnp.where(live, value, 0.0).astype(jnp.bfloat16)
        if t + 1 in ends:
            n = ends.index(t + 1)
            rows = pl.ds(ends[n - 1] if n else 0, ends[n] - (ends[n - 1] if n else 0))
            copies.append(pltpu.make_async_copy(done.at[rows], o_ref.at[rows], o_sem.at[n]))
            copies[n].start()
    for copy in copies:
        copy.wait()


def finish(tokens, count, back, sizes, w_out):
    times, slots, width = tokens.shape
    rows = slots * SLOT
    return pl.pallas_call(
        finish_kernel,
        out_shape=jax.ShapeDtypeStruct(tokens.shape, tokens.dtype),
        in_specs=[spec(VMEM), spec(SMEM), spec(VMEM), spec(VMEM), spec(VMEM)],
        out_specs=spec(ANY),
        scratch_shapes=[VMEM((rows, w_out.shape[0]), jnp.bfloat16), VMEM((width // 128, rows, 128), jnp.float32),
                        VMEM(tokens.shape, tokens.dtype), pltpu.SemaphoreType.DMA((4,))],
        compiler_params=pltpu.CompilerParams(vmem_limit_bytes=16 << 20),
        name="finish",
    )(near(tokens), count, near(back), near(sizes), near(w_out))


def on_device(tokens, tube_count, ln_gain, ln_bias, w_qkv, w_out):
    tokens = jnp.transpose(tokens, (1, 0, 2))
    q_all, kv_all, counts, tokens, w_out = project(
        tokens, tube_count, ln_gain.reshape(1, -1), ln_bias.reshape(1, -1), w_qkv, w_out)
    partial = attention(counts, q_all, kv_all, tokens.shape[0])
    mixed = finish(tokens, tube_count, *give_results(counts, partial), w_out)
    return jnp.transpose(mixed, (1, 0, 2))


def solution(mesh):
    in_specs = (P("space", "frame", None), P("space"), P(), P(), P(), P())
    return jax.shard_map(
        on_device, mesh=mesh, in_specs=in_specs, out_specs=P("space", "frame", None), check_vma=False)
```

```python
import functools

import jax
import jax.numpy as jnp
from jax import lax
from jax.experimental import pallas as pl
from jax.experimental.pallas import tpu as pltpu
from jax.sharding import PartitionSpec as P

HEADS = 8
HD = 64
SLOT = 40
KB = 256
UN = 8
QB = 512
DEAD = -1e30
Q_AFTER = 2
SAFE = 100.0
EPSILON = 1e-06
SCALE = 1.4426950408889634 / 8.0
ANY = pl.ANY
VMEM = pltpu.VMEM
SMEM = pltpu.SMEM


def spec(space):
    return pl.BlockSpec(memory_space=space)


def near(array):
    return pltpu.with_memory_space_constraint(array, VMEM)


def place():
    f, s = lax.axis_index("frame"), lax.axis_index("space")
    return f, s, div(s, 4), rem(s, 4)


def remote(src, dst, send, recv, frame, space):
    return pltpu.make_async_remote_copy(
        src_ref=src, dst_ref=dst, send_sem=send, recv_sem=recv,
        device_id={"frame": frame, "space": space}, device_id_type=pl.DeviceIdType.MESH)


def rem(a, n):
    return lax.rem(a, jnp.int32(n))


def div(a, n):
    return lax.div(a, jnp.int32(n))


def each(lo, hi, body):
    def step(i, c):
        body(i)
        return c
    lax.fori_loop(lo, hi, step, 0)


def project_kernel(tok_in, cnt_ref, gain_ref, bias_ref, w_ref, w_last, q_out, kv_out, cnt_out, tok_ref, w_next,
                   w_v, xs, nb, kvs, qs, cnts,
                   w_sem, kv_send, kv_recv, q_send, q_recv, c_send, c_recv, x_send, r_send, pass_recv, rest_recv):
    f, s, x, loc = place()
    times, slots, width = tok_ref.shape
    inner = HEADS * HD

    tok_copy = pltpu.make_async_copy(tok_in, tok_ref, w_sem.at[3])
    tok_copy.start()
    last_copy = pltpu.make_async_copy(w_last, w_next, w_sem.at[4])
    copies = []
    for n, at in enumerate((inner, 2 * inner, 0)):
        cols = pl.ds(at, inner)
        copies.append(pltpu.make_async_copy(w_ref.at[:, cols], w_v.at[:, cols], w_sem.at[n]))
    copies[0].start()
    copies[1].start()

    barrier = pltpu.get_barrier_semaphore()

    def greet(frame, space):
        pl.semaphore_signal(barrier, inc=1, device_id={"frame": frame, "space": space},
                            device_id_type=pl.DeviceIdType.MESH)

    each(1, 32, lambda n: greet(rem(f + div(n, 4), 8), x * 4 + rem(loc + n, 4)))
    each(4, 16, lambda n: greet(f, rem(x * 4 + n, 16)))

    cnts[...] = jnp.full(cnts.shape, cnt_ref[0], jnp.int32)

    tok_copy.wait()
    for t in range(SLOT):
        values = tok_ref[t % times].astype(jnp.float32)
        for c in range(width // 128):
            xs[c, t * slots:t * slots + slots, :] = values[:, 128 * c:128 * c + 128]
    for i in range(slots):
        values = jnp.concatenate(
            [xs[c, pl.ds(i, SLOT, stride=slots), :] for c in range(width // 128)], axis=1)
        center = values - jnp.mean(values, axis=-1, keepdims=True)
        spread = jnp.mean(center * center, axis=-1, keepdims=True)
        normed = center * lax.rsqrt(spread + EPSILON) * gain_ref[...] + bias_ref[...]
        nb[i * SLOT:i * SLOT + SLOT, :] = normed.astype(jnp.bfloat16)

    rows_all = slots * SLOT
    half = rows_all // 2
    low = lax.broadcasted_iota(jnp.int32, (rows_all, 128), 1) < HD
    low_half = lax.broadcasted_iota(jnp.int32, (half, 128), 1) < HD

    copies[0].wait()
    copies[1].wait()
    copies[2].start()
    for g in range(2):
        k4 = jnp.dot(nb[...], w_v[:, inner + 256 * g:inner + 256 * g + 256], preferred_element_type=jnp.float32)
        v4 = jnp.dot(nb[...], w_v[:, 2 * inner + 256 * g:2 * inner + 256 * g + 256],
                     preferred_element_type=jnp.float32)
        for j in range(2):
            k2, v2 = k4[:, 128 * j:128 * j + 128], v4[:, 128 * j:128 * j + 128]
            h = 4 * g + 2 * j
            kvs[h] = jnp.where(low, k2, pltpu.roll(v2, HD, 1)).astype(jnp.bfloat16)
            kvs[h + 1] = jnp.where(low, pltpu.roll(k2, HD, 1), v2).astype(jnp.bfloat16)

    part = div(f, 2)
    mine = rem(f, 2) * 4 + loc
    source = x * 8 + mine
    pl.semaphore_wait(barrier, 43)

    def kv_copy(d):
        h = rem(f + d + 2 * loc, 8)
        stays = (h == f) & (part == loc)
        return stays, h, remote(
            kvs.at[h], kv_out.at[source], kv_send.at[0], kv_recv.at[mine], h, x * 4 + part)

    def kv_start(d):
        stays, h, copy = kv_copy(d)

        @pl.when(stays)
        def _():
            pltpu.make_async_copy(kvs.at[h], kv_out.at[source], kv_recv.at[mine]).start()

        @pl.when(jnp.logical_not(stays))
        def _():
            copy.start()

    each(0, 8, kv_start)

    def count_copy(e):
        return remote(cnts, cnt_out.at[s], c_send.at[0], c_recv.at[0], f, rem(s + e, 16))

    each(1, 16, lambda e: count_copy(e).start())
    pltpu.make_async_copy(cnts, cnt_out.at[s], c_recv.at[0]).start()

    copies[2].wait()
    last_copy.start()
    for g in range(2):
        q4 = jnp.dot(nb[...], w_v[:, 256 * g:256 * g + 256], preferred_element_type=jnp.float32) * SCALE
        for j in range(2):
            q2 = q4[:, 128 * j:128 * j + 128]
            h = 4 * g + 2 * j
            qs[h] = jnp.where(low_half, q2[:half], pltpu.roll(q2[half:], HD, 1)).astype(jnp.bfloat16)
            qs[h + 1] = jnp.where(low_half, pltpu.roll(q2[:half], HD, 1), q2[half:]).astype(jnp.bfloat16)

    me = f * 4 + loc

    def q_copy(n):
        h = rem(f + div(n, 4), 8)
        return remote(qs.at[h], q_out.at[me], q_send.at[0], q_recv.at[0], h, x * 4 + rem(loc + n, 4))

    def ring(piece, send, recv, step):
        return remote(kv_out.at[piece], kv_out.at[piece], send.at[0], recv, f, rem(x + step, 4) * 4 + loc)

    def nth(t):
        u = rem(f - 2 * loc - t + 16, 8)
        return rem(u, 2) * 4 + div(u, 2)

    right, left = rem(x + 1, 4) * 8, rem(x + 3, 4) * 8

    def landed(sem, ref):
        pltpu.make_async_copy(ref, ref, sem).wait()

    def to_right(t, piece):
        even = rem(t, 2) == 0

        @pl.when(even)
        def _():
            ring(piece, x_send, pass_recv.at[t], 1).start()

        @pl.when(jnp.logical_not(even))
        def _():
            ring(piece, x_send, rest_recv.at[0], 1).start()

    def to_left(t, piece):
        odd = rem(t, 2) == 1

        @pl.when(odd)
        def _():
            ring(piece, x_send, pass_recv.at[t], 3).start()

        @pl.when(jnp.logical_not(odd))
        def _():
            ring(piece, x_send, rest_recv.at[0], 3).start()

    def arrived(t):
        i = nth(t)
        piece = x * 8 + i
        landed(kv_recv.at[i], kv_out.at[piece])
        to_right(t, piece)
        to_left(t, piece)

    each(0, Q_AFTER, arrived)
    each(1, 32, lambda n: q_copy(n).start())
    pltpu.make_async_copy(qs.at[f], q_out.at[me], q_recv.at[0]).start()
    each(Q_AFTER, 8, arrived)

    def relay(t):
        piece = left + nth(2 * t)
        landed(pass_recv.at[2 * t], kv_out.at[piece])
        ring(piece, r_send, rest_recv.at[0], 1).start()
        piece = right + nth(2 * t + 1)
        landed(pass_recv.at[2 * t + 1], kv_out.at[piece])
        ring(piece, r_send, rest_recv.at[0], 3).start()

    each(0, 4, relay)

    last_copy.wait()
    landed(kv_send.at[0], kv_out.at[pl.ds(0, 7)])

    @pl.when(part != loc)
    def _():
        landed(kv_send.at[0], kv_out.at[0])

    landed(c_send.at[0], cnt_out.at[pl.ds(0, 15)])
    landed(q_send.at[0], q_out.at[pl.ds(0, 31)])
    landed(x_send.at[0], kv_out.at[pl.ds(0, 16)])
    landed(r_send.at[0], kv_out.at[pl.ds(0, 8)])
    landed(c_recv.at[0], cnt_out)
    landed(q_recv.at[0], q_out)
    landed(rest_recv.at[0], kv_out.at[pl.ds(0, 16)])


def project(tokens, count, gain, bias, w_qkv, w_out):
    times, slots, width = tokens.shape
    rows = slots * SLOT
    bf16, i32 = jnp.bfloat16, jnp.int32
    dma = pltpu.SemaphoreType.DMA
    return pl.pallas_call(
        project_kernel,
        out_shape=(VMEM((32, rows // 2, 128), bf16),
                   VMEM((32, rows, 128), bf16),
                   VMEM((16, 1, 128), i32),
                   VMEM(tokens.shape, bf16), VMEM(w_out.shape, bf16)),
        in_specs=[spec(pltpu.HBM), spec(SMEM), spec(VMEM), spec(VMEM), spec(pltpu.HBM), spec(pltpu.HBM)],
        out_specs=(spec(ANY), spec(ANY), spec(ANY), spec(VMEM), spec(ANY)),
        scratch_shapes=[
            VMEM(w_qkv.shape, bf16), VMEM((width // 128, rows, 128), jnp.float32), VMEM((rows, width), bf16),
            VMEM((HEADS, rows, 128), bf16), VMEM((HEADS, rows // 2, 128), bf16), VMEM((1, 128), i32),
            dma((5,)), dma((1,)), dma((8,)), dma((1,)), dma((1,)), dma((1,)), dma((1,)),
            dma((1,)), dma((1,)), dma((8,)), dma((1,)),
        ],
        compiler_params=pltpu.CompilerParams(collective_id=0, has_side_effects=True),
        name="project",
    )(tokens, count, gain, bias, w_qkv, w_out)


def attention_kernel(cnt_ref, q_ref, kv_ref, acc, kvc, qc, vt, qt, *held, times):
    base = (lax.axis_index("space") // 4) * 4
    kv_flat = kvc.reshape(kvc.shape[0] * SLOT, 128)
    q_flat = qc.reshape(qc.shape[0] * SLOT, 128)
    step_keys = KB

    def take_keys(n, unit):
        for j in range(4):
            for sub in range(2):
                kvc[unit + 2 * j + sub] = kv_ref[n // 4, sub, n % 4, j * SLOT:j * SLOT + SLOT, :]
        return unit + 2 * cnt_ref[n, 0, 0]

    unit = jnp.int32(0)
    for n in range(16):
        unit = take_keys(n, unit)
    key_units = unit
    for n in range(-(-step_keys // SLOT)):
        kvc[key_units + n] = kv_ref[0, 0, 0, 0:SLOT, :]

    unit = jnp.int32(0)
    for j in range(4):
        if j == 2:
            low_units = unit
        for l in range(4):
            live = j < cnt_ref[base + l, 0, 0]
            for f in range(8):
                qc[unit + f] = q_ref[f, l, (j % 2) * SLOT:(j % 2) * SLOT + SLOT, :]
            unit = unit + jnp.where(live, 8, 0)
    query_rows = unit * SLOT
    query_tiles = (query_rows + QB - 1) // QB
    key_rows = key_units * SLOT
    key_steps = (key_rows + step_keys - 1) // step_keys

    key_at = lax.broadcasted_iota(jnp.int32, (HD, KB), 1)
    row16 = lax.broadcasted_iota(jnp.int32, (16, KB), 0)

    def shape_keys(b, longest):
        turned = jnp.transpose(kv_flat[pl.ds(pl.multiple_of(b * KB, KB), KB), :])
        index = key_at + b * KB
        live = (index % SLOT < times) & (index < key_rows)
        vt[b, 0:HD, :] = jnp.where(live, turned[HD:], jnp.bfloat16(0.0))
        vt[b, HD:HD + 16, :] = jnp.where(live[:16] & (row16 == 0), 1.0, 0.0).astype(jnp.bfloat16)
        keys = jnp.where(live, turned[:HD], jnp.bfloat16(0.0)).astype(jnp.float32)
        return jnp.maximum(longest, jnp.sum(keys * keys, axis=0, keepdims=True))

    def in_pairs(body):
        return lambda i, longest: body(2 * i + 1, body(2 * i, longest))

    longest_key = lax.fori_loop(0, (key_steps + 1) // 2, in_pairs(shape_keys), jnp.zeros((1, KB), jnp.float32))

    col = lax.broadcasted_iota(jnp.int32, (HD, QB), 1)
    low_rows = low_units * SLOT

    def shape_queries(t, longest):
        turned = jnp.transpose(q_flat[pl.ds(pl.multiple_of(t * QB, QB), QB), :])
        index = col + t * QB
        query = jnp.where(index < low_rows, turned[:HD], turned[HD:])
        query = jnp.where(index < query_rows, query, jnp.bfloat16(0.0))
        qt[t, 0:HD, :] = query
        qt[t, HD:, :] = jnp.zeros((HD, QB), jnp.bfloat16)
        query = query.astype(jnp.float32)
        return jnp.maximum(longest, jnp.sum(query * query, axis=0, keepdims=True))

    longest_query = lax.fori_loop(0, (query_tiles + 1) // 2, in_pairs(shape_queries), jnp.zeros((1, QB), jnp.float32))
    safe = jnp.max(longest_key) * jnp.max(longest_query) < SAFE * SAFE

    def block_scores(b, t):
        keys = kv_flat[pl.ds(pl.multiple_of(b * KB, KB), KB), :]
        return jnp.dot(keys, qt[t], preferred_element_type=jnp.float32)

    def clear(t):
        acc[t] = jnp.zeros((HD + 16, QB), jnp.float32)

    def after(item):
        t, b = item
        turn = b + 1 == key_steps
        return jnp.minimum(jnp.where(turn, t + 1, t), query_tiles), jnp.where(turn, 0, b + 1)

    def add(u, item):
        t, b = item
        acc[t] += jnp.dot(vt[b], held[u][...], preferred_element_type=jnp.float32)

    def weigh(u, item):
        t, b = item
        held[u][...] = jnp.exp2(block_scores(b, t)).astype(jnp.bfloat16)

    def plain(i, carry):
        before, now = carry
        then = now[-1]
        later = []
        for u in range(UN):
            add(u, before[u])
            weigh(u, now[u])
            then = after(then)
            later.append(then)
        return now, tuple(later)

    def plain_all():
        each(0, query_tiles, clear)
        first = [(jnp.int32(0), jnp.int32(0))]
        for _ in range(UN - 1):
            first.append(after(first[-1]))
        for u in range(UN):
            weigh(u, first[u])
        second = [after(first[-1])]
        for _ in range(UN - 1):
            second.append(after(second[-1]))
        steps = (query_tiles * key_steps + UN - 1) // UN
        last, _ = lax.fori_loop(1, steps, plain, (tuple(first), tuple(second)))
        for u in range(UN):
            add(u, last[u])

    def shifted_tile(t):
        def step(b, carry):
            best, total = carry
            scores = block_scores(b, t)
            best_next = jnp.maximum(best, jnp.max(scores, axis=0, keepdims=True))
            weights = jnp.exp2(scores - best_next).astype(jnp.bfloat16)
            total = total * jnp.exp2(best - best_next) + jnp.dot(
                vt[b], weights, preferred_element_type=jnp.float32)
            return best_next, total

        best, total = lax.fori_loop(
            0, key_steps, step,
            (jnp.full((1, QB), DEAD, jnp.float32), jnp.zeros((HD + 16, QB), jnp.float32)))
        acc[t] = total
        acc[t, HD + 8:HD + 9, :] = best

    @pl.when(safe)
    def _():
        plain_all()

    @pl.when(jnp.logical_not(safe))
    def _():
        each(0, query_tiles, shifted_tile)


def attention(counts, q_all, kv_all, times):
    sources, half_rows, _ = q_all.shape
    q_units, k_units = 4 * sources, 4 * sources
    q_rows = (q_units * SLOT + QB - 1) // QB * QB
    step = KB
    k_rows = (k_units * SLOT + step - 1) // step * step
    fill = -(-step // SLOT)
    return pl.pallas_call(
        functools.partial(attention_kernel, times=times),
        out_shape=VMEM((q_rows // QB + 1, HD + 16, QB), jnp.float32),
        in_specs=[spec(SMEM), spec(VMEM), spec(VMEM)],
        out_specs=spec(VMEM),
        scratch_shapes=[
            VMEM((k_units + max(fill, 8), SLOT, 128), jnp.bfloat16),
            VMEM((q_units + 8, SLOT, 128), jnp.bfloat16),
            VMEM((k_rows // KB, HD + 16, KB), jnp.bfloat16),
            VMEM((q_rows // QB + 1, 128, QB), jnp.bfloat16),
            *[VMEM((KB, QB), jnp.bfloat16) for _ in range(UN)],
        ],
        compiler_params=pltpu.CompilerParams(vmem_limit_bytes=32 << 20),
        name="attention",
    )(counts, near(q_all.reshape(8, 4, half_rows, 128)),
      near(kv_all.reshape(4, 2, 4, 2 * half_rows, 128)))


def return_kernel(cnt_ref, acc, back_ref, back_lse, of, packed, sizes, theirs, size_theirs, both, size_both,
                  t_send, t_recv, o_send, o_recv, l_send, l_recv):
    f, _, x, loc = place()
    hi, core = div(loc, 2), rem(loc, 2)
    half_rows = packed.shape[1]
    barrier = pltpu.get_barrier_semaphore()

    def greet(frame, there):
        pl.semaphore_signal(barrier, inc=1, device_id={"frame": frame, "space": x * 4 + there},
                            device_id_type=pl.DeviceIdType.MESH)

    greet(f, hi * 2 + 1 - core)
    for n in range(1, 16):
        greet(rem(f + n // 2, 8), rem(hi + n, 2) * 2 + core)

    starts, unit = [], jnp.int32(0)
    for j in range(4):
        for l in range(4):
            live = j < cnt_ref[x * 4 + l, 0, 0]
            starts.append(jnp.where(live, unit, 0))
            unit = unit + jnp.where(live, 8, 0)
        if j == 1:
            low_rows = unit * SLOT
    lane = lax.broadcasted_iota(jnp.int32, (SLOT, 128), 1)
    in_low = lane < HD
    of_flat = of.reshape(of.shape[0] * SLOT, 128)
    col = lax.broadcasted_iota(jnp.int32, (HD, QB), 1)

    def put(t):
        weight_sum = acc[t, HD:HD + 1, :]
        out = acc[t, 0:HD, :] / weight_sum
        lse = jnp.broadcast_to(acc[t, HD + 8:HD + 9, :] + jnp.log2(weight_sum), (HD, QB))
        low = col + t * QB < low_rows
        both = jnp.concatenate([jnp.where(low, out, lse), jnp.where(low, lse, out)], axis=0)
        of_flat[pl.ds(pl.multiple_of(t * QB, QB), QB), :] = jnp.transpose(both)

    each(0, acc.shape[0] - 1, put)

    def gather(frame, kept):
        for l in range(4):
            i = (l % 2) * 16 + (l // 2) * 8
            for j in range(2):
                first = of[starts[j * 4 + l] + frame]
                second = of[starts[j * 4 + 8 + l] + frame]
                packed[i + frame, j * SLOT:j * SLOT + SLOT, :] = jnp.where(in_low, first, second).astype(jnp.bfloat16)
                kept[j] = jnp.where(rem(lane, HD) == i + frame, jnp.where(in_low, second, first), kept[j])
        return kept

    kept = lax.fori_loop(0, 8, gather, [jnp.zeros((SLOT, 128), jnp.float32)] * 2)
    rows = jnp.transpose(jnp.concatenate([*kept, jnp.zeros((128 - 2 * SLOT, 128), jnp.float32)], axis=0))
    sizes[0] = rows[HD:HD + 32]
    sizes[1] = rows[0:32]

    keep = core * 16
    give = 16 - keep

    def twin(src, dst, n):
        return remote(src, dst, t_send.at[n], t_recv.at[n], f, x * 4 + hi * 2 + 1 - core)

    pl.semaphore_wait(barrier, 16)
    order = (1 - hi, hi)
    shares = [twin(sizes.at[:, pl.ds(give, 16), :], size_theirs, 0)]
    for n in range(2):
        shares.append(twin(packed.at[pl.ds(give + 8 * order[n], 8)], theirs.at[pl.ds(8 * n, 8)], 1 + n))
    for copy in shares:
        copy.start()
    shares[0].wait_recv()

    turned = []
    for n in range(2):
        one = jnp.concatenate([sizes[n, pl.ds(pl.multiple_of(keep + 8 * o, 8), 8), :] for o in order], axis=0)
        two = jnp.concatenate([size_theirs[n, pl.ds(pl.multiple_of(8 * o, 8), 8), :] for o in order], axis=0)
        top = jnp.maximum(one, two)
        one, two = jnp.exp2(one - top), jnp.exp2(two - top)
        total = one + two
        whole = top + jnp.log2(total)
        for r in range(16):
            size_both[r, n:n + 1, :] = whole[r:r + 1]
        turned.append(jnp.transpose(
            jnp.concatenate([one / total, two / total, jnp.zeros((96, 128), jnp.float32)], axis=0)))
    low = lax.broadcasted_iota(jnp.int32, (half_rows, 128), 1) < HD
    me = hi * 8 + f

    def send(n, frame):
        r = n * 8 + frame
        space = x * 4 + order[n] * 2 + core
        remote(both.at[r], back_ref.at[me], o_send.at[0], o_recv.at[0], frame, space).start()
        remote(size_both.at[r], back_lse.at[me], l_send.at[0], l_recv.at[0], frame, space).start()

    for n in range(2):
        shares[1 + n].wait_recv()
        for r in range(8 * n, 8 * n + 8):
            one = jnp.where(low, turned[0][0:half_rows, r:r + 1], turned[1][0:half_rows, r:r + 1])
            two = jnp.where(low, turned[0][0:half_rows, 16 + r:17 + r], turned[1][0:half_rows, 16 + r:17 + r])
            own = packed[keep + 8 * order[n] + r % 8].astype(jnp.float32)
            both[r] = (own * one + theirs[r].astype(jnp.float32) * two).astype(jnp.bfloat16)
        for d in range(8 - n):
            send(n, rem(f + 1 + d, 8))
    pltpu.make_async_copy(both.at[8 + f], back_ref.at[me], o_recv.at[0]).start()
    pltpu.make_async_copy(size_both.at[8 + f], back_lse.at[me], l_recv.at[0]).start()

    for copy in shares:
        copy.wait_send()
    for sem, ref in ((o_send, back_ref.at[pl.ds(0, 15)]), (l_send, back_lse.at[pl.ds(0, 15)]),
                     (o_recv, back_ref), (l_recv, back_lse)):
        pltpu.make_async_copy(ref, ref, sem.at[0]).wait()


def give_results(counts, partial):
    dma = pltpu.SemaphoreType.DMA
    bf16, f32 = jnp.bfloat16, jnp.float32
    half_rows = 2 * SLOT
    return pl.pallas_call(
        return_kernel,
        out_shape=(VMEM((16, half_rows, 128), bf16), VMEM((16, 2, 128), f32)),
        in_specs=[spec(SMEM), spec(VMEM)],
        out_specs=(spec(ANY), spec(ANY)),
        scratch_shapes=[
            VMEM(((partial.shape[0] - 1) * QB // SLOT, SLOT, 128), f32),
            VMEM((32, half_rows, 128), bf16), VMEM((2, 32, 128), f32),
            VMEM((16, half_rows, 128), bf16), VMEM((2, 16, 128), f32),
            VMEM((16, half_rows, 128), bf16), VMEM((16, 2, 128), f32),
            dma((3,)), dma((3,)), dma((1,)), dma((1,)), dma((1,)), dma((1,))],
        compiler_params=pltpu.CompilerParams(
            collective_id=1, has_side_effects=True, vmem_limit_bytes=16 << 20),
        name="give_results",
    )(counts, near(partial))


def finish_kernel(tok_ref, cnt_ref, back_ref, lse_ref, w_ref, o_ref, att, ys, done, o_sem):
    times, slots, width = tok_ref.shape
    half = slots * SLOT // 2
    rows = slots * SLOT

    def shares(n):
        sizes = [lse_ref[p * 8:p * 8 + 8, n, :] for p in range(2)]
        top = jnp.maximum(sizes[0], sizes[1])
        powers = [jnp.exp2(v - top) for v in sizes]
        total = powers[0] + powers[1]
        return jnp.transpose(
            jnp.concatenate([v / total for v in powers] + [jnp.zeros((112, 128), jnp.float32)], axis=0))

    first, second = shares(0), shares(1)
    low = lax.broadcasted_iota(jnp.int32, (half, 128), 1) < HD

    def merged(h):
        out = jnp.zeros((half, 128), jnp.float32)
        for p in range(2):
            n = p * 8 + h
            share = jnp.where(low, first[0:half, n:n + 1], second[0:half, n:n + 1])
            out = out + back_ref[n].astype(jnp.float32) * share
        return out

    for j in range(HEADS // 2):
        a, b = merged(2 * j), merged(2 * j + 1)
        cols = slice(128 * j, 128 * j + 128)
        att[0:half, cols] = jnp.where(low, a, pltpu.roll(b, HD, 1)).astype(jnp.bfloat16)
        att[half:rows, cols] = jnp.where(low, pltpu.roll(a, HD, 1), b).astype(jnp.bfloat16)
    for c in range(width // 256):
        cols = slice(256 * c, 256 * c + 256)
        mixed = jnp.dot(att[...], w_ref[:, cols], preferred_element_type=jnp.float32)
        for i in range(slots):
            for e in range(2):
                ys[2 * c + e, pl.ds(i, SLOT, stride=slots), :] = (
                    mixed[i * SLOT:i * SLOT + SLOT, 128 * e:128 * e + 128])
    live = lax.broadcasted_iota(jnp.int32, (slots, width), 0) < cnt_ref[0]
    ends, copies = [times // 4, times // 2, times * 3 // 4, times], []
    for t in range(times):
        mixed = jnp.concatenate([ys[c, t * slots:t * slots + slots, :] for c in range(width // 128)], axis=1)
        value = tok_ref[t].astype(jnp.float32) + mixed
        done[t] = jnp.where(live, value, 0.0).astype(jnp.bfloat16)
        if t + 1 in ends:
            n = ends.index(t + 1)
            rows = pl.ds(ends[n - 1] if n else 0, ends[n] - (ends[n - 1] if n else 0))
            copies.append(pltpu.make_async_copy(done.at[rows], o_ref.at[rows], o_sem.at[n]))
            copies[n].start()
    for copy in copies:
        copy.wait()


def finish(tokens, count, back, sizes, w_out):
    times, slots, width = tokens.shape
    rows = slots * SLOT
    return pl.pallas_call(
        finish_kernel,
        out_shape=jax.ShapeDtypeStruct(tokens.shape, tokens.dtype),
        in_specs=[spec(VMEM), spec(SMEM), spec(VMEM), spec(VMEM), spec(VMEM)],
        out_specs=spec(ANY),
        scratch_shapes=[VMEM((rows, w_out.shape[0]), jnp.bfloat16), VMEM((width // 128, rows, 128), jnp.float32),
                        VMEM(tokens.shape, tokens.dtype), pltpu.SemaphoreType.DMA((4,))],
        compiler_params=pltpu.CompilerParams(vmem_limit_bytes=16 << 20),
        name="finish",
    )(near(tokens), count, near(back), near(sizes), near(w_out))


def on_device(tokens, tube_count, ln_gain, ln_bias, w_qkv, w_out):
    tokens = jnp.transpose(tokens, (1, 0, 2))
    q_all, kv_all, counts, tokens, w_out = project(
        tokens, tube_count, ln_gain.reshape(1, -1), ln_bias.reshape(1, -1), w_qkv, w_out)
    partial = attention(counts, q_all, kv_all, tokens.shape[0])
    mixed = finish(tokens, tube_count, *give_results(counts, partial), w_out)
    return jnp.transpose(mixed, (1, 0, 2))


def solution(mesh):
    in_specs = (P("space", "frame", None), P("space"), P(), P(), P(), P())
    return jax.shard_map(
        on_device, mesh=mesh, in_specs=in_specs, out_specs=P("space", "frame", None), check_vma=False)
```
